32 devices in a mesh: dp: 1 (over z), sp2: 4 (over y), sp: 8 (over x, core).
Axes of the slice: x: 4, y: 4, z: 1, core: 2. Of those that a mesh axis runs over, the one named last changes fastest.
The devices are a block of a 4x4x8 slice.
Arguments:
- x: bfloat16 [8, 64, 512, 128], P('dp', 'sp', 'sp2')
- w_a: bfloat16 [3, 3, 3, 128, 128], replicated
- bn_a: float32 [3, 2, 128], replicated
- w_down: bfloat16 [3, 3, 128, 256], replicated
- bn_down: float32 [2, 256], replicated
- w_b: bfloat16 [2, 3, 3, 256, 256], replicated
- bn_b: float32 [2, 2, 256], replicated
Outputs:
- output: bfloat16 [8, 32, 256, 256], P('dp', 'sp', 'sp2')
All inputs are finite; a program needn't handle non-finite values.
Results may differ from the reference program's by a relative error of at most 0.00807789.
Values are sent between devices in bfloat16 or wider.
A program may use at most 768 MiB of HBM per device.

```python
import jax
import jax.numpy as jnp
from jax import lax

IMAGES = 8
IMG_HEIGHT = 64
IMG_WIDTH = 512
CHAN_A = 128
CHAN_B = 256
LAYERS_A = 3
LAYERS_B = 2

CONV_DIMS = ("NHWC", "HWIO", "NHWC")
SAME_PADS = ((1, 1), (1, 1))
DOWN_PADS = ((0, 1), (0, 1))


def norm_pairs(pair_key, lead_shape, num_chan):
    gain_key, shift_key = jax.random.split(pair_key)
    gains = 1.0 + 0.3 * jax.random.normal(gain_key, lead_shape + (1, num_chan), jnp.float32)
    shifts = 0.5 * jax.random.normal(shift_key, lead_shape + (1, num_chan), jnp.float32)
    return jnp.concatenate([gains, shifts], axis=-2)


def conv_weights(w_key, lead_shape, chan_in, chan_out):
    raw_w = jax.random.normal(w_key, lead_shape + (3, 3, chan_in, chan_out), jnp.float32)
    return (raw_w * (9 * chan_in) ** -0.5).astype(jnp.bfloat16)


def setup_inputs(seed: int = 0, part: int = 0) -> dict:
    sub_keys = jax.random.split(jax.random.key(seed), 7)
    img_keys = jax.random.split(jax.random.fold_in(sub_keys[0], part), 3)
    noise = jax.random.normal(img_keys[0], (IMAGES, IMG_HEIGHT, IMG_WIDTH, CHAN_A), jnp.float32)
    row_amp = jax.random.normal(img_keys[1], (IMAGES, 1, 1, CHAN_A), jnp.float32)
    col_amp = jax.random.normal(img_keys[2], (IMAGES, 1, 1, CHAN_A), jnp.float32)
    row_pos = (2.0 * (jnp.arange(IMG_HEIGHT, dtype=jnp.float32) + 0.5) / IMG_HEIGHT - 1.0).reshape(1, IMG_HEIGHT, 1, 1)
    col_pos = (2.0 * (jnp.arange(IMG_WIDTH, dtype=jnp.float32) + 0.5) / IMG_WIDTH - 1.0).reshape(1, 1, IMG_WIDTH, 1)
    images = (noise + 1.5 * row_amp * row_pos + col_amp * col_pos).astype(jnp.bfloat16)
    return {
        "x": images,
        "w_a": conv_weights(sub_keys[1], (LAYERS_A,), CHAN_A, CHAN_A),
        "bn_a": norm_pairs(sub_keys[2], (LAYERS_A,), CHAN_A),
        "w_down": conv_weights(sub_keys[3], (), CHAN_A, CHAN_B),
        "bn_down": norm_pairs(sub_keys[4], (), CHAN_B),
        "w_b": conv_weights(sub_keys[5], (LAYERS_B,), CHAN_B, CHAN_B),
        "bn_b": norm_pairs(sub_keys[6], (LAYERS_B,), CHAN_B),
    }


def conv_bn(act_in, weight, norm_pair, stride, pad_pairs):
    pre_norm = lax.conv_general_dilated(act_in.astype(jnp.float32), weight.astype(jnp.float32), (stride, stride), pad_pairs, dimension_numbers=CONV_DIMS)
    num_pos = pre_norm.shape[0] * pre_norm.shape[1] * pre_norm.shape[2]
    mean_val = jnp.sum(pre_norm, axis=(0, 1, 2)) / num_pos
    var_val = jnp.sum(pre_norm * pre_norm, axis=(0, 1, 2)) / num_pos - mean_val * mean_val
    normed = norm_pair[0] * (pre_norm - mean_val) * lax.rsqrt(var_val + 1e-5) + norm_pair[1]
    return jnp.maximum(normed, 0.0).astype(jnp.bfloat16)


def reference(x, w_a, bn_a, w_down, bn_down, w_b, bn_b):
    def stage_step(carry_act, layer_in):
        return conv_bn(carry_act, layer_in[0], layer_in[1], 1, SAME_PADS), None

    act_out, scan_rest = lax.scan(stage_step, x, (w_a, bn_a))
    act_out = conv_bn(act_out, w_down, bn_down, 2, DOWN_PADS)
    act_out, scan_rest = lax.scan(stage_step, act_out, (w_b, bn_b))
    return act_out
```

```python
import functools

import jax
import jax.numpy as jnp
from jax import lax
from jax.experimental import pallas as pl
from jax.experimental.pallas import tpu as pltpu
from jax.sharding import PartitionSpec as P

MESH = pl.DeviceIdType.MESH
F32 = jnp.float32
BF16 = jnp.bfloat16
EPS = 1e-5
PAD = 8


def net_kernel(dims, x, w_a, bn_a, w_down, bn_down, w_b, bn_b, y,
               xin, xh, xf, za, zb, ha, hb, yfa, yfb, ya, sa, yb,
               cs, cl, ksa, kla, ksb, klb, ta, tb, wy, ws, wd, wb, ga, gd, gb, yo,
               in_sem, w_sem, row_recv, row_send, col_recv, col_send, cor_recv, cor_send, st_recv, st_send, out_sem):
    rows_n, cols_n, n_img, height, width, chan = dims
    n_dev = rows_n * cols_n
    half_w = width // 2
    low_h = height // 2
    xstride = width + 2 * PAD
    fstride = half_w + 2 * PAD
    sp = lax.axis_index("sp")
    sp2 = lax.axis_index("sp2")
    me = sp2 * rows_n + sp
    has_up = sp > 0
    has_down = sp < rows_n - 1
    has_left = sp2 > 0
    has_right = sp2 < cols_n - 1
    row_ok = (has_up, has_down)
    col_ok = (has_left, has_right)
    cor_ok = tuple(r & c for r in row_ok for c in col_ok)

    def device(d_sp, d_sp2):
        return {"sp": sp + d_sp, "sp2": sp2 + d_sp2}

    for i in range(n_img):
        pltpu.make_async_copy(x.at[i], xin.at[i], in_sem.at[i]).start()
    weight_copies = []
    for kx, dst, k0, n0 in ((1, wy, 0, 0), (1, wy, chan, chan), (0, wy, 0, chan), (2, wy, chan, 0), (0, ws, 0, 0), (2, ws, chan, chan)):
        weight_copies.append((w_a.at[:, :, kx], dst.at[:, :, pl.ds(k0, chan), pl.ds(n0, chan)]))
    weight_copies.append((w_down.at[:, 0], wd.at[:, 0, pl.ds(0, chan), :]))
    weight_copies.append((w_down.at[:, 1], wd.at[:, 0, pl.ds(chan, chan), :]))
    weight_copies.append((w_down.at[:, 2], wd.at[:, 1, pl.ds(chan, chan), :]))
    weight_copies.append((w_b, wb))
    weight_copies.append((bn_a, ga))
    weight_copies.append((bn_down, gd))
    weight_copies.append((bn_b, gb))
    weight_copies = [pltpu.make_async_copy(s, d, w_sem.at[k]) for k, (s, d) in enumerate(weight_copies)]
    for copy in weight_copies:
        copy.start()

    barrier = pltpu.get_barrier_semaphore()

    def to_device(index):
        return {"sp": lax.rem(index, rows_n), "sp2": lax.div(index, rows_n)}

    def greet(k, carry):
        pl.semaphore_signal(barrier, inc=1, device_id=to_device(lax.rem(me + k, n_dev)), device_id_type=MESH)
        return carry

    lax.fori_loop(1, n_dev, greet, 0)

    zeros = jnp.zeros((chan, chan), BF16)
    for layer in range(3):
        for ky in range(3):
            ws[layer, ky, 0:chan, chan:2 * chan] = zeros
            ws[layer, ky, chan:2 * chan, 0:chan] = zeros
    for ky in range(3):
        wd[ky, 1, 0:chan, :] = jnp.zeros((chan, 2 * chan), BF16)

    for i in range(n_img):
        pltpu.make_async_copy(x.at[i], xin.at[i], in_sem.at[i]).wait()
    for i in range(n_img):
        for side, col0, line in ((0, 0, 0), (1, width - 16, 15)):
            blk = xin[i, :, col0:col0 + 16, :].astype(F32)
            yfa[0:height * 16, :] = blk.reshape(height * 16, chan)
            edge = yfa[pl.ds(line, height, stride=16), :]
            cs[0, side, i] = edge
            ksa[0, side, i] = edge[0:1]
            ksa[0, 2 + side, i] = edge[height - 1:height]

    pl.semaphore_wait(barrier, n_dev - 1)

    def cor_bufs(e):
        return (ksa.at[e], kla.at[e]) if e < 4 else (ksb.at[e - 4], klb.at[e - 4])

    def start_cols(e, sides=(0, 1), corners=(0, 1, 2, 3)):
        for side in sides:
            d = -1 if side == 0 else 1

            @pl.when(col_ok[side])
            def _():
                pltpu.make_async_remote_copy(cs.at[e, side], cl.at[e, 1 - side], col_send.at[e, side], col_recv.at[e, 1 - side],
                                             device_id=device(0, d), device_id_type=MESH).start()
        src, dst = cor_bufs(e)
        for corner in corners:
            d_sp = -1 if corner < 2 else 1
            d_sp2 = -1 if corner % 2 == 0 else 1

            @pl.when(cor_ok[corner])
            def _():
                pltpu.make_async_remote_copy(src.at[corner], dst.at[3 - corner], cor_send.at[e, corner], cor_recv.at[e, 3 - corner],
                                             device_id=device(d_sp, d_sp2), device_id_type=MESH).start()

    def wait_cols(e, sides=(0, 1), corners=(0, 1, 2, 3)):
        for side in sides:
            @pl.when(col_ok[side])
            def _():
                pltpu.make_async_copy(cl.at[e, side], cl.at[e, side], col_recv.at[e, side]).wait()
        src, dst = cor_bufs(e)
        for corner in corners:
            @pl.when(cor_ok[corner])
            def _():
                pltpu.make_async_copy(dst.at[corner], dst.at[corner], cor_recv.at[e, corner]).wait()

    def wait_col_sends(e, sides=(0, 1), corners=(0, 1, 2, 3)):
        for side in sides:
            @pl.when(col_ok[side])
            def _():
                pltpu.make_async_copy(cs.at[e, side], cs.at[e, side], col_send.at[e, side]).wait()
        src, dst = cor_bufs(e)
        for corner in corners:
            @pl.when(cor_ok[corner])
            def _():
                pltpu.make_async_copy(src.at[corner], src.at[corner], cor_send.at[e, corner]).wait()

    def row_landing(e, side):
        if e == 0:
            return xh.at[side]
        return ha.at[e - 1, side] if e < 4 else hb.at[e - 4, side]

    def send_row(e, side, i, src):
        @pl.when(row_ok[side])
        def _():
            pltpu.make_async_remote_copy(src, row_landing(e, 1 - side).at[i], row_send.at[e, side, i], row_recv.at[e, 1 - side, i],
                                         device_id=device(-1 if side == 0 else 1, 0), device_id_type=MESH).start()

    def wait_row(e, side, i):
        @pl.when(row_ok[side])
        def _():
            ref = row_landing(e, side).at[i]
            pltpu.make_async_copy(ref, ref, row_recv.at[e, side, i]).wait()

    def wait_row_sends(e, sides=(0, 1)):
        for side in sides:
            @pl.when(row_ok[side])
            def _():
                ref = row_landing(e, side)

                def one(i, carry):
                    pltpu.make_async_copy(ref.at[i], ref.at[i], row_send.at[e, side, i]).wait()
                    return carry

                lax.fori_loop(0, n_img, one, 0)

    def sums_refs(e):
        return ta.at[e] if e < 3 else tb.at[e - 3]

    def start_sums(e, part):
        buf = sums_refs(e)
        buf[me] = part

        def send(k, carry):
            to = to_device(lax.rem(me + k, n_dev))
            pltpu.make_async_remote_copy(buf.at[me], buf.at[me], st_send.at[e], st_recv.at[e], device_id=to, device_id_type=MESH).start()
            return carry

        lax.fori_loop(1, n_dev, send, 0)

    def finish_sums(e, num_pos):
        buf = sums_refs(e)
        rest = buf.at[pl.ds(0, n_dev - 1)]
        pltpu.make_async_copy(rest, rest, st_recv.at[e]).wait()
        total = jnp.sum(buf[...], axis=0) / num_pos
        lines = total.shape[0] // 2
        mean = total[0:lines]
        var = total[lines:] - mean * mean
        return mean, lax.rsqrt(var + EPS)

    def bn(z, par):
        mean, inv, gain, shift = par
        return jnp.maximum(gain * (z - mean) * inv + shift, 0.0)

    def keep(cond, val):
        return jnp.where(cond, val, 0.0)

    def prep_x(i):
        for side in range(2):
            wait_row(0, side, i)
        last = height + 1
        for r in range(height):
            xf[pl.ds((r + 1) * xstride + PAD, width), :] = xin[i, r].astype(F32)
        xf[pl.ds(PAD, width), :] = keep(has_up, xh[0, i].astype(F32))
        xf[pl.ds(last * xstride + PAD, width), :] = keep(has_down, xh[1, i].astype(F32))
        xf[pl.ds(xstride + PAD - 1, height, stride=xstride), :] = keep(has_left, cl[0, 0, i])
        xf[pl.ds(xstride + PAD + width, height, stride=xstride), :] = keep(has_right, cl[0, 1, i])
        for corner in range(4):
            row = 0 if corner < 2 else last
            col = PAD - 1 if corner % 2 == 0 else PAD + width
            xf[row * xstride + col:row * xstride + col + 1, :] = keep(cor_ok[corner], kla[0, corner, i])
        for r in range(height + 2):
            base = r * xstride + PAD
            even = xf[pl.ds(base, half_w, stride=2), :]
            odd = xf[pl.ds(base + 1, half_w, stride=2), :]
            before = xf[pl.ds(base - 1, half_w, stride=2), :]
            after = xf[pl.ds(base + 2, half_w, stride=2), :]
            ya[r] = jnp.concatenate([even, odd], axis=1).astype(BF16)
            sa[r] = jnp.concatenate([before, after], axis=1).astype(BF16)

    def norm_a(e, slot, par, i, up=True):
        last = height + 1
        lo = 0 if up else 1
        for side in (0, 1) if up else (1,):
            wait_row(e, side, i)
        for r in range(lo, height + 2):
            if r == 0:
                val = keep(has_up, bn(ha[e - 1, 0, i], par))
            elif r == last:
                val = keep(has_down, bn(ha[e - 1, 1, i], par))
            else:
                val = bn(za[slot, i, pl.ds((r - 1) * 2 * half_w, 2 * half_w), :], par)
            base = r * 2 * fstride + PAD
            yfa[base:base + half_w, :] = val[0:half_w]
            yfa[base + fstride:base + fstride + half_w, :] = val[half_w:]
        if up:
            yfa[pl.ds(3 * fstride + PAD - 1, height, stride=2 * fstride), :] = keep(has_left, bn(cl[e, 0, i], par))
        yfa[pl.ds(2 * fstride + PAD + half_w, height, stride=2 * fstride), :] = keep(has_right, bn(cl[e, 1, i], par))
        for corner in range(4) if up else (3,):
            row = 0 if corner < 2 else last
            at = row * 2 * fstride + (fstride + PAD - 1 if corner % 2 == 0 else PAD + half_w)
            yfa[at:at + 1, :] = keep(cor_ok[corner], bn(kla[e, corner, i], par))
        for r in range(lo, height + 2):
            base = r * 2 * fstride + PAD
            even = yfa[base:base + half_w, :]
            odd = yfa[base + fstride:base + fstride + half_w, :]
            before = yfa[base + fstride - 1:base + fstride - 1 + half_w, :]
            after = yfa[base + 1:base + 1 + half_w, :]
            ya[r] = jnp.concatenate([even, odd], axis=1).astype(BF16)
            sa[r] = jnp.concatenate([before, after], axis=1).astype(BF16)

    def norm_b(e, slot, par, i):
        last = low_h + 1
        halves = [tuple(p[h:h + 1] for p in par) for h in range(2)]
        tall = tuple(jnp.concatenate([p] * low_h, axis=0) for p in par)
        for side in range(2):
            wait_row(e, side, i)
        for r in range(low_h + 2):
            for h in range(2):
                if r == 0:
                    val = keep(has_up, bn(hb[e - 4, 0, i, pl.ds(h * half_w, half_w), :], halves[h]))
                elif r == last:
                    val = keep(has_down, bn(hb[e - 4, 1, i, pl.ds(h * half_w, half_w), :], halves[h]))
                else:
                    val = bn(zb[slot, i, pl.ds(((r - 1) * 2 + h) * half_w, half_w), :], halves[h])
                base = (r * 2 + h) * fstride + PAD
                yfb[base:base + half_w, :] = val
        yfb[pl.ds(2 * fstride + PAD - 1, 2 * low_h, stride=fstride), :] = keep(has_left, bn(cl[e, 0, i], tall))
        yfb[pl.ds(2 * fstride + PAD + half_w, 2 * low_h, stride=fstride), :] = keep(has_right, bn(cl[e, 1, i], tall))
        for corner in range(4):
            row = 0 if corner < 2 else last
            val = keep(cor_ok[corner], bn(klb[e - 4, corner, i], par))
            for h in range(2):
                at = (row * 2 + h) * fstride + (PAD - 1 if corner % 2 == 0 else PAD + half_w)
                yfb[at:at + 1, :] = val[h:h + 1]
        for r in range(low_h + 2):
            base = r * 2 * fstride + PAD
            for kx in range(3):
                at = base + kx - 1
                yb[kx, r] = jnp.concatenate([yfb[at:at + half_w, :], yfb[at + fstride:at + fstride + half_w, :]], axis=1).astype(BF16)

    def add_sums(acc, carry):
        tiles = acc.reshape(acc.shape[0] // 8, 8, acc.shape[1])
        return carry[0] + jnp.sum(tiles, axis=0), carry[1] + jnp.sum(tiles * tiles, axis=0)

    zero_sums = (jnp.zeros((8, 2 * chan), F32), jnp.zeros((8, 2 * chan), F32))

    def edges_a(e, slot, i, rows=(0, 1)):
        first = za[slot, i, pl.ds(0, height, stride=2 * half_w), :]
        final = za[slot, i, pl.ds(2 * half_w - 1, height, stride=2 * half_w), :]
        for side, edge in enumerate((first, final)):
            cs[e, side, i] = edge
            ksa[e, side, i] = edge[0:1]
            ksa[e, 2 + side, i] = edge[height - 1:height]
        for side in rows:
            at = 0 if side == 0 else (height - 1) * 2 * half_w
            send_row(e, side, i, za.at[slot, i, pl.ds(at, 2 * half_w), :])

    def edges_b(e, slot, i):
        first = zb[slot, i, pl.ds(0, 2 * low_h, stride=half_w), :]
        final = zb[slot, i, pl.ds(half_w - 1, 2 * low_h, stride=half_w), :]
        for side, edge in enumerate((first, final)):
            cs[e, side, i] = edge
            ksb[e - 4, side, i] = edge[0:2]
            ksb[e - 4, 2 + side, i] = edge[2 * low_h - 2:2 * low_h]
        for side in range(2):
            at = 0 if side == 0 else (low_h - 1) * 2 * half_w
            send_row(e, side, i, zb.at[slot, i, pl.ds(at, 2 * half_w), :])

    def store_z(ref, slot, i, acc, rows):
        for r in range(rows):
            at = r * 2 * half_w
            ref[slot, i, at:at + half_w, :] = acc[r * half_w:(r + 1) * half_w, 0:chan]
            ref[slot, i, at + half_w:at + 2 * half_w, :] = acc[r * half_w:(r + 1) * half_w, chan:2 * chan]

    def layer_a(layer, prep, rows):
        e, slot = layer + 1, layer % 2

        def image(i, carry):
            prep(i)
            acc = None
            for ky in range(3):
                for ref, w in ((ya, wy), (sa, ws)):
                    lhs = ref[ky:ky + height].reshape(height * half_w, 2 * chan)
                    d = jnp.dot(lhs, w[layer, ky], preferred_element_type=F32)
                    acc = d if acc is None else acc + d
            store_z(za, slot, i, acc, height)
            edges_a(e, slot, i, rows)
            return add_sums(acc, carry)

        s1, s2 = lax.fori_loop(0, n_img, image, zero_sums)
        s1, s2 = (jnp.sum(s, axis=0, keepdims=True) for s in (s1, s2))
        return jnp.concatenate([s1[:, 0:chan] + s1[:, chan:], s2[:, 0:chan] + s2[:, chan:]], axis=0)

    def layer_down(prep):
        def image(i, carry):
            prep(i)
            acc = None
            for ky in range(3):
                for part, ref in enumerate((ya, sa)):
                    lhs = jnp.concatenate([ref[1 + 2 * r + ky] for r in range(low_h)], axis=0)
                    d = jnp.dot(lhs, wd[ky, part], preferred_element_type=F32)
                    acc = d if acc is None else acc + d
            store_z(zb, 0, i, acc, low_h)
            edges_b(4, 0, i)
            return add_sums(acc, carry)

        return wide_part(lax.fori_loop(0, n_img, image, zero_sums))

    def wide_part(sums):
        s1, s2 = (jnp.sum(s, axis=0, keepdims=True) for s in sums)
        return jnp.concatenate([s1[:, 0:chan], s1[:, chan:], s2[:, 0:chan], s2[:, chan:]], axis=0)

    def layer_b(layer, prep, edges):
        slot = (layer + 1) % 2

        def image(i, carry):
            prep(i)
            acc = None
            for ky in range(3):
                for kx in range(3):
                    lhs = yb[kx, ky:ky + low_h].reshape(low_h * half_w, 2 * chan)
                    d = jnp.dot(lhs, wb[layer, ky, kx], preferred_element_type=F32)
                    acc = d if acc is None else acc + d
            store_z(zb, slot, i, acc, low_h)
            if edges:
                edges_b(5 + layer, slot, i)
            return add_sums(acc, carry)

        return wide_part(lax.fori_loop(0, n_img, image, zero_sums))

    for side in range(2):
        def send_x(i, carry, side=side):
            send_row(0, side, i, xin.at[i, 0 if side == 0 else height - 1])
            return carry

        lax.fori_loop(0, n_img, send_x, 0)
    start_cols(0)
    for copy in weight_copies:
        copy.wait()
    wait_cols(0)

    pos_a = n_dev * n_img * height * width
    pos_b = n_dev * n_img * low_h * half_w

    def params_a(e, layer):
        mean, inv = finish_sums(e, pos_a)
        return mean, inv, ga[layer, 0:1], ga[layer, 1:2]

    def params_b(e, ref):
        mean, inv = finish_sums(e, pos_b)
        gain = jnp.concatenate([ref[0:1, 0:chan], ref[0:1, chan:]], axis=0)
        shift = jnp.concatenate([ref[1:2, 0:chan], ref[1:2, chan:]], axis=0)
        return mean, inv, gain, shift

    start_sums(0, layer_a(0, prep_x, (0, 1)))
    start_cols(1)

    wait_row_sends(0)
    wait_col_sends(0)
    wait_cols(1)
    par = params_a(0, 0)
    start_sums(1, layer_a(1, functools.partial(norm_a, 1, 0, par), (0, 1)))
    start_cols(2)

    wait_row_sends(1)
    wait_col_sends(1)
    wait_cols(2)
    par = params_a(1, 1)
    start_sums(2, layer_a(2, functools.partial(norm_a, 2, 1, par), (0,)))
    start_cols(3, (0,), (0,))

    wait_row_sends(2)
    wait_col_sends(2)
    wait_cols(3, (1,), (3,))
    par = params_a(2, 2)
    start_sums(3, layer_down(functools.partial(norm_a, 3, 0, par, up=False)))
    start_cols(4)

    wait_row_sends(3, (0,))
    wait_col_sends(3, (0,), (0,))
    wait_cols(4)
    par = params_b(3, gd)
    start_sums(4, layer_b(0, functools.partial(norm_b, 4, 0, par), True))
    start_cols(5)

    wait_row_sends(4)
    wait_col_sends(4)
    wait_cols(5)
    par = params_b(4, gb.at[0])
    start_sums(5, layer_b(1, functools.partial(norm_b, 5, 1, par), False))

    wait_row_sends(5)
    wait_col_sends(5)
    par = params_b(5, gb.at[1])
    halves = [tuple(p[h:h + 1] for p in par) for h in range(2)]

    def finish(i, carry):
        for r in range(low_h):
            vals = [bn(zb[0, i, pl.ds((r * 2 + h) * half_w, half_w), :], halves[h]) for h in range(2)]
            yo[i, r] = jnp.concatenate(vals, axis=1).astype(BF16)
        pltpu.make_async_copy(yo.at[i], y.at[i], out_sem.at[i]).start()
        return carry

    lax.fori_loop(0, n_img, finish, 0)

    for e in range(6):
        buf = sums_refs(e)
        rest = buf.at[pl.ds(0, n_dev - 1)]
        pltpu.make_async_copy(rest, rest, st_send.at[e]).wait()

    def drain(i, carry):
        pltpu.make_async_copy(yo.at[i], y.at[i], out_sem.at[i]).wait()
        return carry

    lax.fori_loop(0, n_img, drain, 0)


def net(rows_n, cols_n, x, w_a, bn_a, w_down, bn_down, w_b, bn_b):
    n_img, height, width, chan = x.shape
    half_w, low_h = width // 2, height // 2
    n_dev = rows_n * cols_n
    fstride = half_w + 2 * PAD
    vmem, dma = pltpu.VMEM, pltpu.SemaphoreType.DMA
    scratch = [
        vmem((n_img, height, width, chan), BF16),
        vmem((2, n_img, width, chan), BF16),
        vmem(((height + 2) * (width + 2 * PAD), chan), F32),
        vmem((2, n_img, height * 2 * half_w, chan), F32),
        vmem((2, n_img, low_h * 2 * half_w, chan), F32),
        vmem((3, 2, n_img, 2 * half_w, chan), F32),
        vmem((2, 2, n_img, 2 * half_w, chan), F32),
        vmem(((height + 2) * 2 * fstride, chan), F32),
        vmem(((low_h + 2) * 2 * fstride, chan), F32),
        vmem((height + 2, half_w, 2 * chan), BF16),
        vmem((height + 2, half_w, 2 * chan), BF16),
        vmem((3, low_h + 2, half_w, 2 * chan), BF16),
        vmem((6, 2, n_img, height, chan), F32),
        vmem((6, 2, n_img, height, chan), F32),
        vmem((4, 4, n_img, 1, chan), F32),
        vmem((4, 4, n_img, 1, chan), F32),
        vmem((2, 4, n_img, 2, chan), F32),
        vmem((2, 4, n_img, 2, chan), F32),
        vmem((3, n_dev, 2, chan), F32),
        vmem((3, n_dev, 4, chan), F32),
        vmem((3, 3, 2 * chan, 2 * chan), BF16),
        vmem((3, 3, 2 * chan, 2 * chan), BF16),
        vmem((3, 2, 2 * chan, 2 * chan), BF16),
        vmem(w_b.shape, BF16),
        vmem(bn_a.shape, F32),
        vmem(bn_down.shape, F32),
        vmem(bn_b.shape, F32),
        vmem((n_img, low_h, half_w, 2 * chan), BF16),
        dma((n_img,)),
        dma((13,)),
        dma((6, 2, n_img)),
        dma((6, 2, n_img)),
        dma((6, 2)),
        dma((6, 2)),
        dma((6, 4)),
        dma((6, 4)),
        dma((6,)),
        dma((6,)),
        dma((n_img,)),
    ]
    any_spec = pl.BlockSpec(memory_space=pl.ANY)
    return pl.pallas_call(
        functools.partial(net_kernel, (rows_n, cols_n, n_img, height, width, chan)),
        out_shape=jax.ShapeDtypeStruct((n_img, low_h, half_w, 2 * chan), BF16),
        in_specs=[any_spec] * 7,
        out_specs=any_spec,
        scratch_shapes=scratch,
        compiler_params=pltpu.CompilerParams(collective_id=0, has_side_effects=True, vmem_limit_bytes=56 * 1024 * 1024),
        name="conv_bn_net",
    )(x, w_a, bn_a, w_down, bn_down, w_b, bn_b)


def solution(mesh):
    tile_spec = P("dp", "sp", "sp2", None)
    per_device = functools.partial(net, mesh.shape["sp"], mesh.shape["sp2"])
    return jax.shard_map(per_device, mesh=mesh, in_specs=(tile_spec, P(), P(), P(), P(), P(), P()), out_specs=tile_spec, check_vma=False)
```

```python
import functools

import jax
import jax.numpy as jnp
from jax import lax
from jax.experimental import pallas as pl
from jax.experimental.pallas import tpu as pltpu
from jax.sharding import PartitionSpec as P

MESH = pl.DeviceIdType.MESH
F32 = jnp.float32
BF16 = jnp.bfloat16
EPS = 1e-5
PAD = 8
SIDES = (0, 1)
CORNERS = (0, 1, 2, 3)
TAPS = range(3)
EARLY_A = 4
EARLY_B = 2


def net_kernel(dims, x, w_a, bn_a, w_down, bn_down, w_b, bn_b, zo, so,
               xin, xh, xf0, xf1, za0, za1, zb0, zb1, ha, hb, yfa0, yfa1, yfb0, yfb1, ya0, ya1, sa0, sa1, yb0, yb1,
               cs, cl, ksa, kla, ksb, klb, ta, tb, wy, ws, wd, wb, ga, gd, gb,
               in_sem, w_sem, row_recv, row_send, col_recv, col_send, cor_recv, cor_send, st_recv, st_send):
    rows_n, cols_n, n_img, height, width, chan = dims
    n_dev = rows_n * cols_n
    half_w, low_h = width // 2, height // 2
    line, wide = 2 * half_w, 2 * chan
    xstride = width + 2 * PAD
    fstride = half_w + 2 * PAD
    xfs, zas, zbs, yfas, yfbs, yas, sas, ybs = (xf0, xf1), (za0, za1), (zb0, zb1), (yfa0, yfa1), (yfb0, yfb1), (ya0, ya1), (sa0, sa1), (yb0, yb1)
    sp = lax.axis_index("sp")
    sp2 = lax.axis_index("sp2")
    me = sp2 * rows_n + sp
    has_up = sp > 0
    has_down = sp < rows_n - 1
    has_left = sp2 > 0
    has_right = sp2 < cols_n - 1
    row_ok = (has_up, has_down)
    col_ok = (has_left, has_right)
    cor_ok = tuple(r & c for r in row_ok for c in col_ok)

    def device(d_sp, d_sp2):
        return {"sp": sp + d_sp, "sp2": sp2 + d_sp2}

    for i in range(n_img):
        pltpu.make_async_copy(x.at[i], xin.at[i], in_sem.at[i]).start()
    weight_copies = []
    for kx, dst, k0, n0 in ((1, wy, 0, 0), (1, wy, chan, chan), (0, wy, 0, chan), (2, wy, chan, 0), (0, ws, 0, 0), (2, ws, chan, chan)):
        weight_copies.append((w_a.at[:, :, kx], dst.at[:, :, pl.ds(k0, chan), pl.ds(n0, chan)]))
    weight_copies.append((w_down.at[:, 0], wd.at[:, 0, pl.ds(0, chan), :]))
    weight_copies.append((w_down.at[:, 1], wd.at[:, 0, pl.ds(chan, chan), :]))
    weight_copies.append((w_down.at[:, 2], wd.at[:, 1, pl.ds(chan, chan), :]))
    weight_copies.append((w_b, wb))
    weight_copies.append((bn_a, ga))
    weight_copies.append((bn_down, gd))
    weight_copies.append((bn_b, gb))
    weight_copies = [pltpu.make_async_copy(s, d, w_sem.at[k]) for k, (s, d) in enumerate(weight_copies)]
    for copy in weight_copies:
        copy.start()

    barrier = pltpu.get_barrier_semaphore()

    chips = rows_n // 2
    chip, core = lax.div(sp, 2), lax.rem(sp, 2)
    lines = [[lax.rem(chip + d, chips) * 2 + c for c in (core, 1 - core)] for d in range(chips)]
    files = [lax.rem(sp2 + d, cols_n) for d in range(cols_n)]
    hops = {(dx, dy): min(dx, chips - dx) + min(dy, cols_n - dy) for dx in range(chips) for dy in range(cols_n)}
    others = [{"sp": lines[dx][flip], "sp2": files[dy]} for dx, dy in sorted(hops, key=lambda o: -hops[o]) for flip in (1, 0) if (dx, dy, flip) != (0, 0, 0)]

    for other in others:
        pl.semaphore_signal(barrier, inc=1, device_id=other, device_id_type=MESH)

    zeros = jnp.zeros((chan, chan), BF16)
    for layer in TAPS:
        for ky in TAPS:
            ws[layer, ky, 0:chan, chan:wide] = zeros
            ws[layer, ky, chan:wide, 0:chan] = zeros
    for ky in TAPS:
        wd[ky, 1, 0:chan, :] = jnp.zeros((chan, wide), BF16)

    for i in range(n_img):
        pltpu.make_async_copy(x.at[i], xin.at[i], in_sem.at[i]).wait()
    for i in range(n_img):
        for side, col0, pick in ((0, 0, 0), (1, width - 16, 15)):
            blk = xin[i, :, col0:col0 + 16, :].astype(F32)
            yfa0[0:height * 16, :] = blk.reshape(height * 16, chan)
            edge = yfa0[pl.ds(pick, height, stride=16), :]
            cs[0, side, i] = edge
            ksa[0, side, i] = edge[0:1]
            ksa[0, 2 + side, i] = edge[height - 1:height]

    pl.semaphore_wait(barrier, n_dev - 1)

    def cor_bufs(e):
        return (ksa.at[e], kla.at[e]) if e < 4 else (ksb.at[e - 4], klb.at[e - 4])

    def start_cols(e, sides=SIDES, corners=CORNERS):
        for side in sides:
            d = -1 if side == 0 else 1

            @pl.when(col_ok[side])
            def _():
                pltpu.make_async_remote_copy(cs.at[e, side], cl.at[e, 1 - side], col_send.at[e, side], col_recv.at[e, 1 - side],
                                             device_id=device(0, d), device_id_type=MESH).start()
        src, dst = cor_bufs(e)
        for corner in corners:
            d_sp = -1 if corner < 2 else 1
            d_sp2 = -1 if corner % 2 == 0 else 1

            @pl.when(cor_ok[corner])
            def _():
                pltpu.make_async_remote_copy(src.at[corner], dst.at[3 - corner], cor_send.at[e, corner], cor_recv.at[e, 3 - corner],
                                             device_id=device(d_sp, d_sp2), device_id_type=MESH).start()

    def wait_cols(e, sides=SIDES, corners=CORNERS):
        for side in sides:
            @pl.when(col_ok[side])
            def _():
                pltpu.make_async_copy(cl.at[e, side], cl.at[e, side], col_recv.at[e, side]).wait()
        src, dst = cor_bufs(e)
        for corner in corners:
            @pl.when(cor_ok[corner])
            def _():
                pltpu.make_async_copy(dst.at[corner], dst.at[corner], cor_recv.at[e, corner]).wait()

    def wait_col_sends(e, sides=SIDES, corners=CORNERS):
        for side in sides:
            @pl.when(col_ok[side])
            def _():
                pltpu.make_async_copy(cs.at[e, side], cs.at[e, side], col_send.at[e, side]).wait()
        src, dst = cor_bufs(e)
        for corner in corners:
            @pl.when(cor_ok[corner])
            def _():
                pltpu.make_async_copy(src.at[corner], src.at[corner], cor_send.at[e, corner]).wait()

    def row_landing(e, side):
        if e == 0:
            return xh.at[side]
        return ha.at[e - 1, side] if e < 4 else hb.at[e - 4, side]

    def row_source(e, side, i):
        if e == 0:
            return xin.at[i, 0 if side == 0 else height - 1]
        src, n_rows = (zas[(e - 1) % 2], height) if e < 4 else (zbs[e % 2], low_h)
        return src.at[i, pl.ds(0 if side == 0 else (n_rows - 1) * line, line)]

    def send_rows(e, sides, images, cond=True):
        for side in sides:
            @pl.when(row_ok[side] & cond)
            def _():
                for i in images:
                    pltpu.make_async_remote_copy(row_source(e, side, i), row_landing(e, 1 - side).at[i], row_send.at[e, side, i],
                                                 row_recv.at[e, 1 - side, i], device_id=device(-1 if side == 0 else 1, 0),
                                                 device_id_type=MESH).start()

    def wait_rows(e, sides, images, cond=True):
        for side in sides:
            @pl.when(row_ok[side] & cond)
            def _():
                for i in images:
                    ref = row_landing(e, side).at[i]
                    pltpu.make_async_copy(ref, ref, row_recv.at[e, side, i]).wait()

    def wait_row_sends(e, sides=SIDES):
        for side in sides:
            @pl.when(row_ok[side])
            def _():
                ref = row_landing(e, side)

                def one(i, carry):
                    pltpu.make_async_copy(ref.at[i], ref.at[i], row_send.at[e, side, i]).wait()
                    return carry

                lax.fori_loop(0, n_img, one, 0)

    def sums_refs(e):
        return ta.at[e] if e < 3 else tb.at[e - 3]

    def start_sums(e, part):
        buf = sums_refs(e)
        buf[me] = part

        for other in others:
            pltpu.make_async_remote_copy(buf.at[me], buf.at[me], st_send.at[e], st_recv.at[e], device_id=other, device_id_type=MESH).start()

    def finish_sums(e, num_pos):
        buf = sums_refs(e)
        rest = buf.at[pl.ds(0, n_dev - 1)]
        pltpu.make_async_copy(rest, rest, st_recv.at[e]).wait()
        total = jnp.sum(buf[...], axis=0) / num_pos
        lines = total.shape[0] // 2
        mean = total[0:lines]
        var = total[lines:] - mean * mean
        return mean, lax.rsqrt(var + EPS)

    def bn(z, par):
        mean, inv, gain, shift = par
        return jnp.maximum(gain * (z - mean) * inv + shift, 0.0)

    def keep(cond, val):
        return jnp.where(cond, val, 0.0)

    def prep_x(i, k):
        xf, ya, sa = xfs[k], yas[k], sas[k]
        last = height + 1
        for r in range(height):
            xf[pl.ds((r + 1) * xstride + PAD, width), :] = xin[i, r].astype(F32)
        xf[pl.ds(PAD, width), :] = keep(has_up, xh[0, i].astype(F32))
        xf[pl.ds(last * xstride + PAD, width), :] = keep(has_down, xh[1, i].astype(F32))
        xf[pl.ds(xstride + PAD - 1, height, stride=xstride), :] = keep(has_left, cl[0, 0, i])
        xf[pl.ds(xstride + PAD + width, height, stride=xstride), :] = keep(has_right, cl[0, 1, i])
        for corner in CORNERS:
            row = 0 if corner < 2 else last
            col = PAD - 1 if corner % 2 == 0 else PAD + width
            xf[row * xstride + col:row * xstride + col + 1, :] = keep(cor_ok[corner], kla[0, corner, i])
        for r in range(height + 2):
            base = r * xstride + PAD
            even = xf[pl.ds(base, half_w, stride=2), :]
            odd = xf[pl.ds(base + 1, half_w, stride=2), :]
            before = xf[pl.ds(base - 1, half_w, stride=2), :]
            after = xf[pl.ds(base + 2, half_w, stride=2), :]
            ya[r] = jnp.concatenate([even, odd], axis=1).astype(BF16)
            sa[r] = jnp.concatenate([before, after], axis=1).astype(BF16)

    def norm_a(e, par, i, k, up=True):
        za, yfa, ya, sa = zas[(e - 1) % 2], yfas[k], yas[k], sas[k]
        last = height + 1
        lo = 0 if up else 1
        for r in range(lo, height + 2):
            if r == 0:
                val = keep(has_up, bn(ha[e - 1, 0, i], par))
            elif r == last:
                val = keep(has_down, bn(ha[e - 1, 1, i], par))
            else:
                val = bn(za[i, pl.ds((r - 1) * line, line), :], par)
            base = r * 2 * fstride + PAD
            yfa[base:base + half_w, :] = val[0:half_w]
            yfa[base + fstride:base + fstride + half_w, :] = val[half_w:]
        if up:
            yfa[pl.ds(3 * fstride + PAD - 1, height, stride=2 * fstride), :] = keep(has_left, bn(cl[e, 0, i], par))
        yfa[pl.ds(2 * fstride + PAD + half_w, height, stride=2 * fstride), :] = keep(has_right, bn(cl[e, 1, i], par))
        for corner in CORNERS if up else (3,):
            row = 0 if corner < 2 else last
            at = row * 2 * fstride + (fstride + PAD - 1 if corner % 2 == 0 else PAD + half_w)
            yfa[at:at + 1, :] = keep(cor_ok[corner], bn(kla[e, corner, i], par))
        for r in range(lo, height + 2):
            base = r * 2 * fstride + PAD
            even = yfa[base:base + half_w, :]
            odd = yfa[base + fstride:base + fstride + half_w, :]
            before = yfa[base + fstride - 1:base + fstride - 1 + half_w, :]
            after = yfa[base + 1:base + 1 + half_w, :]
            ya[r] = jnp.concatenate([even, odd], axis=1).astype(BF16)
            sa[r] = jnp.concatenate([before, after], axis=1).astype(BF16)

    def norm_b(e, par, i, k):
        zb, yfb, yb = zbs[e % 2], yfbs[k], ybs[k]
        last = low_h + 1
        halves = [tuple(p[h:h + 1] for p in par) for h in SIDES]
        tall = tuple(jnp.concatenate([p] * low_h, axis=0) for p in par)
        for r in range(low_h + 2):
            for h in SIDES:
                if r == 0:
                    val = keep(has_up, bn(hb[e - 4, 0, i, pl.ds(h * half_w, half_w), :], halves[h]))
                elif r == last:
                    val = keep(has_down, bn(hb[e - 4, 1, i, pl.ds(h * half_w, half_w), :], halves[h]))
                else:
                    val = bn(zb[i, pl.ds(((r - 1) * 2 + h) * half_w, half_w), :], halves[h])
                base = (r * 2 + h) * fstride + PAD
                yfb[base:base + half_w, :] = val
        yfb[pl.ds(2 * fstride + PAD - 1, 2 * low_h, stride=fstride), :] = keep(has_left, bn(cl[e, 0, i], tall))
        yfb[pl.ds(2 * fstride + PAD + half_w, 2 * low_h, stride=fstride), :] = keep(has_right, bn(cl[e, 1, i], tall))
        for corner in CORNERS:
            row = 0 if corner < 2 else last
            val = keep(cor_ok[corner], bn(klb[e - 4, corner, i], par))
            for h in SIDES:
                at = (row * 2 + h) * fstride + (PAD - 1 if corner % 2 == 0 else PAD + half_w)
                yfb[at:at + 1, :] = val[h:h + 1]
        for r in range(low_h + 2):
            base = r * 2 * fstride + PAD
            for kx in TAPS:
                at = base + kx - 1
                yb[kx, r] = jnp.concatenate([yfb[at:at + half_w, :], yfb[at + fstride:at + fstride + half_w, :]], axis=1).astype(BF16)

    def add_sums(acc, carry):
        tiles = acc.reshape(acc.shape[0] // 8, 8, acc.shape[1])
        return carry[0] + jnp.sum(tiles, axis=0), carry[1] + jnp.sum(tiles * tiles, axis=0)

    zero_sums = (jnp.zeros((8, wide), F32), jnp.zeros((8, wide), F32))

    def edges_a(e, i):
        za = zas[(e - 1) % 2]
        first = za[i, pl.ds(0, height, stride=line), :]
        final = za[i, pl.ds(line - 1, height, stride=line), :]
        for side, edge in enumerate((first, final)):
            cs[e, side, i] = edge
            ksa[e, side, i] = edge[0:1]
            ksa[e, 2 + side, i] = edge[height - 1:height]

    def edges_b(e, i):
        zb = zbs[e % 2]
        first = zb[i, pl.ds(0, 2 * low_h, stride=half_w), :]
        final = zb[i, pl.ds(half_w - 1, 2 * low_h, stride=half_w), :]
        for side, edge in enumerate((first, final)):
            cs[e, side, i] = edge
            ksb[e - 4, side, i] = edge[0:2]
            ksb[e - 4, 2 + side, i] = edge[2 * low_h - 2:2 * low_h]

    def store_z(ref, i, acc, rows):
        for r in range(rows):
            at = r * line
            ref[i, at:at + half_w, :] = acc[r * half_w:(r + 1) * half_w, 0:chan]
            ref[i, at + half_w:at + line, :] = acc[r * half_w:(r + 1) * half_w, chan:wide]

    def products(pairs):
        acc = None
        for lhs, w in pairs:
            d = jnp.dot(lhs, w, preferred_element_type=F32)
            acc = d if acc is None else acc + d
        return acc

    def conv_a(layer, i, k, carry):
        pairs = []
        for ky in TAPS:
            for ref, w in ((yas[k], wy), (sas[k], ws)):
                pairs.append((ref[ky:ky + height].reshape(height * half_w, wide), w[layer, ky]))
        acc = products(pairs)
        store_z(zas[layer % 2], i, acc, height)
        edges_a(layer + 1, i)
        return add_sums(acc, carry)

    def conv_down(i, k, carry):
        pairs = []
        for ky in TAPS:
            for part, ref in enumerate((yas[k], sas[k])):
                pairs.append((jnp.concatenate([ref[1 + 2 * r + ky] for r in range(low_h)], axis=0), wd[ky, part]))
        acc = products(pairs)
        store_z(zbs[0], i, acc, low_h)
        edges_b(4, i)
        return add_sums(acc, carry)

    def conv_b(layer, i, k, carry):
        pairs = []
        for ky in TAPS:
            for kx in TAPS:
                pairs.append((ybs[k][kx, ky:ky + low_h].reshape(low_h * half_w, wide), wb[layer, ky, kx]))
        acc = products(pairs)
        if layer == 0:
            store_z(zb1, i, acc, low_h)
            edges_b(5, i)
        else:
            zo[i] = acc.reshape(low_h, half_w, wide)
        return add_sums(acc, carry)

    def layer(e, prep, conv, in_sides, out_sides, early):
        wait_rows(e, in_sides, (0,))
        prep(0, 0)

        def pair(j, carry):
            i = 2 * j
            wait_rows(e, in_sides, (i + 1,))
            wait_rows(e, in_sides, (i + 2,), i + 2 < n_img)
            prep(i + 1, 1)
            carry = conv(i, 0, carry)
            prep(lax.min(i + 2, n_img - 1), 0)
            carry = conv(i + 1, 1, carry)
            send_rows(e + 1, out_sides, (i, i + 1), i < early)
            return carry

        s1, s2 = lax.fori_loop(0, n_img // 2, pair, zero_sums)
        s1, s2 = (jnp.sum(s, axis=0, keepdims=True) for s in (s1, s2))
        if e < 3:
            part = [s1[:, 0:chan] + s1[:, chan:], s2[:, 0:chan] + s2[:, chan:]]
        else:
            part = [s1[:, 0:chan], s1[:, chan:], s2[:, 0:chan], s2[:, chan:]]
        start_sums(e, jnp.concatenate(part, axis=0))
        if e < 5:
            both = len(out_sides) == 2
            start_cols(e + 1, SIDES if both else (0,), CORNERS if both else (0,))
            send_rows(e + 1, out_sides, range(early, n_img))

    send_rows(0, SIDES, range(n_img))
    start_cols(0)
    for copy in weight_copies:
        copy.wait()
    wait_cols(0)

    pos_a = n_dev * n_img * height * width
    pos_b = n_dev * n_img * low_h * half_w

    def params_a(e, layer):
        mean, inv = finish_sums(e, pos_a)
        return mean, inv, ga[layer, 0:1], ga[layer, 1:2]

    def params_b(e, ref):
        mean, inv = finish_sums(e, pos_b)
        gain = jnp.concatenate([ref[0:1, 0:chan], ref[0:1, chan:]], axis=0)
        shift = jnp.concatenate([ref[1:2, 0:chan], ref[1:2, chan:]], axis=0)
        return mean, inv, gain, shift

    part = functools.partial
    layer(0, prep_x, part(conv_a, 0), SIDES, SIDES, EARLY_A)

    wait_row_sends(0)
    wait_col_sends(0)
    wait_cols(1)
    layer(1, part(norm_a, 1, params_a(0, 0)), part(conv_a, 1), SIDES, SIDES, EARLY_A)

    wait_row_sends(1)
    wait_col_sends(1)
    wait_cols(2)
    layer(2, part(norm_a, 2, params_a(1, 1)), part(conv_a, 2), SIDES, (0,), EARLY_A)

    wait_row_sends(2)
    wait_col_sends(2)
    wait_cols(3, (1,), (3,))
    layer(3, part(norm_a, 3, params_a(2, 2), up=False), conv_down, (1,), SIDES, EARLY_B)

    wait_row_sends(3, (0,))
    wait_col_sends(3, (0,), (0,))
    wait_cols(4)
    layer(4, part(norm_b, 4, params_b(3, gd)), part(conv_b, 0), SIDES, SIDES, EARLY_B)

    wait_row_sends(4)
    wait_col_sends(4)
    wait_cols(5)
    layer(5, part(norm_b, 5, params_b(4, gb.at[0])), part(conv_b, 1), SIDES, (), 0)

    wait_row_sends(5)
    wait_col_sends(5)
    mean, inv = finish_sums(5, pos_b)
    so[...] = jnp.concatenate([mean, inv], axis=0)

    for e in range(6):
        buf = sums_refs(e)
        rest = buf.at[pl.ds(0, n_dev - 1)]
        pltpu.make_async_copy(rest, rest, st_send.at[e]).wait()


def net(rows_n, cols_n, x, w_a, bn_a, w_down, bn_down, w_b, bn_b):
    n_img, height, width, chan = x.shape
    half_w, low_h = width // 2, height // 2
    n_dev = rows_n * cols_n
    vmem, dma = pltpu.VMEM, pltpu.SemaphoreType.DMA
    line, wide = 2 * half_w, 2 * chan
    plane = half_w + 2 * PAD
    a_sums, b_sums = 3, 3
    n_ex = a_sums + b_sums
    two, corners = len(SIDES), len(CORNERS)
    scratch = [
        vmem(x.shape, BF16),
        vmem((two, n_img, width, chan), BF16),
        *[vmem(((height + 2) * (width + 2 * PAD), chan), F32)] * two,
        *[vmem((n_img, height * line, chan), F32)] * two,
        *[vmem((n_img, low_h * line, chan), F32)] * two,
        vmem((a_sums, two, n_img, line, chan), F32),
        vmem((b_sums - 1, two, n_img, line, chan), F32),
        *[vmem(((height + 2) * 2 * plane, chan), F32)] * two,
        *[vmem(((low_h + 2) * 2 * plane, chan), F32)] * two,
        *[vmem((height + 2, half_w, wide), BF16)] * 4,
        *[vmem((3, low_h + 2, half_w, wide), BF16)] * two,
        *[vmem((n_ex, two, n_img, height, chan), F32)] * two,
        *[vmem((a_sums + 1, corners, n_img, 1, chan), F32)] * two,
        *[vmem((b_sums - 1, corners, n_img, 2, chan), F32)] * two,
        vmem((a_sums, n_dev, 2, chan), F32),
        vmem((b_sums, n_dev, 4, chan), F32),
        *[vmem((a_sums, 3, wide, wide), BF16)] * two,
        vmem((3, two, wide, wide), BF16),
        vmem(w_b.shape, BF16),
        vmem(bn_a.shape, F32),
        vmem(bn_down.shape, F32),
        vmem(bn_b.shape, F32),
        dma((n_img,)),
        dma((13,)),
        *[dma((n_ex, two, n_img))] * two,
        *[dma((n_ex, two))] * two,
        *[dma((n_ex, corners))] * two,
        *[dma((n_ex,))] * two,
    ]
    hbm_spec = pl.BlockSpec(memory_space=pltpu.HBM)
    z, stats = pl.pallas_call(
        functools.partial(net_kernel, (rows_n, cols_n, n_img, height, width, chan)),
        out_shape=(jax.ShapeDtypeStruct((n_img, low_h, half_w, wide), F32), jax.ShapeDtypeStruct((4, chan), F32)),
        in_specs=[hbm_spec] * 7,
        out_specs=(pl.BlockSpec(memory_space=pltpu.VMEM),) * 2,
        scratch_shapes=scratch,
        compiler_params=pltpu.CompilerParams(collective_id=0, has_side_effects=True, vmem_limit_bytes=40 * 1024 * 1024),
        name="conv_bn_net",
    )(x, w_a, bn_a, w_down, bn_down, w_b, bn_b)
    mean, inv = stats.reshape(2, wide)
    gain, shift = bn_b[1]
    return jnp.maximum(gain * (z - mean) * inv + shift, 0.0).astype(BF16)


def solution(mesh):
    tile_spec = P("dp", "sp", "sp2", None)
    per_device = functools.partial(net, mesh.shape["sp"], mesh.shape["sp2"])
    return jax.shard_map(per_device, mesh=mesh, in_specs=(tile_spec, P(), P(), P(), P(), P(), P()), out_specs=tile_spec, check_vma=False)
```

```python
import functools

import jax
import jax.numpy as jnp
from jax import lax
from jax.experimental import pallas as pl
from jax.experimental.pallas import tpu as pltpu
from jax.sharding import PartitionSpec as P

MESH = pl.DeviceIdType.MESH
F32 = jnp.float32
BF16 = jnp.bfloat16
EPS = 1e-5
PAD = 8
SIDES = (0, 1)
CORNERS = (0, 1, 2, 3)
TAPS = range(3)
EARLY_A = 4
EARLY_B = 2


def net_kernel(dims, x, w_a, bn_a, w_down, bn_down, w_b, bn_b, zo, mean_o, inv_o, gain_o, shift_o,
               xin, xh, xf0, xf1, za0, za1, zb0, zb1, ha, hb, yfa0, yfa1, yfb0, yfb1, ya0, ya1, sa0, sa1, yb0, yb1,
               cs, cl, ksa, kla, ksb, klb, ta, tb, wy, ws, wd, wb, ga, gd, gb,
               in_sem, w_sem, row_recv, row_send, col_recv, col_send, cor_recv, cor_send, st_recv, st_send):
    rows_n, cols_n, n_img, height, width, chan = dims
    n_dev = rows_n * cols_n
    half_w, low_h = width // 2, height // 2
    line, wide = 2 * half_w, 2 * chan
    xstride = width + 2 * PAD
    fstride = half_w + 2 * PAD
    xfs, zas, zbs, yfas, yfbs, yas, sas, ybs = (xf0, xf1), (za0, za1), (zb0, zb1), (yfa0, yfa1), (yfb0, yfb1), (ya0, ya1), (sa0, sa1), (yb0, yb1)
    sp = lax.axis_index("sp")
    sp2 = lax.axis_index("sp2")
    me = sp2 * rows_n + sp
    has_up = sp > 0
    has_down = sp < rows_n - 1
    has_left = sp2 > 0
    has_right = sp2 < cols_n - 1
    row_ok = (has_up, has_down)
    col_ok = (has_left, has_right)
    cor_ok = tuple(r & c for r in row_ok for c in col_ok)

    def device(d_sp, d_sp2):
        return {"sp": sp + d_sp, "sp2": sp2 + d_sp2}

    for i in range(n_img):
        pltpu.make_async_copy(x.at[i], xin.at[i], in_sem.at[i]).start()
    weight_copies = []
    for kx, dst, k0, n0 in ((1, wy, 0, 0), (1, wy, chan, chan), (0, wy, 0, chan), (2, wy, chan, 0), (0, ws, 0, 0), (2, ws, chan, chan)):
        weight_copies.append((w_a.at[:, :, kx], dst.at[:, :, pl.ds(k0, chan), pl.ds(n0, chan)]))
    weight_copies.append((w_down.at[:, 0], wd.at[:, 0, pl.ds(0, chan), :]))
    weight_copies.append((w_down.at[:, 1], wd.at[:, 0, pl.ds(chan, chan), :]))
    weight_copies.append((w_down.at[:, 2], wd.at[:, 1, pl.ds(chan, chan), :]))
    weight_copies.append((w_b, wb))
    weight_copies.append((bn_a, ga))
    weight_copies.append((bn_down, gd))
    weight_copies.append((bn_b, gb))
    weight_copies = [pltpu.make_async_copy(s, d, w_sem.at[k]) for k, (s, d) in enumerate(weight_copies)]
    for copy in weight_copies:
        copy.start()

    barrier = pltpu.get_barrier_semaphore()

    chips = rows_n // 2
    chip, core = lax.div(sp, 2), lax.rem(sp, 2)
    lines = [[lax.rem(chip + d, chips) * 2 + c for c in (core, 1 - core)] for d in range(chips)]
    files = [lax.rem(sp2 + d, cols_n) for d in range(cols_n)]
    hops = {(dx, dy): min(dx, chips - dx) + min(dy, cols_n - dy) for dx in range(chips) for dy in range(cols_n)}
    others = [{"sp": lines[dx][flip], "sp2": files[dy]} for dx, dy in sorted(hops, key=lambda o: -hops[o]) for flip in (1, 0) if (dx, dy, flip) != (0, 0, 0)]

    for other in others:
        pl.semaphore_signal(barrier, inc=1, device_id=other, device_id_type=MESH)

    zeros = jnp.zeros((chan, chan), BF16)
    for layer in TAPS:
        for ky in TAPS:
            ws[layer, ky, 0:chan, chan:wide] = zeros
            ws[layer, ky, chan:wide, 0:chan] = zeros
    for ky in TAPS:
        wd[ky, 1, 0:chan, :] = jnp.zeros((chan, wide), BF16)

    for i in range(n_img):
        pltpu.make_async_copy(x.at[i], xin.at[i], in_sem.at[i]).wait()
    for i in range(n_img):
        for side, col0, pick in ((0, 0, 0), (1, width - 16, 15)):
            blk = xin[i, :, col0:col0 + 16, :].astype(F32)
            yfa0[0:height * 16, :] = blk.reshape(height * 16, chan)
            edge = yfa0[pl.ds(pick, height, stride=16), :]
            cs[0, side, i] = edge
            ksa[0, side, i] = edge[0:1]
            ksa[0, 2 + side, i] = edge[height - 1:height]

    pl.semaphore_wait(barrier, n_dev - 1)

    def cor_bufs(e):
        return (ksa.at[e], kla.at[e]) if e < 4 else (ksb.at[e - 4], klb.at[e - 4])

    def start_cols(e, sides=SIDES, corners=CORNERS):
        for side in sides:
            d = -1 if side == 0 else 1

            @pl.when(col_ok[side])
            def _():
                pltpu.make_async_remote_copy(cs.at[e, side], cl.at[e, 1 - side], col_send.at[e, side], col_recv.at[e, 1 - side],
                                             device_id=device(0, d), device_id_type=MESH).start()
        src, dst = cor_bufs(e)
        for corner in corners:
            d_sp = -1 if corner < 2 else 1
            d_sp2 = -1 if corner % 2 == 0 else 1

            @pl.when(cor_ok[corner])
            def _():
                pltpu.make_async_remote_copy(src.at[corner], dst.at[3 - corner], cor_send.at[e, corner], cor_recv.at[e, 3 - corner],
                                             device_id=device(d_sp, d_sp2), device_id_type=MESH).start()

    def wait_cols(e, sides=SIDES, corners=CORNERS):
        for side in sides:
            @pl.when(col_ok[side])
            def _():
                pltpu.make_async_copy(cl.at[e, side], cl.at[e, side], col_recv.at[e, side]).wait()
        src, dst = cor_bufs(e)
        for corner in corners:
            @pl.when(cor_ok[corner])
            def _():
                pltpu.make_async_copy(dst.at[corner], dst.at[corner], cor_recv.at[e, corner]).wait()

    def wait_col_sends(e, sides=SIDES, corners=CORNERS):
        for side in sides:
            @pl.when(col_ok[side])
            def _():
                pltpu.make_async_copy(cs.at[e, side], cs.at[e, side], col_send.at[e, side]).wait()
        src, dst = cor_bufs(e)
        for corner in corners:
            @pl.when(cor_ok[corner])
            def _():
                pltpu.make_async_copy(src.at[corner], src.at[corner], cor_send.at[e, corner]).wait()

    def row_landing(e, side):
        if e == 0:
            return xh.at[side]
        return ha.at[e - 1, side] if e < 4 else hb.at[e - 4, side]

    def row_source(e, side, i):
        if e == 0:
            return xin.at[i, 0 if side == 0 else height - 1]
        src, n_rows = (zas[(e - 1) % 2], height) if e < 4 else (zbs[e % 2], low_h)
        return src.at[i, pl.ds(0 if side == 0 else (n_rows - 1) * line, line)]

    def send_rows(e, sides, images, cond=True):
        for side in sides:
            @pl.when(row_ok[side] & cond)
            def _():
                for i in images:
                    pltpu.make_async_remote_copy(row_source(e, side, i), row_landing(e, 1 - side).at[i], row_send.at[e, side, i],
                                                 row_recv.at[e, 1 - side, i], device_id=device(-1 if side == 0 else 1, 0),
                                                 device_id_type=MESH).start()

    def wait_rows(e, sides, images, cond=True):
        for side in sides:
            @pl.when(row_ok[side] & cond)
            def _():
                for i in images:
                    ref = row_landing(e, side).at[i]
                    pltpu.make_async_copy(ref, ref, row_recv.at[e, side, i]).wait()

    def wait_row_sends(e, sides=SIDES):
        for side in sides:
            @pl.when(row_ok[side])
            def _():
                ref = row_landing(e, side)

                def one(i, carry):
                    pltpu.make_async_copy(ref.at[i], ref.at[i], row_send.at[e, side, i]).wait()
                    return carry

                lax.fori_loop(0, n_img, one, 0)

    def sums_refs(e):
        return ta.at[e] if e < 3 else tb.at[e - 3]

    def start_sums(e, part):
        buf = sums_refs(e)
        buf[me] = part

        for other in others:
            pltpu.make_async_remote_copy(buf.at[me], buf.at[me], st_send.at[e], st_recv.at[e], device_id=other, device_id_type=MESH).start()

    def finish_sums(e, num_pos):
        buf = sums_refs(e)
        rest = buf.at[pl.ds(0, n_dev - 1)]
        pltpu.make_async_copy(rest, rest, st_recv.at[e]).wait()
        total = jnp.sum(buf[...], axis=0) / num_pos
        lines = total.shape[0] // 2
        mean = total[0:lines]
        var = total[lines:] - mean * mean
        return mean, lax.rsqrt(var + EPS)

    def bn(z, par):
        mean, inv, gain, shift = par
        return jnp.maximum(gain * (z - mean) * inv + shift, 0.0)

    def keep(cond, val):
        return jnp.where(cond, val, 0.0)

    def prep_x(i, k):
        xf, ya, sa = xfs[k], yas[k], sas[k]
        last = height + 1
        for r in range(height):
            xf[pl.ds((r + 1) * xstride + PAD, width), :] = xin[i, r].astype(F32)
        xf[pl.ds(PAD, width), :] = keep(has_up, xh[0, i].astype(F32))
        xf[pl.ds(last * xstride + PAD, width), :] = keep(has_down, xh[1, i].astype(F32))
        xf[pl.ds(xstride + PAD - 1, height, stride=xstride), :] = keep(has_left, cl[0, 0, i])
        xf[pl.ds(xstride + PAD + width, height, stride=xstride), :] = keep(has_right, cl[0, 1, i])
        for corner in CORNERS:
            row = 0 if corner < 2 else last
            col = PAD - 1 if corner % 2 == 0 else PAD + width
            xf[row * xstride + col:row * xstride + col + 1, :] = keep(cor_ok[corner], kla[0, corner, i])
        for r in range(height + 2):
            base = r * xstride + PAD
            even = xf[pl.ds(base, half_w, stride=2), :]
            odd = xf[pl.ds(base + 1, half_w, stride=2), :]
            before = xf[pl.ds(base - 1, half_w, stride=2), :]
            after = xf[pl.ds(base + 2, half_w, stride=2), :]
            ya[r] = jnp.concatenate([even, odd], axis=1).astype(BF16)
            sa[r] = jnp.concatenate([before, after], axis=1).astype(BF16)

    def norm_a(e, par, i, k, up=True):
        za, yfa, ya, sa = zas[(e - 1) % 2], yfas[k], yas[k], sas[k]
        last = height + 1
        lo = 0 if up else 1
        for r in range(lo, height + 2):
            if r == 0:
                val = keep(has_up, bn(ha[e - 1, 0, i], par))
            elif r == last:
                val = keep(has_down, bn(ha[e - 1, 1, i], par))
            else:
                val = bn(za[i, pl.ds((r - 1) * line, line), :], par)
            base = r * 2 * fstride + PAD
            yfa[base:base + half_w, :] = val[0:half_w]
            yfa[base + fstride:base + fstride + half_w, :] = val[half_w:]
        if up:
            yfa[pl.ds(3 * fstride + PAD - 1, height, stride=2 * fstride), :] = keep(has_left, bn(cl[e, 0, i], par))
        yfa[pl.ds(2 * fstride + PAD + half_w, height, stride=2 * fstride), :] = keep(has_right, bn(cl[e, 1, i], par))
        for corner in CORNERS if up else (3,):
            row = 0 if corner < 2 else last
            at = row * 2 * fstride + (fstride + PAD - 1 if corner % 2 == 0 else PAD + half_w)
            yfa[at:at + 1, :] = keep(cor_ok[corner], bn(kla[e, corner, i], par))
        for r in range(lo, height + 2):
            base = r * 2 * fstride + PAD
            even = yfa[base:base + half_w, :]
            odd = yfa[base + fstride:base + fstride + half_w, :]
            before = yfa[base + fstride - 1:base + fstride - 1 + half_w, :]
            after = yfa[base + 1:base + 1 + half_w, :]
            ya[r] = jnp.concatenate([even, odd], axis=1).astype(BF16)
            sa[r] = jnp.concatenate([before, after], axis=1).astype(BF16)

    def norm_b(e, par, i, k):
        zb, yfb, yb = zbs[e % 2], yfbs[k], ybs[k]
        last = low_h + 1
        halves = [tuple(p[h:h + 1] for p in par) for h in SIDES]
        tall = tuple(jnp.concatenate([p] * low_h, axis=0) for p in par)
        for r in range(low_h + 2):
            for h in SIDES:
                if r == 0:
                    val = keep(has_up, bn(hb[e - 4, 0, i, pl.ds(h * half_w, half_w), :], halves[h]))
                elif r == last:
                    val = keep(has_down, bn(hb[e - 4, 1, i, pl.ds(h * half_w, half_w), :], halves[h]))
                else:
                    val = bn(zb[i, pl.ds(((r - 1) * 2 + h) * half_w, half_w), :], halves[h])
                base = (r * 2 + h) * fstride + PAD
                yfb[base:base + half_w, :] = val
        yfb[pl.ds(2 * fstride + PAD - 1, 2 * low_h, stride=fstride), :] = keep(has_left, bn(cl[e, 0, i], tall))
        yfb[pl.ds(2 * fstride + PAD + half_w, 2 * low_h, stride=fstride), :] = keep(has_right, bn(cl[e, 1, i], tall))
        for corner in CORNERS:
            row = 0 if corner < 2 else last
            val = keep(cor_ok[corner], bn(klb[e - 4, corner, i], par))
            for h in SIDES:
                at = (row * 2 + h) * fstride + (PAD - 1 if corner % 2 == 0 else PAD + half_w)
                yfb[at:at + 1, :] = val[h:h + 1]
        for r in range(low_h + 2):
            base = r * 2 * fstride + PAD
            for kx in TAPS:
                at = base + kx - 1
                yb[kx, r] = jnp.concatenate([yfb[at:at + half_w, :], yfb[at + fstride:at + fstride + half_w, :]], axis=1).astype(BF16)

    def add_sums(acc, carry):
        tiles = acc.reshape(acc.shape[0] // 8, 8, acc.shape[1])
        return carry[0] + jnp.sum(tiles, axis=0), carry[1] + jnp.sum(tiles * tiles, axis=0)

    zero_sums = (jnp.zeros((8, wide), F32), jnp.zeros((8, wide), F32))

    def edges_a(e, i):
        za = zas[(e - 1) % 2]
        first = za[i, pl.ds(0, height, stride=line), :]
        final = za[i, pl.ds(line - 1, height, stride=line), :]
        for side, edge in enumerate((first, final)):
            cs[e, side, i] = edge
            ksa[e, side, i] = edge[0:1]
            ksa[e, 2 + side, i] = edge[height - 1:height]

    def edges_b(e, i):
        zb = zbs[e % 2]
        first = zb[i, pl.ds(0, 2 * low_h, stride=half_w), :]
        final = zb[i, pl.ds(half_w - 1, 2 * low_h, stride=half_w), :]
        for side, edge in enumerate((first, final)):
            cs[e, side, i] = edge
            ksb[e - 4, side, i] = edge[0:2]
            ksb[e - 4, 2 + side, i] = edge[2 * low_h - 2:2 * low_h]

    def store_z(ref, i, acc, rows):
        for r in range(rows):
            at = r * line
            ref[i, at:at + half_w, :] = acc[r * half_w:(r + 1) * half_w, 0:chan]
            ref[i, at + half_w:at + line, :] = acc[r * half_w:(r + 1) * half_w, chan:wide]

    def products(pairs):
        acc = None
        for lhs, w in pairs:
            d = jnp.dot(lhs, w, preferred_element_type=F32)
            acc = d if acc is None else acc + d
        return acc

    def conv_a(layer, i, k, carry):
        pairs = []
        for ky in TAPS:
            for ref, w in ((yas[k], wy), (sas[k], ws)):
                pairs.append((ref[ky:ky + height].reshape(height * half_w, wide), w[layer, ky]))
        acc = products(pairs)
        store_z(zas[layer % 2], i, acc, height)
        edges_a(layer + 1, i)
        return add_sums(acc, carry)

    def conv_down(i, k, carry):
        pairs = []
        for ky in TAPS:
            for part, ref in enumerate((yas[k], sas[k])):
                pairs.append((jnp.concatenate([ref[1 + 2 * r + ky] for r in range(low_h)], axis=0), wd[ky, part]))
        acc = products(pairs)
        store_z(zbs[0], i, acc, low_h)
        edges_b(4, i)
        return add_sums(acc, carry)

    def conv_b(layer, i, k, carry):
        pairs = []
        for ky in TAPS:
            for kx in TAPS:
                pairs.append((ybs[k][kx, ky:ky + low_h].reshape(low_h * half_w, wide), wb[layer, ky, kx]))
        acc = products(pairs)
        if layer == 0:
            store_z(zb1, i, acc, low_h)
            edges_b(5, i)
        else:
            zo[i] = acc.reshape(low_h, half_w, wide)
        return add_sums(acc, carry)

    def layer(e, prep, conv, in_sides, out_sides, early):
        wait_rows(e, in_sides, (0,))
        prep(0, 0)

        def pair(j, carry):
            i = 2 * j
            wait_rows(e, in_sides, (i + 1,))
            wait_rows(e, in_sides, (i + 2,), i + 2 < n_img)
            prep(i + 1, 1)
            carry = conv(i, 0, carry)
            prep(lax.min(i + 2, n_img - 1), 0)
            carry = conv(i + 1, 1, carry)
            send_rows(e + 1, out_sides, (i, i + 1), i < early)
            return carry

        s1, s2 = lax.fori_loop(0, n_img // 2, pair, zero_sums)
        s1, s2 = (jnp.sum(s, axis=0, keepdims=True) for s in (s1, s2))
        if e < 3:
            part = [s1[:, 0:chan] + s1[:, chan:], s2[:, 0:chan] + s2[:, chan:]]
        else:
            part = [s1[:, 0:chan], s1[:, chan:], s2[:, 0:chan], s2[:, chan:]]
        start_sums(e, jnp.concatenate(part, axis=0))
        if e < 5:
            both = len(out_sides) == 2
            start_cols(e + 1, SIDES if both else (0,), CORNERS if both else (0,))
            send_rows(e + 1, out_sides, range(early, n_img))

    send_rows(0, SIDES, range(n_img))
    start_cols(0)
    for copy in weight_copies:
        copy.wait()
    wait_cols(0)

    pos_a = n_dev * n_img * height * width
    pos_b = n_dev * n_img * low_h * half_w

    def params_a(e, layer):
        mean, inv = finish_sums(e, pos_a)
        return mean, inv, ga[layer, 0:1], ga[layer, 1:2]

    def params_b(e, ref):
        mean, inv = finish_sums(e, pos_b)
        gain = jnp.concatenate([ref[0:1, 0:chan], ref[0:1, chan:]], axis=0)
        shift = jnp.concatenate([ref[1:2, 0:chan], ref[1:2, chan:]], axis=0)
        return mean, inv, gain, shift

    part = functools.partial
    layer(0, prep_x, part(conv_a, 0), SIDES, SIDES, EARLY_A)

    wait_row_sends(0)
    wait_col_sends(0)
    wait_cols(1)
    layer(1, part(norm_a, 1, params_a(0, 0)), part(conv_a, 1), SIDES, SIDES, EARLY_A)

    wait_row_sends(1)
    wait_col_sends(1)
    wait_cols(2)
    layer(2, part(norm_a, 2, params_a(1, 1)), part(conv_a, 2), SIDES, (0,), EARLY_A)

    wait_row_sends(2)
    wait_col_sends(2)
    wait_cols(3, (1,), (3,))
    layer(3, part(norm_a, 3, params_a(2, 2), up=False), conv_down, (1,), SIDES, EARLY_B)

    wait_row_sends(3, (0,))
    wait_col_sends(3, (0,), (0,))
    wait_cols(4)
    layer(4, part(norm_b, 4, params_b(3, gd)), part(conv_b, 0), SIDES, SIDES, EARLY_B)

    wait_row_sends(4)
    wait_col_sends(4)
    wait_cols(5)
    layer(5, part(norm_b, 5, params_b(4, gb.at[0])), part(conv_b, 1), SIDES, (), 0)

    wait_row_sends(5)
    wait_col_sends(5)
    mean, inv = finish_sums(5, pos_b)
    for out, val in ((mean_o, mean), (inv_o, inv)):
        for h in SIDES:
            out[:, h * chan:(h + 1) * chan] = val[h:h + 1]
    gain_o[...] = gb[1, 0:1]
    shift_o[...] = gb[1, 1:2]

    for e in range(6):
        buf = sums_refs(e)
        rest = buf.at[pl.ds(0, n_dev - 1)]
        pltpu.make_async_copy(rest, rest, st_send.at[e]).wait()


def net(rows_n, cols_n, x, w_a, bn_a, w_down, bn_down, w_b, bn_b):
    n_img, height, width, chan = x.shape
    half_w, low_h = width // 2, height // 2
    n_dev = rows_n * cols_n
    vmem, dma = pltpu.VMEM, pltpu.SemaphoreType.DMA
    line, wide = 2 * half_w, 2 * chan
    plane = half_w + 2 * PAD
    a_sums, b_sums = 3, 3
    n_ex = a_sums + b_sums
    two, corners = len(SIDES), len(CORNERS)
    scratch = [
        vmem(x.shape, BF16),
        vmem((two, n_img, width, chan), BF16),
        *[vmem(((height + 2) * (width + 2 * PAD), chan), F32)] * two,
        *[vmem((n_img, height * line, chan), F32)] * two,
        *[vmem((n_img, low_h * line, chan), F32)] * two,
        vmem((a_sums, two, n_img, line, chan), F32),
        vmem((b_sums - 1, two, n_img, line, chan), F32),
        *[vmem(((height + 2) * 2 * plane, chan), F32)] * two,
        *[vmem(((low_h + 2) * 2 * plane, chan), F32)] * two,
        *[vmem((height + 2, half_w, wide), BF16)] * 4,
        *[vmem((3, low_h + 2, half_w, wide), BF16)] * two,
        *[vmem((n_ex, two, n_img, height, chan), F32)] * two,
        *[vmem((a_sums + 1, corners, n_img, 1, chan), F32)] * two,
        *[vmem((b_sums - 1, corners, n_img, 2, chan), F32)] * two,
        vmem((a_sums, n_dev, 2, chan), F32),
        vmem((b_sums, n_dev, 4, chan), F32),
        *[vmem((a_sums, 3, wide, wide), BF16)] * two,
        vmem((3, two, wide, wide), BF16),
        vmem(w_b.shape, BF16),
        vmem(bn_a.shape, F32),
        vmem(bn_down.shape, F32),
        vmem(bn_b.shape, F32),
        dma((n_img,)),
        dma((13,)),
        *[dma((n_ex, two, n_img))] * two,
        *[dma((n_ex, two))] * two,
        *[dma((n_ex, corners))] * two,
        *[dma((n_ex,))] * two,
    ]
    hbm_spec = pl.BlockSpec(memory_space=pltpu.HBM)
    line_out = jax.ShapeDtypeStruct((1, wide), F32)
    z, *vectors = pl.pallas_call(
        functools.partial(net_kernel, (rows_n, cols_n, n_img, height, width, chan)),
        out_shape=(jax.ShapeDtypeStruct((n_img, low_h, half_w, wide), F32),) + (line_out,) * 4,
        in_specs=[hbm_spec] * 7,
        out_specs=(pl.BlockSpec(memory_space=pltpu.VMEM),) * 5,
        scratch_shapes=scratch,
        compiler_params=pltpu.CompilerParams(collective_id=0, has_side_effects=True, vmem_limit_bytes=40 * 1024 * 1024),
        name="conv_bn_net",
    )(*[pltpu.with_memory_space_constraint(arg, pltpu.HBM) for arg in (x, w_a, bn_a, w_down, bn_down, w_b, bn_b)])
    mean, inv, gain, shift = [v.reshape(wide) for v in vectors]
    return jnp.maximum(gain * (z - mean) * inv + shift, 0.0).astype(BF16)


def solution(mesh):
    tile_spec = P("dp", "sp", "sp2", None)
    per_device = functools.partial(net, mesh.shape["sp"], mesh.shape["sp2"])
    return jax.shard_map(per_device, mesh=mesh, in_specs=(tile_spec, P(), P(), P(), P(), P(), P()), out_specs=tile_spec, check_vma=False)
```

```python
import functools

import jax
import jax.numpy as jnp
from jax import lax
from jax.experimental import pallas as pl
from jax.experimental.pallas import tpu as pltpu
from jax.sharding import PartitionSpec as P

MESH = pl.DeviceIdType.MESH
F32 = jnp.float32
BF16 = jnp.bfloat16
EPS = 1e-5
PAD = 8
SIDES = (0, 1)
CORNERS = (0, 1, 2, 3)
TAPS = range(3)
EARLY_A = 4
EARLY_B = 4
GROUP = 4


def net_kernel(dims, x, w_a, bn_a, w_down, bn_down, w_b, bn_b, zo, mean_o, inv_o, gain_o, shift_o,
               xin, xh, xf0, xf1, za0, za1, zb0, zb1, ha, hb, yfa0, yfa1, yfb0, yfb1, ya0, ya1, sa0, sa1, yb0, yb1,
               cs, cl, ksa, kla, ksb, klb, ta, tb, wy, ws, wd, wb, ga, gd, gb,
               in_sem, w_sem, row_recv, row_send, col_recv, col_send, cor_recv, cor_send, st_recv, st_send, meet):
    rows_n, cols_n, n_img, height, width, chan = dims
    n_dev = rows_n * cols_n
    half_w, low_h = width // 2, height // 2
    line, wide = 2 * half_w, 2 * chan
    xstride = width + 2 * PAD
    fstride = half_w + 2 * PAD
    xfs, zas, zbs, yfas, yfbs, yas, sas, ybs = (xf0, xf1), (za0, za1), (zb0, zb1), (yfa0, yfa1), (yfb0, yfb1), (ya0, ya1), (sa0, sa1), (yb0, yb1)
    sp = lax.axis_index("sp")
    sp2 = lax.axis_index("sp2")
    me = sp2 * rows_n + sp
    has_up = sp > 0
    has_down = sp < rows_n - 1
    has_left = sp2 > 0
    has_right = sp2 < cols_n - 1
    row_ok = (has_up, has_down)
    col_ok = (has_left, has_right)
    cor_ok = tuple(r & c for r in row_ok for c in col_ok)

    def device(d_sp, d_sp2):
        return {"sp": sp + d_sp, "sp2": sp2 + d_sp2}

    def ring(step):
        found = []
        for d_sp in (-step, 0, step):
            for d_sp2 in (-step, 0, step):
                if (d_sp or d_sp2) and abs(d_sp2) < cols_n and abs(d_sp) < rows_n:
                    ok = (sp + d_sp >= 0) & (sp + d_sp < rows_n) & (sp2 + d_sp2 >= 0) & (sp2 + d_sp2 < cols_n)
                    found.append((ok, device(d_sp, d_sp2)))
        return found

    def call(sem, step):
        for ok, where in ring(step):
            @pl.when(ok)
            def _():
                pl.semaphore_signal(sem, inc=1, device_id=where, device_id_type=MESH)

    def hear(sem, step):
        pl.semaphore_wait(sem, sum(ok.astype(jnp.int32) for ok, where in ring(step)))

    steps = [1]
    while 2 * steps[-1] < max(rows_n, cols_n) and len(steps) < meet.shape[0]:
        steps.append(2 * steps[-1])

    barrier = pltpu.get_barrier_semaphore()
    call(barrier, 1)

    chips = rows_n // 2
    chip, core = lax.div(sp, 2), lax.rem(sp, 2)
    lines = [[lax.rem(chip + d, chips) * 2 + c for c in (core, 1 - core)] for d in range(chips)]
    files = [lax.rem(sp2 + d, cols_n) for d in range(cols_n)]
    hops = {(dx, dy): min(dx, chips - dx) + min(dy, cols_n - dy) for dx in range(chips) for dy in range(cols_n)}
    others = [{"sp": lines[dx][flip], "sp2": files[dy]} for dx, dy in sorted(hops, key=lambda o: -hops[o]) for flip in (1, 0) if (dx, dy, flip) != (0, 0, 0)]

    for i in range(n_img):
        pltpu.make_async_copy(x.at[i], xin.at[i], in_sem.at[i]).start()
    weight_copies = []
    for kx, dst, k0, n0 in ((1, wy, 0, 0), (1, wy, chan, chan), (0, wy, 0, chan), (2, wy, chan, 0), (0, ws, 0, 0), (2, ws, chan, chan)):
        weight_copies.append((w_a.at[:, :, kx], dst.at[:, :, pl.ds(k0, chan), pl.ds(n0, chan)]))
    weight_copies.append((w_down.at[:, 0], wd.at[:, 0, pl.ds(0, chan), :]))
    weight_copies.append((w_down.at[:, 1], wd.at[:, 0, pl.ds(chan, chan), :]))
    weight_copies.append((w_down.at[:, 2], wd.at[:, 1, pl.ds(chan, chan), :]))
    weight_copies.append((w_b, wb))
    weight_copies.append((bn_a, ga))
    weight_copies.append((bn_down, gd))
    weight_copies.append((bn_b, gb))
    weight_copies = [pltpu.make_async_copy(s, d, w_sem.at[k]) for k, (s, d) in enumerate(weight_copies)]
    for copy in weight_copies:
        copy.start()

    zeros = jnp.zeros((chan, chan), BF16)
    for layer in TAPS:
        for ky in TAPS:
            ws[layer, ky, 0:chan, chan:wide] = zeros
            ws[layer, ky, chan:wide, 0:chan] = zeros
    for ky in TAPS:
        wd[ky, 1, 0:chan, :] = jnp.zeros((chan, wide), BF16)

    for i in range(n_img):
        pltpu.make_async_copy(x.at[i], xin.at[i], in_sem.at[i]).wait()
    for i in range(n_img):
        for side, col0, pick in ((0, 0, 0), (1, width - 16, 15)):
            blk = xin[i, :, col0:col0 + 16, :].astype(F32)
            at = side * height * 16
            za0[i, at:at + height * 16, :] = blk.reshape(height * 16, chan)
            edge = za0[i, pl.ds(at + pick, height, stride=16), :]
            cs[0, side, i] = edge
            ksa[0, side, i] = edge[0:1]
            ksa[0, 2 + side, i] = edge[height - 1:height]

    hear(barrier, 1)

    def cor_bufs(e):
        return (ksa.at[e], kla.at[e]) if e < 4 else (ksb.at[e - 4], klb.at[e - 4])

    def start_cols(e, sides=SIDES, corners=CORNERS):
        for side in sides:
            d = -1 if side == 0 else 1

            @pl.when(col_ok[side])
            def _():
                pltpu.make_async_remote_copy(cs.at[e, side], cl.at[e, 1 - side], col_send.at[e, side], col_recv.at[e, 1 - side],
                                             device_id=device(0, d), device_id_type=MESH).start()
        src, dst = cor_bufs(e)
        for corner in corners:
            d_sp = -1 if corner < 2 else 1
            d_sp2 = -1 if corner % 2 == 0 else 1

            @pl.when(cor_ok[corner])
            def _():
                pltpu.make_async_remote_copy(src.at[corner], dst.at[3 - corner], cor_send.at[e, corner], cor_recv.at[e, 3 - corner],
                                             device_id=device(d_sp, d_sp2), device_id_type=MESH).start()

    def wait_cols(e, sides=SIDES, corners=CORNERS):
        for side in sides:
            @pl.when(col_ok[side])
            def _():
                pltpu.make_async_copy(cl.at[e, side], cl.at[e, side], col_recv.at[e, side]).wait()
        src, dst = cor_bufs(e)
        for corner in corners:
            @pl.when(cor_ok[corner])
            def _():
                pltpu.make_async_copy(dst.at[corner], dst.at[corner], cor_recv.at[e, corner]).wait()

    def wait_col_sends(e, sides=SIDES, corners=CORNERS):
        for side in sides:
            @pl.when(col_ok[side])
            def _():
                pltpu.make_async_copy(cs.at[e, side], cs.at[e, side], col_send.at[e, side]).wait()
        src, dst = cor_bufs(e)
        for corner in corners:
            @pl.when(cor_ok[corner])
            def _():
                pltpu.make_async_copy(src.at[corner], src.at[corner], cor_send.at[e, corner]).wait()

    def row_landing(e, side):
        if e == 0:
            return xh.at[side]
        return ha.at[e - 1, side] if e < 4 else hb.at[e - 4, side]

    def row_source(e, side, i):
        if e == 0:
            return xin.at[i, 0 if side == 0 else height - 1]
        src, n_rows = (zas[(e - 1) % 2], height) if e < 4 else (zbs[e % 2], low_h)
        return src.at[i, pl.ds(0 if side == 0 else (n_rows - 1) * line, line)]

    def send_rows(e, sides, images, cond=True):
        for side in sides:
            @pl.when(row_ok[side] & cond)
            def _():
                for i in images:
                    pltpu.make_async_remote_copy(row_source(e, side, i), row_landing(e, 1 - side).at[i], row_send.at[e, side, i],
                                                 row_recv.at[e, 1 - side, i], device_id=device(-1 if side == 0 else 1, 0),
                                                 device_id_type=MESH).start()

    def wait_rows(e, sides, images, cond=True):
        for side in sides:
            @pl.when(row_ok[side] & cond)
            def _():
                for i in images:
                    ref = row_landing(e, side).at[i]
                    pltpu.make_async_copy(ref, ref, row_recv.at[e, side, i]).wait()

    def wait_row_sends(e, sides=SIDES):
        for side in sides:
            @pl.when(row_ok[side])
            def _():
                ref = row_landing(e, side)

                def one(i, carry):
                    pltpu.make_async_copy(ref.at[i], ref.at[i], row_send.at[e, side, i]).wait()
                    return carry

                lax.fori_loop(0, n_img, one, 0)

    def sums_refs(e):
        return ta.at[e] if e < 3 else tb.at[e - 3]

    def start_sums(e, part):
        buf = sums_refs(e)
        buf[me] = part

        for other in others:
            pltpu.make_async_remote_copy(buf.at[me], buf.at[me], st_send.at[e], st_recv.at[e], device_id=other, device_id_type=MESH).start()

    def finish_sums(e, num_pos):
        buf = sums_refs(e)
        rest = buf.at[pl.ds(0, n_dev - 1)]
        pltpu.make_async_copy(rest, rest, st_recv.at[e]).wait()
        total = jnp.sum(buf[...], axis=0) / num_pos
        lines = total.shape[0] // 2
        mean = total[0:lines]
        var = total[lines:] - mean * mean
        return mean, lax.rsqrt(var + EPS)

    def bn(z, par):
        mean, inv, gain, shift = par
        return jnp.maximum(gain * (z - mean) * inv + shift, 0.0)

    def keep(cond, val):
        return jnp.where(cond, val, 0.0)

    def prep_x(i, k):
        xf, ya, sa = xfs[k], yas[k], sas[k]
        last = height + 1
        for r in range(height):
            xf[pl.ds((r + 1) * xstride + PAD, width), :] = xin[i, r].astype(F32)
        xf[pl.ds(PAD, width), :] = keep(has_up, xh[0, i].astype(F32))
        xf[pl.ds(last * xstride + PAD, width), :] = keep(has_down, xh[1, i].astype(F32))
        xf[pl.ds(xstride + PAD - 1, height, stride=xstride), :] = keep(has_left, cl[0, 0, i])
        xf[pl.ds(xstride + PAD + width, height, stride=xstride), :] = keep(has_right, cl[0, 1, i])
        for corner in CORNERS:
            row = 0 if corner < 2 else last
            col = PAD - 1 if corner % 2 == 0 else PAD + width
            xf[row * xstride + col:row * xstride + col + 1, :] = keep(cor_ok[corner], kla[0, corner, i])
        for r in range(height + 2):
            base = r * xstride + PAD
            even = xf[pl.ds(base, half_w, stride=2), :]
            odd = xf[pl.ds(base + 1, half_w, stride=2), :]
            before = xf[pl.ds(base - 1, half_w, stride=2), :]
            after = xf[pl.ds(base + 2, half_w, stride=2), :]
            ya[r] = jnp.concatenate([even, odd], axis=1).astype(BF16)
            sa[r] = jnp.concatenate([before, after], axis=1).astype(BF16)

    def norm_a(e, par, i, k, up=True):
        za, yfa, ya, sa = zas[(e - 1) % 2], yfas[k], yas[k], sas[k]
        last = height + 1
        lo = 0 if up else 1
        for r in range(lo, height + 2):
            if r == 0:
                val = keep(has_up, bn(ha[e - 1, 0, i], par))
            elif r == last:
                val = keep(has_down, bn(ha[e - 1, 1, i], par))
            else:
                val = bn(za[i, pl.ds((r - 1) * line, line), :], par)
            base = r * 2 * fstride + PAD
            yfa[base:base + half_w, :] = val[0:half_w]
            yfa[base + fstride:base + fstride + half_w, :] = val[half_w:]
        if up:
            yfa[pl.ds(3 * fstride + PAD - 1, height, stride=2 * fstride), :] = keep(has_left, bn(cl[e, 0, i], par))
        yfa[pl.ds(2 * fstride + PAD + half_w, height, stride=2 * fstride), :] = keep(has_right, bn(cl[e, 1, i], par))
        for corner in CORNERS if up else (3,):
            row = 0 if corner < 2 else last
            at = row * 2 * fstride + (fstride + PAD - 1 if corner % 2 == 0 else PAD + half_w)
            yfa[at:at + 1, :] = keep(cor_ok[corner], bn(kla[e, corner, i], par))
        for r in range(lo, height + 2):
            base = r * 2 * fstride + PAD
            even = yfa[base:base + half_w, :]
            odd = yfa[base + fstride:base + fstride + half_w, :]
            before = yfa[base + fstride - 1:base + fstride - 1 + half_w, :]
            after = yfa[base + 1:base + 1 + half_w, :]
            ya[r] = jnp.concatenate([even, odd], axis=1).astype(BF16)
            sa[r] = jnp.concatenate([before, after], axis=1).astype(BF16)

    def norm_b(e, par, i, k):
        zb, yfb, yb = zbs[e % 2], yfbs[k], ybs[k]
        last = low_h + 1
        halves = [tuple(p[h:h + 1] for p in par) for h in SIDES]
        tall = tuple(jnp.concatenate([p] * low_h, axis=0) for p in par)
        for r in range(low_h + 2):
            for h in SIDES:
                if r == 0:
                    val = keep(has_up, bn(hb[e - 4, 0, i, pl.ds(h * half_w, half_w), :], halves[h]))
                elif r == last:
                    val = keep(has_down, bn(hb[e - 4, 1, i, pl.ds(h * half_w, half_w), :], halves[h]))
                else:
                    val = bn(zb[i, pl.ds(((r - 1) * 2 + h) * half_w, half_w), :], halves[h])
                base = (r * 2 + h) * fstride + PAD
                yfb[base:base + half_w, :] = val
        yfb[pl.ds(2 * fstride + PAD - 1, 2 * low_h, stride=fstride), :] = keep(has_left, bn(cl[e, 0, i], tall))
        yfb[pl.ds(2 * fstride + PAD + half_w, 2 * low_h, stride=fstride), :] = keep(has_right, bn(cl[e, 1, i], tall))
        for corner in CORNERS:
            row = 0 if corner < 2 else last
            val = keep(cor_ok[corner], bn(klb[e - 4, corner, i], par))
            for h in SIDES:
                at = (row * 2 + h) * fstride + (PAD - 1 if corner % 2 == 0 else PAD + half_w)
                yfb[at:at + 1, :] = val[h:h + 1]
        for r in range(low_h + 2):
            base = r * 2 * fstride + PAD
            for kx in TAPS:
                at = base + kx - 1
                yb[kx, r] = jnp.concatenate([yfb[at:at + half_w, :], yfb[at + fstride:at + fstride + half_w, :]], axis=1).astype(BF16)

    def add_sums(acc, carry):
        tiles = acc.reshape(acc.shape[0] // 8, 8, acc.shape[1])
        return carry[0] + jnp.sum(tiles, axis=0), carry[1] + jnp.sum(tiles * tiles, axis=0)

    zero_sums = (jnp.zeros((8, wide), F32), jnp.zeros((8, wide), F32))

    def edges_a(e, i):
        za = zas[(e - 1) % 2]
        first = za[i, pl.ds(0, height, stride=line), :]
        final = za[i, pl.ds(line - 1, height, stride=line), :]
        for side, edge in enumerate((first, final)):
            cs[e, side, i] = edge
            ksa[e, side, i] = edge[0:1]
            ksa[e, 2 + side, i] = edge[height - 1:height]

    def edges_b(e, i):
        zb = zbs[e % 2]
        first = zb[i, pl.ds(0, 2 * low_h, stride=half_w), :]
        final = zb[i, pl.ds(half_w - 1, 2 * low_h, stride=half_w), :]
        for side, edge in enumerate((first, final)):
            cs[e, side, i] = edge
            ksb[e - 4, side, i] = edge[0:2]
            ksb[e - 4, 2 + side, i] = edge[2 * low_h - 2:2 * low_h]

    def store_z(ref, i, acc, rows):
        for r in range(rows):
            at = r * line
            ref[i, at:at + half_w, :] = acc[r * half_w:(r + 1) * half_w, 0:chan]
            ref[i, at + half_w:at + line, :] = acc[r * half_w:(r + 1) * half_w, chan:wide]

    def products(pairs):
        acc = None
        for lhs, w in pairs:
            d = jnp.dot(lhs, w, preferred_element_type=F32)
            acc = d if acc is None else acc + d
        return acc

    def conv_a(layer, i, k, carry):
        pairs = []
        for ky in TAPS:
            for ref, w in ((yas[k], wy), (sas[k], ws)):
                pairs.append((ref[ky:ky + height].reshape(height * half_w, wide), w[layer, ky]))
        acc = products(pairs)
        store_z(zas[layer % 2], i, acc, height)
        edges_a(layer + 1, i)
        return add_sums(acc, carry)

    def conv_down(i, k, carry):
        pairs = []
        for ky in TAPS:
            for part, ref in enumerate((yas[k], sas[k])):
                pairs.append((jnp.concatenate([ref[1 + 2 * r + ky] for r in range(low_h)], axis=0), wd[ky, part]))
        acc = products(pairs)
        store_z(zbs[0], i, acc, low_h)
        edges_b(4, i)
        return add_sums(acc, carry)

    def conv_b(layer, i, k, carry):
        pairs = []
        for ky in TAPS:
            for kx in TAPS:
                pairs.append((ybs[k][kx, ky:ky + low_h].reshape(low_h * half_w, wide), wb[layer, ky, kx]))
        acc = products(pairs)
        if layer == 0:
            store_z(zb1, i, acc, low_h)
            edges_b(5, i)
        else:
            zo[i] = acc.reshape(low_h, half_w, wide)
        return add_sums(acc, carry)

    def layer(e, prep, conv, in_sides, out_sides, early):
        wait_rows(e, in_sides, (0,))
        prep(0, 0)

        def group(j, carry):
            i = GROUP * j
            wait_rows(e, in_sides, [i + u for u in range(1, GROUP)])
            wait_rows(e, in_sides, (i + GROUP,), i + GROUP < n_img)
            for u in range(GROUP):
                nxt = u + 1
                prep(i + nxt if nxt < GROUP else lax.min(i + nxt, n_img - 1), nxt % 2)
                carry = conv(i + u, u % 2, carry)
            send_rows(e + 1, out_sides, [i + u for u in range(GROUP)], i < early)
            return carry

        s1, s2 = lax.fori_loop(0, n_img // GROUP, group, zero_sums)
        s1, s2 = (jnp.sum(s, axis=0, keepdims=True) for s in (s1, s2))
        if e < 3:
            part = [s1[:, 0:chan] + s1[:, chan:], s2[:, 0:chan] + s2[:, chan:]]
        else:
            part = [s1[:, 0:chan], s1[:, chan:], s2[:, 0:chan], s2[:, chan:]]
        start_sums(e, jnp.concatenate(part, axis=0))
        if e < 5:
            both = len(out_sides) == 2
            start_cols(e + 1, SIDES if both else (0,), CORNERS if both else (0,))
            send_rows(e + 1, out_sides, range(early, n_img))

    call(meet.at[0], steps[0])
    start_cols(0)
    send_rows(0, SIDES, range(n_img))
    for copy in weight_copies[:6]:
        copy.wait()
    for k, step in enumerate(steps):
        hear(meet.at[k], step)
        if k + 1 < len(steps):
            call(meet.at[k + 1], steps[k + 1])
    wait_cols(0)

    pos_a = n_dev * n_img * height * width
    pos_b = n_dev * n_img * low_h * half_w

    def params_a(e, layer):
        mean, inv = finish_sums(e, pos_a)
        return mean, inv, ga[layer, 0:1], ga[layer, 1:2]

    def params_b(e, ref):
        mean, inv = finish_sums(e, pos_b)
        gain = jnp.concatenate([ref[0:1, 0:chan], ref[0:1, chan:]], axis=0)
        shift = jnp.concatenate([ref[1:2, 0:chan], ref[1:2, chan:]], axis=0)
        return mean, inv, gain, shift

    part = functools.partial
    layer(0, prep_x, part(conv_a, 0), SIDES, SIDES, EARLY_A)

    for copy in weight_copies[6:]:
        copy.wait()
    wait_row_sends(0)
    wait_col_sends(0)
    wait_cols(1)
    layer(1, part(norm_a, 1, params_a(0, 0)), part(conv_a, 1), SIDES, SIDES, EARLY_A)

    wait_row_sends(1)
    wait_col_sends(1)
    wait_cols(2)
    layer(2, part(norm_a, 2, params_a(1, 1)), part(conv_a, 2), SIDES, (0,), EARLY_A)

    wait_row_sends(2)
    wait_col_sends(2)
    wait_cols(3, (1,), (3,))
    layer(3, part(norm_a, 3, params_a(2, 2), up=False), conv_down, (1,), SIDES, EARLY_B)

    wait_row_sends(3, (0,))
    wait_col_sends(3, (0,), (0,))
    wait_cols(4)
    layer(4, part(norm_b, 4, params_b(3, gd)), part(conv_b, 0), SIDES, SIDES, EARLY_B)

    wait_row_sends(4)
    wait_col_sends(4)
    wait_cols(5)
    layer(5, part(norm_b, 5, params_b(4, gb.at[0])), part(conv_b, 1), SIDES, (), 0)

    wait_row_sends(5)
    wait_col_sends(5)
    mean, inv = finish_sums(5, pos_b)
    for out, val in ((mean_o, mean), (inv_o, inv)):
        for h in SIDES:
            out[:, h * chan:(h + 1) * chan] = val[h:h + 1]
    gain_o[...] = gb[1, 0:1]
    shift_o[...] = gb[1, 1:2]

    for e in range(6):
        buf = sums_refs(e)
        rest = buf.at[pl.ds(0, n_dev - 1)]
        pltpu.make_async_copy(rest, rest, st_send.at[e]).wait()


def net(rows_n, cols_n, x, w_a, bn_a, w_down, bn_down, w_b, bn_b):
    n_img, height, width, chan = x.shape
    half_w, low_h = width // 2, height // 2
    n_dev = rows_n * cols_n
    vmem, dma = pltpu.VMEM, pltpu.SemaphoreType.DMA
    line, wide = 2 * half_w, 2 * chan
    plane = half_w + 2 * PAD
    a_sums, b_sums = 3, 3
    n_ex = a_sums + b_sums
    two, corners = len(SIDES), len(CORNERS)
    scratch = [
        vmem(x.shape, BF16),
        vmem((two, n_img, width, chan), BF16),
        *[vmem(((height + 2) * (width + 2 * PAD), chan), F32)] * two,
        *[vmem((n_img, height * line, chan), F32)] * two,
        *[vmem((n_img, low_h * line, chan), F32)] * two,
        vmem((a_sums, two, n_img, line, chan), F32),
        vmem((b_sums - 1, two, n_img, line, chan), F32),
        *[vmem(((height + 2) * 2 * plane, chan), F32)] * two,
        *[vmem(((low_h + 2) * 2 * plane, chan), F32)] * two,
        *[vmem((height + 2, half_w, wide), BF16)] * 4,
        *[vmem((3, low_h + 2, half_w, wide), BF16)] * two,
        *[vmem((n_ex, two, n_img, height, chan), F32)] * two,
        *[vmem((a_sums + 1, corners, n_img, 1, chan), F32)] * two,
        *[vmem((b_sums - 1, corners, n_img, 2, chan), F32)] * two,
        vmem((a_sums, n_dev, 2, chan), F32),
        vmem((b_sums, n_dev, 4, chan), F32),
        *[vmem((a_sums, 3, wide, wide), BF16)] * two,
        vmem((3, two, wide, wide), BF16),
        vmem(w_b.shape, BF16),
        vmem(bn_a.shape, F32),
        vmem(bn_down.shape, F32),
        vmem(bn_b.shape, F32),
        dma((n_img,)),
        dma((13,)),
        *[dma((n_ex, two, n_img))] * two,
        *[dma((n_ex, two))] * two,
        *[dma((n_ex, corners))] * two,
        *[dma((n_ex,))] * two,
        pltpu.SemaphoreType.REGULAR((3,)),
    ]
    hbm_spec = pl.BlockSpec(memory_space=pltpu.HBM)
    line_out = jax.ShapeDtypeStruct((1, wide), F32)
    z, *vectors = pl.pallas_call(
        functools.partial(net_kernel, (rows_n, cols_n, n_img, height, width, chan)),
        out_shape=(jax.ShapeDtypeStruct((n_img, low_h, half_w, wide), F32),) + (line_out,) * 4,
        in_specs=[hbm_spec] * 7,
        out_specs=(pl.BlockSpec(memory_space=pltpu.VMEM),) * 5,
        scratch_shapes=scratch,
        compiler_params=pltpu.CompilerParams(collective_id=0, has_side_effects=True, vmem_limit_bytes=40 * 1024 * 1024),
        name="conv_bn_net",
    )(*[pltpu.with_memory_space_constraint(arg, pltpu.HBM) for arg in (x, w_a, bn_a, w_down, bn_down, w_b, bn_b)])
    mean, inv, gain, shift = [v.reshape(wide) for v in vectors]
    return jnp.maximum(gain * (z - mean) * inv + shift, 0.0).astype(BF16)


def solution(mesh):
    tile_spec = P("dp", "sp", "sp2", None)
    per_device = functools.partial(net, mesh.shape["sp"], mesh.shape["sp2"])
    return jax.shard_map(per_device, mesh=mesh, in_specs=(tile_spec, P(), P(), P(), P(), P(), P()), out_specs=tile_spec, check_vma=False)
```

```python
import functools

import jax
import jax.numpy as jnp
from jax import lax
from jax.experimental import pallas as pl
from jax.experimental.pallas import tpu as pltpu
from jax.sharding import PartitionSpec as P

MESH = pl.DeviceIdType.MESH
F32 = jnp.float32
BF16 = jnp.bfloat16
EPS = 1e-5
PAD = 8
SIDES = (0, 1)
CORNERS = (0, 1, 2, 3)
TAPS = range(3)
EARLY_A = 4
EARLY_B = 2
GROUP = 2


def net_kernel(dims, x, w_a, bn_a, w_down, bn_down, w_b, bn_b, zo, mean_o, inv_o, gain_o, shift_o,
               xin, xh, xf0, xf1, za0, za1, zb0, zb1, ha, hb, yfa0, yfa1, yfb0, yfb1, ya0, ya1, sa0, sa1, yb0, yb1,
               cs, cl, ksa, kla, ksb, klb, ta, tb, wy, ws, wd, wb, ga, gd, gb,
               in_sem, w_sem, row_recv, row_send, col_recv, col_send, cor_recv, cor_send, st_recv, st_send, meet):
    rows_n, cols_n, n_img, height, width, chan = dims
    n_dev = rows_n * cols_n
    half_w, low_h = width // 2, height // 2
    line, wide = 2 * half_w, 2 * chan
    xstride = width + 2 * PAD
    fstride = half_w + 2 * PAD
    xfs, zas, zbs, yfas, yfbs, yas, sas, ybs = (xf0, xf1), (za0, za1), (zb0, zb1), (yfa0, yfa1), (yfb0, yfb1), (ya0, ya1), (sa0, sa1), (yb0, yb1)
    sp = lax.axis_index("sp")
    sp2 = lax.axis_index("sp2")
    me = sp2 * rows_n + sp
    has_up = sp > 0
    has_down = sp < rows_n - 1
    has_left = sp2 > 0
    has_right = sp2 < cols_n - 1
    row_ok = (has_up, has_down)
    col_ok = (has_left, has_right)
    cor_ok = tuple(r & c for r in row_ok for c in col_ok)

    def device(d_sp, d_sp2):
        return {"sp": sp + d_sp, "sp2": sp2 + d_sp2}

    def ring(step):
        found = []
        for d_sp in (-step, 0, step):
            for d_sp2 in (-step, 0, step):
                if (d_sp or d_sp2) and abs(d_sp2) < cols_n and abs(d_sp) < rows_n:
                    ok = (sp + d_sp >= 0) & (sp + d_sp < rows_n) & (sp2 + d_sp2 >= 0) & (sp2 + d_sp2 < cols_n)
                    found.append((ok, device(d_sp, d_sp2)))
        return found

    def call(sem, step):
        for ok, where in ring(step):
            @pl.when(ok)
            def _():
                pl.semaphore_signal(sem, inc=1, device_id=where, device_id_type=MESH)

    def hear(sem, step):
        pl.semaphore_wait(sem, sum(ok.astype(jnp.int32) for ok, where in ring(step)))

    steps = [1]
    while 2 * steps[-1] < max(rows_n, cols_n) and len(steps) < meet.shape[0]:
        steps.append(2 * steps[-1])

    barrier = pltpu.get_barrier_semaphore()
    call(barrier, 1)

    chips = rows_n // 2
    chip, core = lax.div(sp, 2), lax.rem(sp, 2)
    lines = [[lax.rem(chip + d, chips) * 2 + c for c in (core, 1 - core)] for d in range(chips)]
    files = [lax.rem(sp2 + d, cols_n) for d in range(cols_n)]
    hops = {(dx, dy): min(dx, chips - dx) + min(dy, cols_n - dy) for dx in range(chips) for dy in range(cols_n)}
    others = [{"sp": lines[dx][flip], "sp2": files[dy]} for dx, dy in sorted(hops, key=lambda o: -hops[o]) for flip in (1, 0) if (dx, dy, flip) != (0, 0, 0)]

    for i in range(n_img):
        pltpu.make_async_copy(x.at[i], xin.at[i], in_sem.at[i]).start()
    weight_copies = []
    for kx, dst, k0, n0 in ((1, wy, 0, 0), (1, wy, chan, chan), (0, wy, 0, chan), (2, wy, chan, 0), (0, ws, 0, 0), (2, ws, chan, chan)):
        weight_copies.append((w_a.at[:, :, kx], dst.at[:, :, pl.ds(k0, chan), pl.ds(n0, chan)]))
    weight_copies.append((w_down.at[:, 0], wd.at[:, 0, pl.ds(0, chan), :]))
    weight_copies.append((w_down.at[:, 1], wd.at[:, 0, pl.ds(chan, chan), :]))
    weight_copies.append((w_down.at[:, 2], wd.at[:, 1, pl.ds(chan, chan), :]))
    weight_copies.append((w_b, wb))
    weight_copies.append((bn_a, ga))
    weight_copies.append((bn_down, gd))
    weight_copies.append((bn_b, gb))
    weight_copies = [pltpu.make_async_copy(s, d, w_sem.at[k]) for k, (s, d) in enumerate(weight_copies)]
    for copy in weight_copies:
        copy.start()

    zeros = jnp.zeros((chan, chan), BF16)
    for layer in TAPS:
        for ky in TAPS:
            ws[layer, ky, 0:chan, chan:wide] = zeros
            ws[layer, ky, chan:wide, 0:chan] = zeros
    for ky in TAPS:
        wd[ky, 1, 0:chan, :] = jnp.zeros((chan, wide), BF16)

    for i in range(n_img):
        pltpu.make_async_copy(x.at[i], xin.at[i], in_sem.at[i]).wait()
    for i in range(n_img):
        for side, col0, pick in ((0, 0, 0), (1, width - 16, 15)):
            blk = xin[i, :, col0:col0 + 16, :].astype(F32)
            at = side * height * 16
            za0[i, at:at + height * 16, :] = blk.reshape(height * 16, chan)
            edge = za0[i, pl.ds(at + pick, height, stride=16), :]
            cs[0, side, i] = edge
            ksa[0, side, i] = edge[0:1]
            ksa[0, 2 + side, i] = edge[height - 1:height]

    hear(barrier, 1)

    def cor_bufs(e):
        return (ksa.at[e], kla.at[e]) if e < 4 else (ksb.at[e - 4], klb.at[e - 4])

    def start_cols(e, sides=SIDES, corners=CORNERS):
        for side in sides:
            d = -1 if side == 0 else 1

            @pl.when(col_ok[side])
            def _():
                pltpu.make_async_remote_copy(cs.at[e, side], cl.at[e, 1 - side], col_send.at[e, side], col_recv.at[e, 1 - side],
                                             device_id=device(0, d), device_id_type=MESH).start()
        src, dst = cor_bufs(e)
        for corner in corners:
            d_sp = -1 if corner < 2 else 1
            d_sp2 = -1 if corner % 2 == 0 else 1

            @pl.when(cor_ok[corner])
            def _():
                pltpu.make_async_remote_copy(src.at[corner], dst.at[3 - corner], cor_send.at[e, corner], cor_recv.at[e, 3 - corner],
                                             device_id=device(d_sp, d_sp2), device_id_type=MESH).start()

    def wait_cols(e, sides=SIDES, corners=CORNERS):
        for side in sides:
            @pl.when(col_ok[side])
            def _():
                pltpu.make_async_copy(cl.at[e, side], cl.at[e, side], col_recv.at[e, side]).wait()
        src, dst = cor_bufs(e)
        for corner in corners:
            @pl.when(cor_ok[corner])
            def _():
                pltpu.make_async_copy(dst.at[corner], dst.at[corner], cor_recv.at[e, corner]).wait()

    def wait_col_sends(e, sides=SIDES, corners=CORNERS):
        for side in sides:
            @pl.when(col_ok[side])
            def _():
                pltpu.make_async_copy(cs.at[e, side], cs.at[e, side], col_send.at[e, side]).wait()
        src, dst = cor_bufs(e)
        for corner in corners:
            @pl.when(cor_ok[corner])
            def _():
                pltpu.make_async_copy(src.at[corner], src.at[corner], cor_send.at[e, corner]).wait()

    def row_landing(e, side):
        if e == 0:
            return xh.at[side]
        return ha.at[e - 1, side] if e < 4 else hb.at[e - 4, side]

    def row_source(e, side, i):
        if e == 0:
            return xin.at[i, 0 if side == 0 else height - 1]
        src, n_rows = (zas[(e - 1) % 2], height) if e < 4 else (zbs[e % 2], low_h)
        return src.at[i, pl.ds(0 if side == 0 else (n_rows - 1) * line, line)]

    def send_rows(e, sides, images, cond=True):
        for side in sides:
            @pl.when(row_ok[side] & cond)
            def _():
                for i in images:
                    pltpu.make_async_remote_copy(row_source(e, side, i), row_landing(e, 1 - side).at[i], row_send.at[e, side, i],
                                                 row_recv.at[e, 1 - side, i], device_id=device(-1 if side == 0 else 1, 0),
                                                 device_id_type=MESH).start()

    def wait_rows(e, sides, images, cond=True):
        for side in sides:
            @pl.when(row_ok[side] & cond)
            def _():
                for i in images:
                    ref = row_landing(e, side).at[i]
                    pltpu.make_async_copy(ref, ref, row_recv.at[e, side, i]).wait()

    def wait_row_sends(e, sides=SIDES):
        for side in sides:
            @pl.when(row_ok[side])
            def _():
                ref = row_landing(e, side)

                def one(i, carry):
                    pltpu.make_async_copy(ref.at[i], ref.at[i], row_send.at[e, side, i]).wait()
                    return carry

                lax.fori_loop(0, n_img, one, 0)

    def sums_refs(e):
        return ta.at[e] if e < 3 else tb.at[e - 3]

    def start_sums(e, part):
        buf = sums_refs(e)
        buf[me] = part

        for other in others:
            pltpu.make_async_remote_copy(buf.at[me], buf.at[me], st_send.at[e], st_recv.at[e], device_id=other, device_id_type=MESH).start()

    def finish_sums(e, num_pos):
        buf = sums_refs(e)
        rest = buf.at[pl.ds(0, n_dev - 1)]
        pltpu.make_async_copy(rest, rest, st_recv.at[e]).wait()
        total = jnp.sum(buf[...], axis=0) / num_pos
        lines = total.shape[0] // 2
        mean = total[0:lines]
        var = total[lines:] - mean * mean
        return mean, lax.rsqrt(var + EPS)

    def bn(z, par):
        mean, inv, gain, shift = par
        return jnp.maximum(gain * (z - mean) * inv + shift, 0.0)

    def keep(cond, val):
        return jnp.where(cond, val, 0.0)

    def prep_x(i, k):
        xf, ya, sa = xfs[k], yas[k], sas[k]
        last = height + 1
        for r in range(height):
            xf[pl.ds((r + 1) * xstride + PAD, width), :] = xin[i, r].astype(F32)
        xf[pl.ds(PAD, width), :] = keep(has_up, xh[0, i].astype(F32))
        xf[pl.ds(last * xstride + PAD, width), :] = keep(has_down, xh[1, i].astype(F32))
        xf[pl.ds(xstride + PAD - 1, height, stride=xstride), :] = keep(has_left, cl[0, 0, i])
        xf[pl.ds(xstride + PAD + width, height, stride=xstride), :] = keep(has_right, cl[0, 1, i])
        for corner in CORNERS:
            row = 0 if corner < 2 else last
            col = PAD - 1 if corner % 2 == 0 else PAD + width
            xf[row * xstride + col:row * xstride + col + 1, :] = keep(cor_ok[corner], kla[0, corner, i])
        for r in range(height + 2):
            base = r * xstride + PAD
            even = xf[pl.ds(base, half_w, stride=2), :]
            odd = xf[pl.ds(base + 1, half_w, stride=2), :]
            before = xf[pl.ds(base - 1, half_w, stride=2), :]
            after = xf[pl.ds(base + 2, half_w, stride=2), :]
            ya[r] = jnp.concatenate([even, odd], axis=1).astype(BF16)
            sa[r] = jnp.concatenate([before, after], axis=1).astype(BF16)

    def norm_a(e, par, i, k, up=True):
        za, yfa, ya, sa = zas[(e - 1) % 2], yfas[k], yas[k], sas[k]
        last = height + 1
        lo = 0 if up else 1
        for r in range(lo, height + 2):
            if r == 0:
                val = keep(has_up, bn(ha[e - 1, 0, i], par))
            elif r == last:
                val = keep(has_down, bn(ha[e - 1, 1, i], par))
            else:
                val = bn(za[i, pl.ds((r - 1) * line, line), :], par)
            base = r * 2 * fstride + PAD
            yfa[base:base + half_w, :] = val[0:half_w]
            yfa[base + fstride:base + fstride + half_w, :] = val[half_w:]
        if up:
            yfa[pl.ds(3 * fstride + PAD - 1, height, stride=2 * fstride), :] = keep(has_left, bn(cl[e, 0, i], par))
        yfa[pl.ds(2 * fstride + PAD + half_w, height, stride=2 * fstride), :] = keep(has_right, bn(cl[e, 1, i], par))
        for corner in CORNERS if up else (3,):
            row = 0 if corner < 2 else last
            at = row * 2 * fstride + (fstride + PAD - 1 if corner % 2 == 0 else PAD + half_w)
            yfa[at:at + 1, :] = keep(cor_ok[corner], bn(kla[e, corner, i], par))
        for r in range(lo, height + 2):
            base = r * 2 * fstride + PAD
            even = yfa[base:base + half_w, :]
            odd = yfa[base + fstride:base + fstride + half_w, :]
            before = yfa[base + fstride - 1:base + fstride - 1 + half_w, :]
            after = yfa[base + 1:base + 1 + half_w, :]
            ya[r] = jnp.concatenate([even, odd], axis=1).astype(BF16)
            sa[r] = jnp.concatenate([before, after], axis=1).astype(BF16)

    def norm_b(e, par, i, k):
        zb, yfb, yb = zbs[e % 2], yfbs[k], ybs[k]
        last = low_h + 1
        halves = [tuple(p[h:h + 1] for p in par) for h in SIDES]
        tall = tuple(jnp.concatenate([p] * low_h, axis=0) for p in par)
        for r in range(low_h + 2):
            for h in SIDES:
                if r == 0:
                    val = keep(has_up, bn(hb[e - 4, 0, i, pl.ds(h * half_w, half_w), :], halves[h]))
                elif r == last:
                    val = keep(has_down, bn(hb[e - 4, 1, i, pl.ds(h * half_w, half_w), :], halves[h]))
                else:
                    val = bn(zb[i, pl.ds(((r - 1) * 2 + h) * half_w, half_w), :], halves[h])
                base = (r * 2 + h) * fstride + PAD
                yfb[base:base + half_w, :] = val
        yfb[pl.ds(2 * fstride + PAD - 1, 2 * low_h, stride=fstride), :] = keep(has_left, bn(cl[e, 0, i], tall))
        yfb[pl.ds(2 * fstride + PAD + half_w, 2 * low_h, stride=fstride), :] = keep(has_right, bn(cl[e, 1, i], tall))
        for corner in CORNERS:
            row = 0 if corner < 2 else last
            val = keep(cor_ok[corner], bn(klb[e - 4, corner, i], par))
            for h in SIDES:
                at = (row * 2 + h) * fstride + (PAD - 1 if corner % 2 == 0 else PAD + half_w)
                yfb[at:at + 1, :] = val[h:h + 1]
        for r in range(low_h + 2):
            base = r * 2 * fstride + PAD
            for kx in TAPS:
                at = base + kx - 1
                yb[kx, r] = jnp.concatenate([yfb[at:at + half_w, :], yfb[at + fstride:at + fstride + half_w, :]], axis=1).astype(BF16)

    def add_sums(acc, carry):
        tiles = acc.reshape(acc.shape[0] // 8, 8, acc.shape[1])
        return carry[0] + jnp.sum(tiles, axis=0), carry[1] + jnp.sum(tiles * tiles, axis=0)

    zero_sums = (jnp.zeros((8, wide), F32), jnp.zeros((8, wide), F32))

    def edges_a(e, i):
        za = zas[(e - 1) % 2]
        first = za[i, pl.ds(0, height, stride=line), :]
        final = za[i, pl.ds(line - 1, height, stride=line), :]
        for side, edge in enumerate((first, final)):
            cs[e, side, i] = edge
            ksa[e, side, i] = edge[0:1]
            ksa[e, 2 + side, i] = edge[height - 1:height]

    def edges_b(e, i):
        zb = zbs[e % 2]
        first = zb[i, pl.ds(0, 2 * low_h, stride=half_w), :]
        final = zb[i, pl.ds(half_w - 1, 2 * low_h, stride=half_w), :]
        for side, edge in enumerate((first, final)):
            cs[e, side, i] = edge
            ksb[e - 4, side, i] = edge[0:2]
            ksb[e - 4, 2 + side, i] = edge[2 * low_h - 2:2 * low_h]

    def store_z(ref, i, acc, rows):
        for r in range(rows):
            at = r * line
            ref[i, at:at + half_w, :] = acc[r * half_w:(r + 1) * half_w, 0:chan]
            ref[i, at + half_w:at + line, :] = acc[r * half_w:(r + 1) * half_w, chan:wide]

    def products(pairs):
        acc = None
        for lhs, w in pairs:
            d = jnp.dot(lhs, w, preferred_element_type=F32)
            acc = d if acc is None else acc + d
        return acc

    def conv_a(layer, i, k, carry):
        pairs = []
        for ky in TAPS:
            for ref, w in ((yas[k], wy), (sas[k], ws)):
                pairs.append((ref[ky:ky + height].reshape(height * half_w, wide), w[layer, ky]))
        acc = products(pairs)
        store_z(zas[layer % 2], i, acc, height)
        edges_a(layer + 1, i)
        return add_sums(acc, carry)

    def conv_down(i, k, carry):
        pairs = []
        for ky in TAPS:
            for part, ref in enumerate((yas[k], sas[k])):
                pairs.append((jnp.concatenate([ref[1 + 2 * r + ky] for r in range(low_h)], axis=0), wd[ky, part]))
        acc = products(pairs)
        store_z(zbs[0], i, acc, low_h)
        edges_b(4, i)
        return add_sums(acc, carry)

    def conv_b(layer, i, k, carry):
        pairs = []
        for ky in TAPS:
            for kx in TAPS:
                pairs.append((ybs[k][kx, ky:ky + low_h].reshape(low_h * half_w, wide), wb[layer, ky, kx]))
        acc = products(pairs)
        if layer == 0:
            store_z(zb1, i, acc, low_h)
            edges_b(5, i)
        else:
            zo[i] = acc.reshape(low_h, half_w, wide)
        return add_sums(acc, carry)

    def layer(e, prep, conv, in_sides, out_sides, early):
        wait_rows(e, in_sides, (0,))
        prep(0, 0)

        def group(j, carry):
            i = GROUP * j
            wait_rows(e, in_sides, [i + u for u in range(1, GROUP)])
            wait_rows(e, in_sides, (i + GROUP,), i + GROUP < n_img)
            for u in range(GROUP):
                nxt = u + 1
                prep(i + nxt if nxt < GROUP else lax.min(i + nxt, n_img - 1), nxt % 2)
                carry = conv(i + u, u % 2, carry)
            send_rows(e + 1, out_sides, [i + u for u in range(GROUP)], i < early)
            return carry

        s1, s2 = lax.fori_loop(0, n_img // GROUP, group, zero_sums)
        s1, s2 = (jnp.sum(s, axis=0, keepdims=True) for s in (s1, s2))
        if e < 3:
            part = [s1[:, 0:chan] + s1[:, chan:], s2[:, 0:chan] + s2[:, chan:]]
        else:
            part = [s1[:, 0:chan], s1[:, chan:], s2[:, 0:chan], s2[:, chan:]]
        start_sums(e, jnp.concatenate(part, axis=0))
        if e < 5:
            both = len(out_sides) == 2
            start_cols(e + 1, SIDES if both else (0,), CORNERS if both else (0,))
            send_rows(e + 1, out_sides, range(early, n_img))

    call(meet.at[0], steps[0])
    start_cols(0)
    send_rows(0, SIDES, range(n_img))
    for copy in weight_copies[:6]:
        copy.wait()
    for k, step in enumerate(steps):
        hear(meet.at[k], step)
        if k + 1 < len(steps):
            call(meet.at[k + 1], steps[k + 1])
    wait_cols(0)

    pos_a = n_dev * n_img * height * width
    pos_b = n_dev * n_img * low_h * half_w

    def params_a(e, layer):
        mean, inv = finish_sums(e, pos_a)
        return mean, inv, ga[layer, 0:1], ga[layer, 1:2]

    def params_b(e, ref):
        mean, inv = finish_sums(e, pos_b)
        gain = jnp.concatenate([ref[0:1, 0:chan], ref[0:1, chan:]], axis=0)
        shift = jnp.concatenate([ref[1:2, 0:chan], ref[1:2, chan:]], axis=0)
        return mean, inv, gain, shift

    part = functools.partial
    layer(0, prep_x, part(conv_a, 0), SIDES, SIDES, EARLY_A)

    for copy in weight_copies[6:]:
        copy.wait()
    wait_row_sends(0)
    wait_col_sends(0)
    wait_cols(1)
    layer(1, part(norm_a, 1, params_a(0, 0)), part(conv_a, 1), SIDES, SIDES, EARLY_A)

    wait_row_sends(1)
    wait_col_sends(1)
    wait_cols(2)
    layer(2, part(norm_a, 2, params_a(1, 1)), part(conv_a, 2), SIDES, (0,), EARLY_A)

    wait_row_sends(2)
    wait_col_sends(2)
    wait_cols(3, (1,), (3,))
    layer(3, part(norm_a, 3, params_a(2, 2), up=False), conv_down, (1,), SIDES, EARLY_B)

    wait_row_sends(3, (0,))
    wait_col_sends(3, (0,), (0,))
    wait_cols(4)
    layer(4, part(norm_b, 4, params_b(3, gd)), part(conv_b, 0), SIDES, SIDES, EARLY_B)

    wait_row_sends(4)
    wait_col_sends(4)
    wait_cols(5)
    layer(5, part(norm_b, 5, params_b(4, gb.at[0])), part(conv_b, 1), SIDES, (), 0)

    wait_row_sends(5)
    wait_col_sends(5)
    mean, inv = finish_sums(5, pos_b)
    for out, val in ((mean_o, mean), (inv_o, inv)):
        for h in SIDES:
            out[:, h * chan:(h + 1) * chan] = val[h:h + 1]
    gain_o[...] = gb[1, 0:1]
    shift_o[...] = gb[1, 1:2]

    for e in range(6):
        buf = sums_refs(e)
        rest = buf.at[pl.ds(0, n_dev - 1)]
        pltpu.make_async_copy(rest, rest, st_send.at[e]).wait()


def net(rows_n, cols_n, x, w_a, bn_a, w_down, bn_down, w_b, bn_b):
    n_img, height, width, chan = x.shape
    half_w, low_h = width // 2, height // 2
    n_dev = rows_n * cols_n
    vmem, dma = pltpu.VMEM, pltpu.SemaphoreType.DMA
    line, wide = 2 * half_w, 2 * chan
    plane = half_w + 2 * PAD
    a_sums, b_sums = 3, 3
    n_ex = a_sums + b_sums
    two, corners = len(SIDES), len(CORNERS)
    scratch = [
        vmem(x.shape, BF16),
        vmem((two, n_img, width, chan), BF16),
        *[vmem(((height + 2) * (width + 2 * PAD), chan), F32)] * two,
        *[vmem((n_img, height * line, chan), F32)] * two,
        *[vmem((n_img, low_h * line, chan), F32)] * two,
        vmem((a_sums, two, n_img, line, chan), F32),
        vmem((b_sums - 1, two, n_img, line, chan), F32),
        *[vmem(((height + 2) * 2 * plane, chan), F32)] * two,
        *[vmem(((low_h + 2) * 2 * plane, chan), F32)] * two,
        *[vmem((height + 2, half_w, wide), BF16)] * 4,
        *[vmem((3, low_h + 2, half_w, wide), BF16)] * two,
        *[vmem((n_ex, two, n_img, height, chan), F32)] * two,
        *[vmem((a_sums + 1, corners, n_img, 1, chan), F32)] * two,
        *[vmem((b_sums - 1, corners, n_img, 2, chan), F32)] * two,
        vmem((a_sums, n_dev, 2, chan), F32),
        vmem((b_sums, n_dev, 4, chan), F32),
        *[vmem((a_sums, 3, wide, wide), BF16)] * two,
        vmem((3, two, wide, wide), BF16),
        vmem(w_b.shape, BF16),
        vmem(bn_a.shape, F32),
        vmem(bn_down.shape, F32),
        vmem(bn_b.shape, F32),
        dma((n_img,)),
        dma((13,)),
        *[dma((n_ex, two, n_img))] * two,
        *[dma((n_ex, two))] * two,
        *[dma((n_ex, corners))] * two,
        *[dma((n_ex,))] * two,
        pltpu.SemaphoreType.REGULAR((3,)),
    ]
    hbm_spec = pl.BlockSpec(memory_space=pltpu.HBM)
    line_out = jax.ShapeDtypeStruct((1, wide), F32)
    z, *vectors = pl.pallas_call(
        functools.partial(net_kernel, (rows_n, cols_n, n_img, height, width, chan)),
        out_shape=(jax.ShapeDtypeStruct((n_img, low_h, half_w, wide), F32),) + (line_out,) * 4,
        in_specs=[hbm_spec] * 7,
        out_specs=(pl.BlockSpec(memory_space=pltpu.VMEM),) * 5,
        scratch_shapes=scratch,
        compiler_params=pltpu.CompilerParams(collective_id=0, has_side_effects=True, vmem_limit_bytes=40 * 1024 * 1024),
        name="conv_bn_net",
    )(*[pltpu.with_memory_space_constraint(arg, pltpu.HBM) for arg in (x, w_a, bn_a, w_down, bn_down, w_b, bn_b)])
    mean, inv, gain, shift = [v.reshape(wide) for v in vectors]
    return jnp.maximum(gain * (z - mean) * inv + shift, 0.0).astype(BF16)


def solution(mesh):
    tile_spec = P("dp", "sp", "sp2", None)
    per_device = functools.partial(net, mesh.shape["sp"], mesh.shape["sp2"])
    return jax.shard_map(per_device, mesh=mesh, in_specs=(tile_spec, P(), P(), P(), P(), P(), P()), out_specs=tile_spec, check_vma=False)
```

```python
import functools

import jax
import jax.numpy as jnp
from jax import lax
from jax.experimental import pallas as pl
from jax.experimental.pallas import tpu as pltpu
from jax.sharding import PartitionSpec as P

MESH = pl.DeviceIdType.MESH
F32 = jnp.float32
BF16 = jnp.bfloat16
EPS = 1e-5
PAD = 8
SIDES = (0, 1)
CORNERS = (0, 1, 2, 3)
TAPS = range(3)
EARLY_A = 4
EARLY_B = 2


def net_kernel(dims, x, w_a, bn_a, w_down, bn_down, w_b, bn_b, zo, mean_o, inv_o, gain_o, shift_o,
               xin, xh, xf0, xf1, za0, za1, zb0, zb1, ha, hb, yfa0, yfa1, yfb0, yfb1, ya0, ya1, sa0, sa1, yb0, yb1,
               cs, cl, ksa, kla, ksb, klb, ta, tb, wy, ws, wd, wb, ga, gd, gb,
               in_sem, w_sem, row_recv, row_send, col_recv, col_send, cor_recv, cor_send, st_recv, st_send, meet):
    rows_n, cols_n, n_img, height, width, chan = dims
    n_dev = rows_n * cols_n
    half_w, low_h = width // 2, height // 2
    line, wide = 2 * half_w, 2 * chan
    xstride = width + 2 * PAD
    fstride = half_w + 2 * PAD
    xfs, zas, zbs, yfas, yfbs, yas, sas, ybs = (xf0, xf1), (za0, za1), (zb0, zb1), (yfa0, yfa1), (yfb0, yfb1), (ya0, ya1), (sa0, sa1), (yb0, yb1)
    sp = lax.axis_index("sp")
    sp2 = lax.axis_index("sp2")
    me = sp2 * rows_n + sp
    has_up = sp > 0
    has_down = sp < rows_n - 1
    has_left = sp2 > 0
    has_right = sp2 < cols_n - 1
    row_ok = (has_up, has_down)
    col_ok = (has_left, has_right)
    cor_ok = tuple(r & c for r in row_ok for c in col_ok)

    def device(d_sp, d_sp2):
        return {"sp": sp + d_sp, "sp2": sp2 + d_sp2}

    def ring(step):
        found = []
        for d_sp in (-step, 0, step):
            for d_sp2 in (-step, 0, step):
                if (d_sp or d_sp2) and abs(d_sp2) < cols_n and abs(d_sp) < rows_n:
                    ok = (sp + d_sp >= 0) & (sp + d_sp < rows_n) & (sp2 + d_sp2 >= 0) & (sp2 + d_sp2 < cols_n)
                    found.append((ok, device(d_sp, d_sp2)))
        return found

    def call(sem, step):
        for ok, where in ring(step):
            @pl.when(ok)
            def _():
                pl.semaphore_signal(sem, inc=1, device_id=where, device_id_type=MESH)

    def hear(sem, step):
        pl.semaphore_wait(sem, sum(ok.astype(jnp.int32) for ok, where in ring(step)))

    steps = [1]
    while 2 * steps[-1] < max(rows_n, cols_n) and len(steps) < meet.shape[0]:
        steps.append(2 * steps[-1])

    def meet_again(k):
        if k < len(steps):
            hear(meet.at[k], steps[k])
        if k + 1 < len(steps):
            call(meet.at[k + 1], steps[k + 1])

    barrier = pltpu.get_barrier_semaphore()
    call(barrier, 1)

    chips = rows_n // 2
    chip, core = lax.div(sp, 2), lax.rem(sp, 2)
    others = []
    for d in sorted(range(chips), key=lambda d: -min(d, chips - d)):
        at = lax.rem(chip + d, chips) * 2
        others.append((at + 1 - core, at + core))

    for i in range(n_img):
        pltpu.make_async_copy(x.at[i], xin.at[i], in_sem.at[i]).start()
    weight_copies = []
    for kx, dst, k0, n0 in ((1, wy, 0, 0), (1, wy, chan, chan), (0, wy, 0, chan), (2, wy, chan, 0), (0, ws, 0, 0), (2, ws, chan, chan)):
        weight_copies.append((w_a.at[:, :, kx], dst.at[:, :, pl.ds(k0, chan), pl.ds(n0, chan)]))
    weight_copies.append((w_down.at[:, 0], wd.at[:, 0, pl.ds(0, chan), :]))
    weight_copies.append((w_down.at[:, 1], wd.at[:, 0, pl.ds(chan, chan), :]))
    weight_copies.append((w_down.at[:, 2], wd.at[:, 1, pl.ds(chan, chan), :]))
    weight_copies.append((w_b, wb))
    weight_copies.append((bn_a, ga))
    weight_copies.append((bn_down, gd))
    weight_copies.append((bn_b, gb))
    weight_copies = [pltpu.make_async_copy(s, d, w_sem.at[k]) for k, (s, d) in enumerate(weight_copies)]
    for copy in weight_copies:
        copy.start()

    zeros = jnp.zeros((chan, chan), BF16)
    for layer in TAPS:
        for ky in TAPS:
            ws[layer, ky, 0:chan, chan:wide] = zeros
            ws[layer, ky, chan:wide, 0:chan] = zeros
    for ky in TAPS:
        wd[ky, 1, 0:chan, :] = jnp.zeros((chan, wide), BF16)

    for i in range(n_img):
        pltpu.make_async_copy(x.at[i], xin.at[i], in_sem.at[i]).wait()
    for i in range(n_img):
        for side, col0, pick in ((0, 0, 0), (1, width - 16, 15)):
            blk = xin[i, :, col0:col0 + 16, :].astype(F32)
            at = side * height * 16
            za0[i, at:at + height * 16, :] = blk.reshape(height * 16, chan)
            edge = za0[i, pl.ds(at + pick, height, stride=16), :]
            cs[0, side, i] = edge
            ksa[0, side, i] = edge[0:1]
            ksa[0, 2 + side, i] = edge[height - 1:height]

    hear(barrier, 1)

    def cor_bufs(e):
        return (ksa.at[e], kla.at[e]) if e < 4 else (ksb.at[e - 4], klb.at[e - 4])

    def start_cols(e, sides=SIDES, corners=CORNERS):
        for side in sides:
            d = -1 if side == 0 else 1

            @pl.when(col_ok[side])
            def _():
                pltpu.make_async_remote_copy(cs.at[e, side], cl.at[e, 1 - side], col_send.at[e, side], col_recv.at[e, 1 - side],
                                             device_id=device(0, d), device_id_type=MESH).start()
        src, dst = cor_bufs(e)
        for corner in corners:
            d_sp = -1 if corner < 2 else 1
            d_sp2 = -1 if corner % 2 == 0 else 1

            @pl.when(cor_ok[corner])
            def _():
                pltpu.make_async_remote_copy(src.at[corner], dst.at[3 - corner], cor_send.at[e, corner], cor_recv.at[e, 3 - corner],
                                             device_id=device(d_sp, d_sp2), device_id_type=MESH).start()

    def wait_cols(e, sides=SIDES, corners=CORNERS):
        for side in sides:
            @pl.when(col_ok[side])
            def _():
                pltpu.make_async_copy(cl.at[e, side], cl.at[e, side], col_recv.at[e, side]).wait()
        src, dst = cor_bufs(e)
        for corner in corners:
            @pl.when(cor_ok[corner])
            def _():
                pltpu.make_async_copy(dst.at[corner], dst.at[corner], cor_recv.at[e, corner]).wait()

    def wait_col_sends(e, sides=SIDES, corners=CORNERS):
        for side in sides:
            @pl.when(col_ok[side])
            def _():
                pltpu.make_async_copy(cs.at[e, side], cs.at[e, side], col_send.at[e, side]).wait()
        src, dst = cor_bufs(e)
        for corner in corners:
            @pl.when(cor_ok[corner])
            def _():
                pltpu.make_async_copy(src.at[corner], src.at[corner], cor_send.at[e, corner]).wait()

    def row_landing(e, side):
        if e == 0:
            return xh.at[side]
        return ha.at[e - 1, side] if e < 4 else hb.at[e - 4, side]

    def row_source(e, side, i):
        if e == 0:
            return xin.at[i, 0 if side == 0 else height - 1]
        src, n_rows = (zas[(e - 1) % 2], height) if e < 4 else (zbs[e % 2], low_h)
        return src.at[i, pl.ds(0 if side == 0 else (n_rows - 1) * line, line)]

    def send_rows(e, sides, images, cond=True):
        for side in sides:
            @pl.when(row_ok[side] & cond)
            def _():
                for i in images:
                    pltpu.make_async_remote_copy(row_source(e, side, i), row_landing(e, 1 - side).at[i], row_send.at[e, side, i],
                                                 row_recv.at[e, 1 - side, i], device_id=device(-1 if side == 0 else 1, 0),
                                                 device_id_type=MESH).start()

    def wait_rows(e, sides, images, cond=True):
        for side in sides:
            @pl.when(row_ok[side] & cond)
            def _():
                for i in images:
                    ref = row_landing(e, side).at[i]
                    pltpu.make_async_copy(ref, ref, row_recv.at[e, side, i]).wait()

    def wait_row_sends(e, sides=SIDES):
        for side in sides:
            @pl.when(row_ok[side])
            def _():
                ref = row_landing(e, side)

                def one(i, carry):
                    pltpu.make_async_copy(ref.at[i], ref.at[i], row_send.at[e, side, i]).wait()
                    return carry

                lax.fori_loop(0, n_img, one, 0)

    def sums_refs(e):
        return ta.at[e] if e < 3 else tb.at[e - 3]

    def start_sums(e, part):
        buf = sums_refs(e)
        buf[me] = part

        def send(to_sp, to_sp2):
            pltpu.make_async_remote_copy(buf.at[me], buf.at[me], st_send.at[e], st_recv.at[e], device_id={"sp": to_sp, "sp2": to_sp2},
                                         device_id_type=MESH).start()

        for k, pair in enumerate(others):
            def send_file(t, carry, pair=pair):
                to_sp2 = lax.rem(sp2 + cols_n // 2 + lax.select(lax.rem(t, 2) == 0, lax.div(t + 1, 2), -lax.div(t + 1, 2)), cols_n)
                for to_sp in pair:
                    send(to_sp, to_sp2)
                return carry

            lax.fori_loop(0, cols_n if k + 1 < len(others) else cols_n - 1, send_file, 0)
        send(others[-1][0], sp2)

    def finish_sums(e, num_pos):
        buf = sums_refs(e)
        rest = buf.at[pl.ds(0, n_dev - 1)]
        pltpu.make_async_copy(rest, rest, st_recv.at[e]).wait()
        total = jnp.sum(buf[...], axis=0) / num_pos
        lines = total.shape[0] // 2
        mean = total[0:lines]
        var = total[lines:] - mean * mean
        return mean, lax.rsqrt(var + EPS)

    def bn(z, par):
        mean, inv, gain, shift = par
        return jnp.maximum(gain * (z - mean) * inv + shift, 0.0)

    def keep(cond, val):
        return jnp.where(cond, val, 0.0)

    def prep_x(i, k):
        xf, ya, sa = xfs[k], yas[k], sas[k]
        last = height + 1
        for r in range(height):
            xf[pl.ds((r + 1) * xstride + PAD, width), :] = xin[i, r].astype(F32)
        xf[pl.ds(PAD, width), :] = keep(has_up, xh[0, i].astype(F32))
        xf[pl.ds(last * xstride + PAD, width), :] = keep(has_down, xh[1, i].astype(F32))
        xf[pl.ds(xstride + PAD - 1, height, stride=xstride), :] = keep(has_left, cl[0, 0, i])
        xf[pl.ds(xstride + PAD + width, height, stride=xstride), :] = keep(has_right, cl[0, 1, i])
        for corner in CORNERS:
            row = 0 if corner < 2 else last
            col = PAD - 1 if corner % 2 == 0 else PAD + width
            xf[row * xstride + col:row * xstride + col + 1, :] = keep(cor_ok[corner], kla[0, corner, i])
        for r in range(height + 2):
            base = r * xstride + PAD
            even = xf[pl.ds(base, half_w, stride=2), :]
            odd = xf[pl.ds(base + 1, half_w, stride=2), :]
            before = xf[pl.ds(base - 1, half_w, stride=2), :]
            after = xf[pl.ds(base + 2, half_w, stride=2), :]
            ya[r] = jnp.concatenate([even, odd], axis=1).astype(BF16)
            sa[r] = jnp.concatenate([before, after], axis=1).astype(BF16)

    def norm_a(e, par, i, k, up=True):
        za, yfa, ya, sa = zas[(e - 1) % 2], yfas[k], yas[k], sas[k]
        last = height + 1
        lo = 0 if up else 1
        for r in range(lo, height + 2):
            if r == 0:
                val = keep(has_up, bn(ha[e - 1, 0, i], par))
            elif r == last:
                val = keep(has_down, bn(ha[e - 1, 1, i], par))
            else:
                val = bn(za[i, pl.ds((r - 1) * line, line), :], par)
            base = r * 2 * fstride + PAD
            yfa[base:base + half_w, :] = val[0:half_w]
            yfa[base + fstride:base + fstride + half_w, :] = val[half_w:]
        if up:
            yfa[pl.ds(3 * fstride + PAD - 1, height, stride=2 * fstride), :] = keep(has_left, bn(cl[e, 0, i], par))
        yfa[pl.ds(2 * fstride + PAD + half_w, height, stride=2 * fstride), :] = keep(has_right, bn(cl[e, 1, i], par))
        for corner in CORNERS if up else (3,):
            row = 0 if corner < 2 else last
            at = row * 2 * fstride + (fstride + PAD - 1 if corner % 2 == 0 else PAD + half_w)
            yfa[at:at + 1, :] = keep(cor_ok[corner], bn(kla[e, corner, i], par))
        for r in range(lo, height + 2):
            base = r * 2 * fstride + PAD
            even = yfa[base:base + half_w, :]
            odd = yfa[base + fstride:base + fstride + half_w, :]
            before = yfa[base + fstride - 1:base + fstride - 1 + half_w, :]
            after = yfa[base + 1:base + 1 + half_w, :]
            ya[r] = jnp.concatenate([even, odd], axis=1).astype(BF16)
            sa[r] = jnp.concatenate([before, after], axis=1).astype(BF16)

    def norm_b(e, par, i, k):
        zb, yfb, yb = zbs[e % 2], yfbs[k], ybs[k]
        last = low_h + 1
        halves = [tuple(p[h:h + 1] for p in par) for h in SIDES]
        tall = tuple(jnp.concatenate([p] * low_h, axis=0) for p in par)
        for r in range(low_h + 2):
            for h in SIDES:
                if r == 0:
                    val = keep(has_up, bn(hb[e - 4, 0, i, pl.ds(h * half_w, half_w), :], halves[h]))
                elif r == last:
                    val = keep(has_down, bn(hb[e - 4, 1, i, pl.ds(h * half_w, half_w), :], halves[h]))
                else:
                    val = bn(zb[i, pl.ds(((r - 1) * 2 + h) * half_w, half_w), :], halves[h])
                base = (r * 2 + h) * fstride + PAD
                yfb[base:base + half_w, :] = val
        yfb[pl.ds(2 * fstride + PAD - 1, 2 * low_h, stride=fstride), :] = keep(has_left, bn(cl[e, 0, i], tall))
        yfb[pl.ds(2 * fstride + PAD + half_w, 2 * low_h, stride=fstride), :] = keep(has_right, bn(cl[e, 1, i], tall))
        for corner in CORNERS:
            row = 0 if corner < 2 else last
            val = keep(cor_ok[corner], bn(klb[e - 4, corner, i], par))
            for h in SIDES:
                at = (row * 2 + h) * fstride + (PAD - 1 if corner % 2 == 0 else PAD + half_w)
                yfb[at:at + 1, :] = val[h:h + 1]
        for r in range(low_h + 2):
            base = r * 2 * fstride + PAD
            for kx in TAPS:
                at = base + kx - 1
                yb[kx, r] = jnp.concatenate([yfb[at:at + half_w, :], yfb[at + fstride:at + fstride + half_w, :]], axis=1).astype(BF16)

    def add_sums(acc, carry):
        tiles = acc.reshape(acc.shape[0] // 8, 8, acc.shape[1])
        return carry[0] + jnp.sum(tiles, axis=0), carry[1] + jnp.sum(tiles * tiles, axis=0)

    zero_sums = (jnp.zeros((8, wide), F32), jnp.zeros((8, wide), F32))

    def edges_a(e, i):
        za = zas[(e - 1) % 2]
        first = za[i, pl.ds(0, height, stride=line), :]
        final = za[i, pl.ds(line - 1, height, stride=line), :]
        for side, edge in enumerate((first, final)):
            cs[e, side, i] = edge
            ksa[e, side, i] = edge[0:1]
            ksa[e, 2 + side, i] = edge[height - 1:height]

    def edges_b(e, i):
        zb = zbs[e % 2]
        first = zb[i, pl.ds(0, 2 * low_h, stride=half_w), :]
        final = zb[i, pl.ds(half_w - 1, 2 * low_h, stride=half_w), :]
        for side, edge in enumerate((first, final)):
            cs[e, side, i] = edge
            ksb[e - 4, side, i] = edge[0:2]
            ksb[e - 4, 2 + side, i] = edge[2 * low_h - 2:2 * low_h]

    def store_z(ref, i, acc, rows):
        for r in range(rows):
            at = r * line
            ref[i, at:at + half_w, :] = acc[r * half_w:(r + 1) * half_w, 0:chan]
            ref[i, at + half_w:at + line, :] = acc[r * half_w:(r + 1) * half_w, chan:wide]

    def products(pairs):
        acc = None
        for lhs, w in pairs:
            d = jnp.dot(lhs, w, preferred_element_type=F32)
            acc = d if acc is None else acc + d
        return acc

    def conv_a(layer, i, k, carry):
        pairs = []
        for ky in TAPS:
            for ref, w in ((yas[k], wy), (sas[k], ws)):
                pairs.append((ref[ky:ky + height].reshape(height * half_w, wide), w[layer, ky]))
        acc = products(pairs)
        store_z(zas[layer % 2], i, acc, height)
        edges_a(layer + 1, i)
        return add_sums(acc, carry)

    def conv_down(i, k, carry):
        pairs = []
        for ky in TAPS:
            for part, ref in enumerate((yas[k], sas[k])):
                pairs.append((jnp.concatenate([ref[1 + 2 * r + ky] for r in range(low_h)], axis=0), wd[ky, part]))
        acc = products(pairs)
        store_z(zbs[0], i, acc, low_h)
        edges_b(4, i)
        return add_sums(acc, carry)

    def conv_b(layer, i, k, carry):
        pairs = []
        for ky in TAPS:
            for kx in TAPS:
                pairs.append((ybs[k][kx, ky:ky + low_h].reshape(low_h * half_w, wide), wb[layer, ky, kx]))
        acc = products(pairs)
        if layer == 0:
            store_z(zb1, i, acc, low_h)
            edges_b(5, i)
        else:
            zo[i] = acc.reshape(low_h, half_w, wide)
        return add_sums(acc, carry)

    def layer(e, prep, conv, in_sides, out_sides, early):
        wait_rows(e, in_sides, (0,))
        prep(0, 0)

        half = n_img // 2

        def pair(j, carry):
            i = 2 * j
            wait_rows(e, in_sides, (i + 1, i + 2))
            for u in SIDES:
                prep(i + u + 1, 1 - u)
                carry = conv(i + u, u, carry)
            send_rows(e + 1, out_sides, (i, i + 1), i < early)
            return carry

        carry = lax.fori_loop(0, half // 2, pair, zero_sums)
        wait_rows(e, in_sides, range(half + 1, n_img))
        if e == 0:
            meet_again(1)
        for i in range(half, n_img):
            if i + 1 < n_img:
                prep(i + 1, (i + 1) % 2)
            carry = conv(i, i % 2, carry)
        s1, s2 = carry
        s1, s2 = (jnp.sum(s, axis=0, keepdims=True) for s in (s1, s2))
        if e < 3:
            part = [s1[:, 0:chan] + s1[:, chan:], s2[:, 0:chan] + s2[:, chan:]]
        else:
            part = [s1[:, 0:chan], s1[:, chan:], s2[:, 0:chan], s2[:, chan:]]
        if e == 0:
            for k in range(2, len(steps)):
                meet_again(k)
        start_sums(e, jnp.concatenate(part, axis=0))
        if e < 5:
            both = len(out_sides) == 2
            start_cols(e + 1, SIDES if both else (0,), CORNERS if both else (0,))
            send_rows(e + 1, out_sides, range(early, n_img))

    call(meet.at[0], steps[0])
    start_cols(0)
    send_rows(0, SIDES, range(n_img))
    for copy in weight_copies[:6]:
        copy.wait()
    meet_again(0)
    wait_cols(0)

    pos_a = n_dev * n_img * height * width
    pos_b = n_dev * n_img * low_h * half_w

    def params_a(e, layer):
        mean, inv = finish_sums(e, pos_a)
        return mean, inv, ga[layer, 0:1], ga[layer, 1:2]

    def params_b(e, ref):
        mean, inv = finish_sums(e, pos_b)
        gain = jnp.concatenate([ref[0:1, 0:chan], ref[0:1, chan:]], axis=0)
        shift = jnp.concatenate([ref[1:2, 0:chan], ref[1:2, chan:]], axis=0)
        return mean, inv, gain, shift

    part = functools.partial
    layer(0, prep_x, part(conv_a, 0), SIDES, SIDES, EARLY_A)

    for copy in weight_copies[6:]:
        copy.wait()
    wait_row_sends(0)
    wait_col_sends(0)
    wait_cols(1)
    layer(1, part(norm_a, 1, params_a(0, 0)), part(conv_a, 1), SIDES, SIDES, EARLY_A)

    wait_row_sends(1)
    wait_col_sends(1)
    wait_cols(2)
    layer(2, part(norm_a, 2, params_a(1, 1)), part(conv_a, 2), SIDES, (0,), EARLY_A)

    wait_row_sends(2)
    wait_col_sends(2)
    wait_cols(3, (1,), (3,))
    layer(3, part(norm_a, 3, params_a(2, 2), up=False), conv_down, (1,), SIDES, EARLY_B)

    wait_row_sends(3, (0,))
    wait_col_sends(3, (0,), (0,))
    wait_cols(4)
    layer(4, part(norm_b, 4, params_b(3, gd)), part(conv_b, 0), SIDES, SIDES, EARLY_B)

    wait_row_sends(4)
    wait_col_sends(4)
    wait_cols(5)
    layer(5, part(norm_b, 5, params_b(4, gb.at[0])), part(conv_b, 1), SIDES, (), 0)

    wait_row_sends(5)
    wait_col_sends(5)
    mean, inv = finish_sums(5, pos_b)
    for out, val in ((mean_o, mean), (inv_o, inv)):
        for h in SIDES:
            out[:, h * chan:(h + 1) * chan] = val[h:h + 1]
    gain_o[...] = gb[1, 0:1]
    shift_o[...] = gb[1, 1:2]

    for e in range(6):
        buf = sums_refs(e)
        rest = buf.at[pl.ds(0, n_dev - 1)]
        pltpu.make_async_copy(rest, rest, st_send.at[e]).wait()


def net(rows_n, cols_n, x, w_a, bn_a, w_down, bn_down, w_b, bn_b):
    n_img, height, width, chan = x.shape
    half_w, low_h = width // 2, height // 2
    n_dev = rows_n * cols_n
    vmem, dma = pltpu.VMEM, pltpu.SemaphoreType.DMA
    line, wide = 2 * half_w, 2 * chan
    plane = half_w + 2 * PAD
    a_sums, b_sums = 3, 3
    n_ex = a_sums + b_sums
    two, corners = len(SIDES), len(CORNERS)
    scratch = [
        vmem(x.shape, BF16),
        vmem((two, n_img, width, chan), BF16),
        *[vmem(((height + 2) * (width + 2 * PAD), chan), F32)] * two,
        *[vmem((n_img, height * line, chan), F32)] * two,
        *[vmem((n_img, low_h * line, chan), F32)] * two,
        vmem((a_sums, two, n_img, line, chan), F32),
        vmem((b_sums - 1, two, n_img, line, chan), F32),
        *[vmem(((height + 2) * 2 * plane, chan), F32)] * two,
        *[vmem(((low_h + 2) * 2 * plane, chan), F32)] * two,
        *[vmem((height + 2, half_w, wide), BF16)] * 4,
        *[vmem((3, low_h + 2, half_w, wide), BF16)] * two,
        *[vmem((n_ex, two, n_img, height, chan), F32)] * two,
        *[vmem((a_sums + 1, corners, n_img, 1, chan), F32)] * two,
        *[vmem((b_sums - 1, corners, n_img, 2, chan), F32)] * two,
        vmem((a_sums, n_dev, 2, chan), F32),
        vmem((b_sums, n_dev, 4, chan), F32),
        *[vmem((a_sums, 3, wide, wide), BF16)] * two,
        vmem((3, two, wide, wide), BF16),
        vmem(w_b.shape, BF16),
        vmem(bn_a.shape, F32),
        vmem(bn_down.shape, F32),
        vmem(bn_b.shape, F32),
        dma((n_img,)),
        dma((13,)),
        *[dma((n_ex, two, n_img))] * two,
        *[dma((n_ex, two))] * two,
        *[dma((n_ex, corners))] * two,
        *[dma((n_ex,))] * two,
        pltpu.SemaphoreType.REGULAR((3,)),
    ]
    hbm_spec = pl.BlockSpec(memory_space=pltpu.HBM)
    line_out = jax.ShapeDtypeStruct((1, wide), F32)
    z, *vectors = pl.pallas_call(
        functools.partial(net_kernel, (rows_n, cols_n, n_img, height, width, chan)),
        out_shape=(jax.ShapeDtypeStruct((n_img, low_h, half_w, wide), F32),) + (line_out,) * 4,
        in_specs=[hbm_spec] * 7,
        out_specs=(pl.BlockSpec(memory_space=pltpu.VMEM),) * 5,
        scratch_shapes=scratch,
        compiler_params=pltpu.CompilerParams(collective_id=0, has_side_effects=True, vmem_limit_bytes=40 * 1024 * 1024),
        name="conv_bn_net",
    )(*[pltpu.with_memory_space_constraint(arg, pltpu.HBM) for arg in (x, w_a, bn_a, w_down, bn_down, w_b, bn_b)])
    mean, inv, gain, shift = [v.reshape(wide) for v in vectors]
    return jnp.maximum(gain * (z - mean) * inv + shift, 0.0).astype(BF16)


def solution(mesh):
    tile_spec = P("dp", "sp", "sp2", None)
    per_device = functools.partial(net, mesh.shape["sp"], mesh.shape["sp2"])
    return jax.shard_map(per_device, mesh=mesh, in_specs=(tile_spec, P(), P(), P(), P(), P(), P()), out_specs=tile_spec, check_vma=False)
```

```python
import functools

import jax
import jax.numpy as jnp
from jax import lax
from jax.experimental import pallas as pl
from jax.experimental.pallas import tpu as pltpu
from jax.sharding import PartitionSpec as P

MESH = pl.DeviceIdType.MESH
F32 = jnp.float32
BF16 = jnp.bfloat16
EPS = 1e-5
PAD = 8
SIDES = (0, 1)
CORNERS = (0, 1, 2, 3)
TAPS = range(3)
EARLY_A = 2
EARLY_B = 2


def net_kernel(dims, x, w_a, bn_a, w_down, bn_down, w_b, bn_b, zo, mean_o, inv_o, gain_o, shift_o,
               xin, xh, xf0, xf1, za0, za1, zb0, zb1, ha, hb, yfa0, yfa1, yfb0, yfb1, ya0, ya1, sa0, sa1, yb0, yb1,
               cs, cl, ksa, kla, ksb, klb, ta, tb, wy, ws, wd, wb, ga, gd, gb,
               in_sem, w_sem, row_recv, row_send, col_recv, col_send, cor_recv, cor_send, st_recv, st_send, meet):
    rows_n, cols_n, n_img, height, width, chan = dims
    n_dev = rows_n * cols_n
    half_w, low_h = width // 2, height // 2
    line, wide = 2 * half_w, 2 * chan
    xstride = width + 2 * PAD
    fstride = half_w + 2 * PAD
    xfs, zas, zbs, yfas, yfbs, yas, sas, ybs = (xf0, xf1), (za0, za1), (zb0, zb1), (yfa0, yfa1), (yfb0, yfb1), (ya0, ya1), (sa0, sa1), (yb0, yb1)
    sp = lax.axis_index("sp")
    sp2 = lax.axis_index("sp2")
    me = sp2 * rows_n + sp
    has_up = sp > 0
    has_down = sp < rows_n - 1
    has_left = sp2 > 0
    has_right = sp2 < cols_n - 1
    row_ok = (has_up, has_down)
    col_ok = (has_left, has_right)
    cor_ok = tuple(r & c for r in row_ok for c in col_ok)

    def device(d_sp, d_sp2):
        return {"sp": sp + d_sp, "sp2": sp2 + d_sp2}

    def ring(step):
        found = []
        for d_sp in (-step, 0, step):
            for d_sp2 in (-step, 0, step):
                if (d_sp or d_sp2) and abs(d_sp2) < cols_n and abs(d_sp) < rows_n:
                    ok = (sp + d_sp >= 0) & (sp + d_sp < rows_n) & (sp2 + d_sp2 >= 0) & (sp2 + d_sp2 < cols_n)
                    found.append((ok, device(d_sp, d_sp2)))
        return found

    def call(sem, step):
        for ok, where in ring(step):
            @pl.when(ok)
            def _():
                pl.semaphore_signal(sem, inc=1, device_id=where, device_id_type=MESH)

    def hear(sem, step):
        pl.semaphore_wait(sem, sum(ok.astype(jnp.int32) for ok, where in ring(step)))

    steps = [1]
    while 2 * steps[-1] < max(rows_n, cols_n) and len(steps) < meet.shape[0]:
        steps.append(2 * steps[-1])

    def meet_again(k):
        if k < len(steps):
            hear(meet.at[k], steps[k])
        if k + 1 < len(steps):
            call(meet.at[k + 1], steps[k + 1])

    chips = rows_n // 2
    chip, core = lax.div(sp, 2), lax.rem(sp, 2)
    others = []
    for d in sorted(range(chips), key=lambda d: -min(d, chips - d)):
        at = lax.rem(chip + d, chips) * 2
        others.append((at + 1 - core, at + core))

    for i in range(n_img):
        pltpu.make_async_copy(x.at[i], xin.at[i], in_sem.at[i]).start()
    weight_copies = []
    for kx, dst, k0, n0 in ((1, wy, 0, 0), (1, wy, chan, chan), (0, wy, 0, chan), (2, wy, chan, 0), (0, ws, 0, 0), (2, ws, chan, chan)):
        weight_copies.append((w_a.at[:, :, kx], dst.at[:, :, pl.ds(k0, chan), pl.ds(n0, chan)]))
    weight_copies.append((w_down.at[:, 0], wd.at[:, 0, pl.ds(0, chan), :]))
    weight_copies.append((w_down.at[:, 1], wd.at[:, 0, pl.ds(chan, chan), :]))
    weight_copies.append((w_down.at[:, 2], wd.at[:, 1, pl.ds(chan, chan), :]))
    weight_copies.append((w_b, wb))
    weight_copies.append((bn_a, ga))
    weight_copies.append((bn_down, gd))
    weight_copies.append((bn_b, gb))
    weight_copies = [pltpu.make_async_copy(s, d, w_sem.at[k]) for k, (s, d) in enumerate(weight_copies)]
    for copy in weight_copies:
        copy.start()

    barrier = pltpu.get_barrier_semaphore()
    call(barrier, 1)

    for i in range(n_img):
        pltpu.make_async_copy(x.at[i], xin.at[i], in_sem.at[i]).wait()
    for i in range(n_img):
        for side, col0, pick in ((0, 0, 0), (1, width - 16, 15)):
            blk = xin[i, :, col0:col0 + 16, :].astype(F32)
            at = side * height * 16
            za0[i, at:at + height * 16, :] = blk.reshape(height * 16, chan)
            edge = za0[i, pl.ds(at + pick, height, stride=16), :]
            cs[0, side, i] = edge
            ksa[0, side, i] = edge[0:1]
            ksa[0, 2 + side, i] = edge[height - 1:height]

    hear(barrier, 1)

    def cor_bufs(e):
        return (ksa.at[e], kla.at[e]) if e < 4 else (ksb.at[e - 4], klb.at[e - 4])

    def start_cols(e, sides=SIDES, corners=CORNERS):
        for side in sides:
            d = -1 if side == 0 else 1

            @pl.when(col_ok[side])
            def _():
                pltpu.make_async_remote_copy(cs.at[e, side], cl.at[e, 1 - side], col_send.at[e, side], col_recv.at[e, 1 - side],
                                             device_id=device(0, d), device_id_type=MESH).start()
        src, dst = cor_bufs(e)
        for corner in corners:
            d_sp = -1 if corner < 2 else 1
            d_sp2 = -1 if corner % 2 == 0 else 1

            @pl.when(cor_ok[corner])
            def _():
                pltpu.make_async_remote_copy(src.at[corner], dst.at[3 - corner], cor_send.at[e, corner], cor_recv.at[e, 3 - corner],
                                             device_id=device(d_sp, d_sp2), device_id_type=MESH).start()

    def wait_cols(e, sides=SIDES, corners=CORNERS):
        for side in sides:
            @pl.when(col_ok[side])
            def _():
                pltpu.make_async_copy(cl.at[e, side], cl.at[e, side], col_recv.at[e, side]).wait()
        src, dst = cor_bufs(e)
        for corner in corners:
            @pl.when(cor_ok[corner])
            def _():
                pltpu.make_async_copy(dst.at[corner], dst.at[corner], cor_recv.at[e, corner]).wait()

    def wait_col_sends(e, sides=SIDES, corners=CORNERS):
        for side in sides:
            @pl.when(col_ok[side])
            def _():
                pltpu.make_async_copy(cs.at[e, side], cs.at[e, side], col_send.at[e, side]).wait()
        src, dst = cor_bufs(e)
        for corner in corners:
            @pl.when(cor_ok[corner])
            def _():
                pltpu.make_async_copy(src.at[corner], src.at[corner], cor_send.at[e, corner]).wait()

    def row_landing(e, side):
        if e == 0:
            return xh.at[side]
        return ha.at[e - 1, side] if e < 4 else hb.at[e - 4, side]

    def row_source(e, side, i):
        if e == 0:
            return xin.at[i, 0 if side == 0 else height - 1]
        src, n_rows = (zas[(e - 1) % 2], height) if e < 4 else (zbs[e % 2], low_h)
        return src.at[i, pl.ds(0 if side == 0 else (n_rows - 1) * line, line)]

    def send_rows(e, sides, images, cond=True):
        for side in sides:
            @pl.when(row_ok[side] & cond)
            def _():
                for i in images:
                    pltpu.make_async_remote_copy(row_source(e, side, i), row_landing(e, 1 - side).at[i], row_send.at[e, side, i],
                                                 row_recv.at[e, 1 - side, i], device_id=device(-1 if side == 0 else 1, 0),
                                                 device_id_type=MESH).start()

    def wait_rows(e, sides, images, cond=True):
        for side in sides:
            @pl.when(row_ok[side] & cond)
            def _():
                for i in images:
                    ref = row_landing(e, side).at[i]
                    pltpu.make_async_copy(ref, ref, row_recv.at[e, side, i]).wait()

    def wait_row_sends(e, sides=SIDES):
        for side in sides:
            @pl.when(row_ok[side])
            def _():
                ref = row_landing(e, side)

                def one(i, carry):
                    pltpu.make_async_copy(ref.at[i], ref.at[i], row_send.at[e, side, i]).wait()
                    return carry

                lax.fori_loop(0, n_img, one, 0)

    def sums_refs(e):
        return ta.at[e] if e < 3 else tb.at[e - 3]

    def start_sums(e, part):
        buf = sums_refs(e)
        buf[me] = part

        def send(to_sp, to_sp2):
            pltpu.make_async_remote_copy(buf.at[me], buf.at[me], st_send.at[e], st_recv.at[e], device_id={"sp": to_sp, "sp2": to_sp2},
                                         device_id_type=MESH).start()

        for k, pair in enumerate(others):
            def send_file(t, carry, pair=pair):
                to_sp2 = lax.rem(sp2 + cols_n // 2 + lax.select(lax.rem(t, 2) == 0, lax.div(t + 1, 2), -lax.div(t + 1, 2)), cols_n)
                for to_sp in pair:
                    send(to_sp, to_sp2)
                return carry

            lax.fori_loop(0, cols_n if k + 1 < len(others) else cols_n - 1, send_file, 0)
        send(others[-1][0], sp2)

    def finish_sums(e, num_pos):
        buf = sums_refs(e)
        rest = buf.at[pl.ds(0, n_dev - 1)]
        pltpu.make_async_copy(rest, rest, st_recv.at[e]).wait()
        total = jnp.sum(buf[...], axis=0) * (1.0 / num_pos)
        lines = total.shape[0] // 2
        mean = total[0:lines]
        var = total[lines:] - mean * mean
        return mean, lax.rsqrt(var + EPS)

    def bn(z, par):
        mean, inv, gain, shift = par
        return jnp.maximum(gain * (z - mean) * inv + shift, 0.0)

    def keep(cond, val):
        return jnp.where(cond, val, 0.0)

    def prep_x(i, k):
        xf, ya, sa = xfs[k], yas[k], sas[k]
        last = height + 1
        for r in range(height):
            xf[pl.ds((r + 1) * xstride + PAD, width), :] = xin[i, r].astype(F32)
        xf[pl.ds(PAD, width), :] = keep(has_up, xh[0, i].astype(F32))
        xf[pl.ds(last * xstride + PAD, width), :] = keep(has_down, xh[1, i].astype(F32))
        xf[pl.ds(xstride + PAD - 1, height, stride=xstride), :] = keep(has_left, cl[0, 0, i])
        xf[pl.ds(xstride + PAD + width, height, stride=xstride), :] = keep(has_right, cl[0, 1, i])
        for corner in CORNERS:
            row = 0 if corner < 2 else last
            col = PAD - 1 if corner % 2 == 0 else PAD + width
            xf[row * xstride + col:row * xstride + col + 1, :] = keep(cor_ok[corner], kla[0, corner, i])
        for r in range(height + 2):
            base = r * xstride + PAD
            even = xf[pl.ds(base, half_w, stride=2), :]
            odd = xf[pl.ds(base + 1, half_w, stride=2), :]
            before = xf[pl.ds(base - 1, half_w, stride=2), :]
            after = xf[pl.ds(base + 2, half_w, stride=2), :]
            ya[r] = jnp.concatenate([even, odd], axis=1).astype(BF16)
            sa[r] = jnp.concatenate([before, after], axis=1).astype(BF16)

    def norm_a(e, par, i, k, up=True):
        za, yfa, ya, sa = zas[(e - 1) % 2], yfas[k], yas[k], sas[k]
        last = height + 1
        lo = 0 if up else 1
        for r in range(lo, height + 2):
            if r == 0:
                val = keep(has_up, bn(ha[e - 1, 0, i], par))
            elif r == last:
                val = keep(has_down, bn(ha[e - 1, 1, i], par))
            else:
                val = bn(za[i, pl.ds((r - 1) * line, line), :], par)
            base = r * 2 * fstride + PAD
            yfa[base:base + half_w, :] = val[0:half_w]
            yfa[base + fstride:base + fstride + half_w, :] = val[half_w:]
        if up:
            yfa[pl.ds(3 * fstride + PAD - 1, height, stride=2 * fstride), :] = keep(has_left, bn(cl[e, 0, i], par))
        yfa[pl.ds(2 * fstride + PAD + half_w, height, stride=2 * fstride), :] = keep(has_right, bn(cl[e, 1, i], par))
        for corner in CORNERS if up else (3,):
            row = 0 if corner < 2 else last
            at = row * 2 * fstride + (fstride + PAD - 1 if corner % 2 == 0 else PAD + half_w)
            yfa[at:at + 1, :] = keep(cor_ok[corner], bn(kla[e, corner, i], par))
        for r in range(lo, height + 2):
            base = r * 2 * fstride + PAD
            even = yfa[base:base + half_w, :]
            odd = yfa[base + fstride:base + fstride + half_w, :]
            before = yfa[base + fstride - 1:base + fstride - 1 + half_w, :]
            after = yfa[base + 1:base + 1 + half_w, :]
            ya[r] = jnp.concatenate([even, odd], axis=1).astype(BF16)
            sa[r] = jnp.concatenate([before, after], axis=1).astype(BF16)

    def norm_b(e, par, i, k):
        zb, yfb, yb = zbs[e % 2], yfbs[k], ybs[k]
        last = low_h + 1
        halves = [tuple(p[h:h + 1] for p in par) for h in SIDES]
        tall = tuple(jnp.concatenate([p] * low_h, axis=0) for p in par)
        for r in range(low_h + 2):
            for h in SIDES:
                if r == 0:
                    val = keep(has_up, bn(hb[e - 4, 0, i, pl.ds(h * half_w, half_w), :], halves[h]))
                elif r == last:
                    val = keep(has_down, bn(hb[e - 4, 1, i, pl.ds(h * half_w, half_w), :], halves[h]))
                else:
                    val = bn(zb[i, pl.ds(((r - 1) * 2 + h) * half_w, half_w), :], halves[h])
                base = (r * 2 + h) * fstride + PAD
                yfb[base:base + half_w, :] = val
        yfb[pl.ds(2 * fstride + PAD - 1, 2 * low_h, stride=fstride), :] = keep(has_left, bn(cl[e, 0, i], tall))
        yfb[pl.ds(2 * fstride + PAD + half_w, 2 * low_h, stride=fstride), :] = keep(has_right, bn(cl[e, 1, i], tall))
        for corner in CORNERS:
            row = 0 if corner < 2 else last
            val = keep(cor_ok[corner], bn(klb[e - 4, corner, i], par))
            for h in SIDES:
                at = (row * 2 + h) * fstride + (PAD - 1 if corner % 2 == 0 else PAD + half_w)
                yfb[at:at + 1, :] = val[h:h + 1]
        for r in range(low_h + 2):
            base = r * 2 * fstride + PAD
            for kx in TAPS:
                at = base + kx - 1
                yb[kx, r] = jnp.concatenate([yfb[at:at + half_w, :], yfb[at + fstride:at + fstride + half_w, :]], axis=1).astype(BF16)

    def add_sums(acc, carry):
        tiles = acc.reshape(acc.shape[0] // 8, 8, acc.shape[1])
        return carry[0] + jnp.sum(tiles, axis=0), carry[1] + jnp.sum(tiles * tiles, axis=0)

    zero_sums = (jnp.zeros((8, wide), F32), jnp.zeros((8, wide), F32))

    def edges_a(e, i):
        za = zas[(e - 1) % 2]
        first = za[i, pl.ds(0, height, stride=line), :]
        final = za[i, pl.ds(line - 1, height, stride=line), :]
        for side, edge in enumerate((first, final)):
            cs[e, side, i] = edge
            ksa[e, side, i] = edge[0:1]
            ksa[e, 2 + side, i] = edge[height - 1:height]

    def edges_b(e, i):
        zb = zbs[e % 2]
        first = zb[i, pl.ds(0, 2 * low_h, stride=half_w), :]
        final = zb[i, pl.ds(half_w - 1, 2 * low_h, stride=half_w), :]
        for side, edge in enumerate((first, final)):
            cs[e, side, i] = edge
            ksb[e - 4, side, i] = edge[0:2]
            ksb[e - 4, 2 + side, i] = edge[2 * low_h - 2:2 * low_h]

    def store_z(ref, i, acc, rows):
        for r in range(rows):
            at = r * line
            ref[i, at:at + half_w, :] = acc[r * half_w:(r + 1) * half_w, 0:chan]
            ref[i, at + half_w:at + line, :] = acc[r * half_w:(r + 1) * half_w, chan:wide]

    def products(pairs):
        acc = None
        for lhs, w in pairs:
            d = jnp.dot(lhs, w, preferred_element_type=F32)
            acc = d if acc is None else acc + d
        return acc

    def conv_a(layer, i, k, carry):
        pairs = []
        for ky in TAPS:
            for ref, w in ((yas[k], wy), (sas[k], ws)):
                pairs.append((ref[ky:ky + height].reshape(height * half_w, wide), w[layer, ky]))
        acc = products(pairs)
        store_z(zas[layer % 2], i, acc, height)
        edges_a(layer + 1, i)
        return add_sums(acc, carry)

    def conv_down(i, k, carry):
        pairs = []
        for ky in TAPS:
            for part, ref in enumerate((yas[k], sas[k])):
                pairs.append((jnp.concatenate([ref[1 + 2 * r + ky] for r in range(low_h)], axis=0), wd[ky, part]))
        acc = products(pairs)
        store_z(zbs[0], i, acc, low_h)
        edges_b(4, i)
        return add_sums(acc, carry)

    def conv_b(layer, i, k, carry):
        pairs = []
        for ky in TAPS:
            for kx in TAPS:
                pairs.append((ybs[k][kx, ky:ky + low_h].reshape(low_h * half_w, wide), wb[layer, ky, kx]))
        acc = products(pairs)
        if layer == 0:
            store_z(zb1, i, acc, low_h)
            edges_b(5, i)
        else:
            zo[i] = acc.reshape(low_h, half_w, wide)
        return add_sums(acc, carry)

    def layer(e, prep, conv, in_sides, out_sides, early):
        wait_rows(e, in_sides, (0,))
        prep(0, 0)

        half = n_img // 2

        def group(j, carry):
            i = half * j
            wait_rows(e, in_sides, [i + u for u in range(1, half)])
            wait_rows(e, in_sides, (i + half,), j == 0)
            if e == 0:
                @pl.when(j == 1)
                def _():
                    meet_again(1)
            for u in range(half):
                nxt = u + 1
                prep(i + nxt if nxt < half else half, nxt % 2)
                carry = conv(i + u, u % 2, carry)
            send_rows(e + 1, out_sides, range(early), j == 0)
            return carry

        s1, s2 = lax.fori_loop(0, 2, group, zero_sums)
        s1, s2 = (jnp.sum(s, axis=0, keepdims=True) for s in (s1, s2))
        if e < 3:
            part = [s1[:, 0:chan] + s1[:, chan:], s2[:, 0:chan] + s2[:, chan:]]
        else:
            part = [s1[:, 0:chan], s1[:, chan:], s2[:, 0:chan], s2[:, chan:]]
        if e == 0:
            for k in range(2, len(steps)):
                meet_again(k)
        start_sums(e, jnp.concatenate(part, axis=0))
        if e < 5:
            both = len(out_sides) == 2
            start_cols(e + 1, SIDES if both else (0,), CORNERS if both else (0,))
            send_rows(e + 1, out_sides, range(early, n_img))

    start_cols(0)
    send_rows(0, SIDES, range(n_img))
    call(meet.at[0], steps[0])
    zeros = jnp.zeros((chan, chan), BF16)
    for depth in TAPS:
        for ky in TAPS:
            ws[depth, ky, 0:chan, chan:wide] = zeros
            ws[depth, ky, chan:wide, 0:chan] = zeros
    for ky in TAPS:
        wd[ky, 1, 0:chan, :] = jnp.zeros((chan, wide), BF16)
    for copy in weight_copies[:6]:
        copy.wait()
    meet_again(0)
    wait_cols(0)

    pos_a = n_dev * n_img * height * width
    pos_b = n_dev * n_img * low_h * half_w

    def params_a(e, layer):
        mean, inv = finish_sums(e, pos_a)
        return mean, inv, ga[layer, 0:1], ga[layer, 1:2]

    def params_b(e, ref):
        mean, inv = finish_sums(e, pos_b)
        gain = jnp.concatenate([ref[0:1, 0:chan], ref[0:1, chan:]], axis=0)
        shift = jnp.concatenate([ref[1:2, 0:chan], ref[1:2, chan:]], axis=0)
        return mean, inv, gain, shift

    part = functools.partial
    layer(0, prep_x, part(conv_a, 0), SIDES, SIDES, EARLY_A)

    for copy in weight_copies[6:]:
        copy.wait()
    wait_row_sends(0)
    wait_col_sends(0)
    wait_cols(1)
    layer(1, part(norm_a, 1, params_a(0, 0)), part(conv_a, 1), SIDES, SIDES, EARLY_A)

    wait_row_sends(1)
    wait_col_sends(1)
    wait_cols(2)
    layer(2, part(norm_a, 2, params_a(1, 1)), part(conv_a, 2), SIDES, (0,), EARLY_A)

    wait_row_sends(2)
    wait_col_sends(2)
    wait_cols(3, (1,), (3,))
    layer(3, part(norm_a, 3, params_a(2, 2), up=False), conv_down, (1,), SIDES, EARLY_B)

    wait_row_sends(3, (0,))
    wait_col_sends(3, (0,), (0,))
    wait_cols(4)
    layer(4, part(norm_b, 4, params_b(3, gd)), part(conv_b, 0), SIDES, SIDES, EARLY_B)

    wait_row_sends(4)
    wait_col_sends(4)
    wait_cols(5)
    layer(5, part(norm_b, 5, params_b(4, gb.at[0])), part(conv_b, 1), SIDES, (), 0)

    wait_row_sends(5)
    wait_col_sends(5)
    mean, inv = finish_sums(5, pos_b)
    for out, val in ((mean_o, mean), (inv_o, inv)):
        for h in SIDES:
            out[:, h * chan:(h + 1) * chan] = val[h:h + 1]
    gain_o[...] = gb[1, 0:1]
    shift_o[...] = gb[1, 1:2]

    for e in range(6):
        buf = sums_refs(e)
        rest = buf.at[pl.ds(0, n_dev - 1)]
        pltpu.make_async_copy(rest, rest, st_send.at[e]).wait()


def net(rows_n, cols_n, x, w_a, bn_a, w_down, bn_down, w_b, bn_b):
    n_img, height, width, chan = x.shape
    half_w, low_h = width // 2, height // 2
    n_dev = rows_n * cols_n
    vmem, dma = pltpu.VMEM, pltpu.SemaphoreType.DMA
    line, wide = 2 * half_w, 2 * chan
    plane = half_w + 2 * PAD
    a_sums, b_sums = 3, 3
    n_ex = a_sums + b_sums
    two, corners = len(SIDES), len(CORNERS)
    scratch = [
        vmem(x.shape, BF16),
        vmem((two, n_img, width, chan), BF16),
        *[vmem(((height + 2) * (width + 2 * PAD), chan), F32)] * two,
        *[vmem((n_img, height * line, chan), F32)] * two,
        *[vmem((n_img, low_h * line, chan), F32)] * two,
        vmem((a_sums, two, n_img, line, chan), F32),
        vmem((b_sums - 1, two, n_img, line, chan), F32),
        *[vmem(((height + 2) * 2 * plane, chan), F32)] * two,
        *[vmem(((low_h + 2) * 2 * plane, chan), F32)] * two,
        *[vmem((height + 2, half_w, wide), BF16)] * 4,
        *[vmem((3, low_h + 2, half_w, wide), BF16)] * two,
        *[vmem((n_ex, two, n_img, height, chan), F32)] * two,
        *[vmem((a_sums + 1, corners, n_img, 1, chan), F32)] * two,
        *[vmem((b_sums - 1, corners, n_img, 2, chan), F32)] * two,
        vmem((a_sums, n_dev, 2, chan), F32),
        vmem((b_sums, n_dev, 4, chan), F32),
        *[vmem((a_sums, 3, wide, wide), BF16)] * two,
        vmem((3, two, wide, wide), BF16),
        vmem(w_b.shape, BF16),
        vmem(bn_a.shape, F32),
        vmem(bn_down.shape, F32),
        vmem(bn_b.shape, F32),
        dma((n_img,)),
        dma((13,)),
        *[dma((n_ex, two, n_img))] * two,
        *[dma((n_ex, two))] * two,
        *[dma((n_ex, corners))] * two,
        *[dma((n_ex,))] * two,
        pltpu.SemaphoreType.REGULAR((3,)),
    ]
    hbm_spec = pl.BlockSpec(memory_space=pltpu.HBM)
    line_out = jax.ShapeDtypeStruct((1, wide), F32)
    z, *vectors = pl.pallas_call(
        functools.partial(net_kernel, (rows_n, cols_n, n_img, height, width, chan)),
        out_shape=(jax.ShapeDtypeStruct((n_img, low_h, half_w, wide), F32),) + (line_out,) * 4,
        in_specs=[hbm_spec] * 7,
        out_specs=(pl.BlockSpec(memory_space=pltpu.VMEM),) * 5,
        scratch_shapes=scratch,
        compiler_params=pltpu.CompilerParams(collective_id=0, has_side_effects=True, vmem_limit_bytes=40 * 1024 * 1024),
        name="conv_bn_net",
    )(*[pltpu.with_memory_space_constraint(arg, pltpu.HBM) for arg in (x, w_a, bn_a, w_down, bn_down, w_b, bn_b)])
    mean, inv, gain, shift = [v.reshape(wide) for v in vectors]
    return jnp.maximum(gain * (z - mean) * inv + shift, 0.0).astype(BF16)


def solution(mesh):
    tile_spec = P("dp", "sp", "sp2", None)
    per_device = functools.partial(net, mesh.shape["sp"], mesh.shape["sp2"])
    return jax.shard_map(per_device, mesh=mesh, in_specs=(tile_spec, P(), P(), P(), P(), P(), P()), out_specs=tile_spec, check_vma=False)
```

```python
import functools

import jax
import jax.numpy as jnp
from jax import lax
from jax.experimental import pallas as pl
from jax.experimental.pallas import tpu as pltpu
from jax.sharding import PartitionSpec as P

MESH = pl.DeviceIdType.MESH
F32 = jnp.float32
BF16 = jnp.bfloat16
EPS = 1e-5
PAD = 8
SIDES = (0, 1)
CORNERS = (0, 1, 2, 3)
TAPS = range(3)
EARLY_A = 4
EARLY_B = 4


def net_kernel(dims, x, w_a, bn_a, w_down, bn_down, w_b, bn_b, zo, mean_o, inv_o, gain_o, shift_o,
               xin, xh, xf0, xf1, za0, za1, zb0, zb1, ha, hb, yfa0, yfa1, yfb0, yfb1, ya0, ya1, sa0, sa1, yb0, yb1,
               cs, cl, ksa, kla, ksb, klb, ta, tb, wy, ws, wd, wb, ga, gd, gb,
               in_sem, w_sem, row_recv, row_send, col_recv, col_send, cor_recv, cor_send, st_recv, st_send, meet):
    rows_n, cols_n, n_img, height, width, chan = dims
    n_dev = rows_n * cols_n
    half_w, low_h = width // 2, height // 2
    line, wide = 2 * half_w, 2 * chan
    xstride = width + 2 * PAD
    fstride = half_w + 2 * PAD
    xfs, zas, zbs, yfas, yfbs, yas, sas, ybs = (xf0, xf1), (za0, za1), (zb0, zb1), (yfa0, yfa1), (yfb0, yfb1), (ya0, ya1), (sa0, sa1), (yb0, yb1)
    sp = lax.axis_index("sp")
    sp2 = lax.axis_index("sp2")
    me = sp2 * rows_n + sp
    has_up = sp > 0
    has_down = sp < rows_n - 1
    has_left = sp2 > 0
    has_right = sp2 < cols_n - 1
    row_ok = (has_up, has_down)
    col_ok = (has_left, has_right)
    cor_ok = tuple(r & c for r in row_ok for c in col_ok)

    def device(d_sp, d_sp2):
        return {"sp": sp + d_sp, "sp2": sp2 + d_sp2}

    def ring(step):
        found = []
        for d_sp in (-step, 0, step):
            for d_sp2 in (-step, 0, step):
                if (d_sp or d_sp2) and abs(d_sp2) < cols_n and abs(d_sp) < rows_n:
                    ok = (sp + d_sp >= 0) & (sp + d_sp < rows_n) & (sp2 + d_sp2 >= 0) & (sp2 + d_sp2 < cols_n)
                    found.append((ok, device(d_sp, d_sp2)))
        return found

    def call(sem, step):
        for ok, where in ring(step):
            @pl.when(ok)
            def _():
                pl.semaphore_signal(sem, inc=1, device_id=where, device_id_type=MESH)

    def hear(sem, step):
        pl.semaphore_wait(sem, sum(ok.astype(jnp.int32) for ok, where in ring(step)))

    steps = [1]
    while 2 * steps[-1] < max(rows_n, cols_n) and len(steps) < meet.shape[0]:
        steps.append(2 * steps[-1])

    def meet_again(k):
        if k < len(steps):
            hear(meet.at[k], steps[k])
        if k + 1 < len(steps):
            call(meet.at[k + 1], steps[k + 1])

    chips = rows_n // 2
    chip, core = lax.div(sp, 2), lax.rem(sp, 2)
    others = []
    for d in sorted(range(chips), key=lambda d: -min(d, chips - d)):
        at = lax.rem(chip + d, chips) * 2
        others.append((at + 1 - core, at + core))

    for i in range(n_img):
        pltpu.make_async_copy(x.at[i], xin.at[i], in_sem.at[i]).start()
    weight_copies = []
    for kx, dst, k0, n0 in ((1, wy, 0, 0), (1, wy, chan, chan), (0, wy, 0, chan), (2, wy, chan, 0), (0, ws, 0, 0), (2, ws, chan, chan)):
        weight_copies.append((w_a.at[:, :, kx], dst.at[:, :, pl.ds(k0, chan), pl.ds(n0, chan)]))
    weight_copies.append((w_down.at[:, 0], wd.at[:, 0, pl.ds(0, chan), :]))
    weight_copies.append((w_down.at[:, 1], wd.at[:, 0, pl.ds(chan, chan), :]))
    weight_copies.append((w_down.at[:, 2], wd.at[:, 1, pl.ds(chan, chan), :]))
    weight_copies.append((w_b, wb))
    weight_copies.append((bn_a, ga))
    weight_copies.append((bn_down, gd))
    weight_copies.append((bn_b, gb))
    weight_copies = [pltpu.make_async_copy(s, d, w_sem.at[k]) for k, (s, d) in enumerate(weight_copies)]
    for copy in weight_copies:
        copy.start()

    barrier = pltpu.get_barrier_semaphore()
    call(barrier, 1)

    for i in range(n_img):
        pltpu.make_async_copy(x.at[i], xin.at[i], in_sem.at[i]).wait()
    for i in range(n_img):
        for side, col0, pick in ((0, 0, 0), (1, width - 16, 15)):
            blk = xin[i, :, col0:col0 + 16, :].astype(F32)
            at = side * height * 16
            za0[i, at:at + height * 16, :] = blk.reshape(height * 16, chan)
            edge = za0[i, pl.ds(at + pick, height, stride=16), :]
            cs[0, side, i] = edge
            ksa[0, side, i] = edge[0:1]
            ksa[0, 2 + side, i] = edge[height - 1:height]

    hear(barrier, 1)

    def cor_bufs(e):
        return (ksa.at[e], kla.at[e]) if e < 4 else (ksb.at[e - 4], klb.at[e - 4])

    def start_cols(e, sides=SIDES, corners=CORNERS):
        for side in sides:
            d = -1 if side == 0 else 1

            @pl.when(col_ok[side])
            def _():
                pltpu.make_async_remote_copy(cs.at[e, side], cl.at[e, 1 - side], col_send.at[e, side], col_recv.at[e, 1 - side],
                                             device_id=device(0, d), device_id_type=MESH).start()
        src, dst = cor_bufs(e)
        for corner in corners:
            d_sp = -1 if corner < 2 else 1
            d_sp2 = -1 if corner % 2 == 0 else 1

            @pl.when(cor_ok[corner])
            def _():
                pltpu.make_async_remote_copy(src.at[corner], dst.at[3 - corner], cor_send.at[e, corner], cor_recv.at[e, 3 - corner],
                                             device_id=device(d_sp, d_sp2), device_id_type=MESH).start()

    def wait_cols(e, sides=SIDES, corners=CORNERS):
        for side in sides:
            @pl.when(col_ok[side])
            def _():
                pltpu.make_async_copy(cl.at[e, side], cl.at[e, side], col_recv.at[e, side]).wait()
        src, dst = cor_bufs(e)
        for corner in corners:
            @pl.when(cor_ok[corner])
            def _():
                pltpu.make_async_copy(dst.at[corner], dst.at[corner], cor_recv.at[e, corner]).wait()

    def wait_col_sends(e, sides=SIDES, corners=CORNERS):
        for side in sides:
            @pl.when(col_ok[side])
            def _():
                pltpu.make_async_copy(cs.at[e, side], cs.at[e, side], col_send.at[e, side]).wait()
        src, dst = cor_bufs(e)
        for corner in corners:
            @pl.when(cor_ok[corner])
            def _():
                pltpu.make_async_copy(src.at[corner], src.at[corner], cor_send.at[e, corner]).wait()

    def row_landing(e, side):
        if e == 0:
            return xh.at[side]
        return ha.at[e - 1, side] if e < 4 else hb.at[e - 4, side]

    def row_source(e, side, i):
        if e == 0:
            return xin.at[i, 0 if side == 0 else height - 1]
        src, n_rows = (zas[(e - 1) % 2], height) if e < 4 else (zbs[e % 2], low_h)
        return src.at[i, pl.ds(0 if side == 0 else (n_rows - 1) * line, line)]

    def send_rows(e, sides, images, cond=True):
        for side in sides:
            @pl.when(row_ok[side] & cond)
            def _():
                for i in images:
                    pltpu.make_async_remote_copy(row_source(e, side, i), row_landing(e, 1 - side).at[i], row_send.at[e, side, i],
                                                 row_recv.at[e, 1 - side, i], device_id=device(-1 if side == 0 else 1, 0),
                                                 device_id_type=MESH).start()

    def wait_rows(e, sides, images, cond=True):
        for side in sides:
            @pl.when(row_ok[side] & cond)
            def _():
                for i in images:
                    ref = row_landing(e, side).at[i]
                    pltpu.make_async_copy(ref, ref, row_recv.at[e, side, i]).wait()

    def wait_row_sends(e, sides=SIDES):
        for side in sides:
            @pl.when(row_ok[side])
            def _():
                ref = row_landing(e, side)

                def one(i, carry):
                    pltpu.make_async_copy(ref.at[i], ref.at[i], row_send.at[e, side, i]).wait()
                    return carry

                lax.fori_loop(0, n_img, one, 0)

    def sums_refs(e):
        return ta.at[e] if e < 3 else tb.at[e - 3]

    def start_sums(e, part):
        buf = sums_refs(e)
        buf[me] = part

        def send(to_sp, to_sp2):
            pltpu.make_async_remote_copy(buf.at[me], buf.at[me], st_send.at[e], st_recv.at[e], device_id={"sp": to_sp, "sp2": to_sp2},
                                         device_id_type=MESH).start()

        for k, pair in enumerate(others):
            def send_file(t, carry, pair=pair):
                to_sp2 = lax.rem(sp2 + cols_n // 2 + lax.select(lax.rem(t, 2) == 0, lax.div(t + 1, 2), -lax.div(t + 1, 2)), cols_n)
                for to_sp in pair:
                    send(to_sp, to_sp2)
                return carry

            lax.fori_loop(0, cols_n if k + 1 < len(others) else cols_n - 1, send_file, 0)
        send(others[-1][0], sp2)

    def finish_sums(e, num_pos):
        buf = sums_refs(e)
        rest = buf.at[pl.ds(0, n_dev - 1)]
        pltpu.make_async_copy(rest, rest, st_recv.at[e]).wait()
        total = jnp.sum(buf[...], axis=0) * (1.0 / num_pos)
        lines = total.shape[0] // 2
        mean = total[0:lines]
        var = total[lines:] - mean * mean
        return mean, lax.rsqrt(var + EPS)

    def bn(z, par):
        mean, inv, gain, shift = par
        return jnp.maximum(gain * (z - mean) * inv + shift, 0.0)

    def keep(cond, val):
        return jnp.where(cond, val, 0.0)

    def prep_x(i, k):
        xf, ya, sa = xfs[k], yas[k], sas[k]
        last = height + 1
        for r in range(height):
            xf[pl.ds((r + 1) * xstride + PAD, width), :] = xin[i, r].astype(F32)
        xf[pl.ds(PAD, width), :] = keep(has_up, xh[0, i].astype(F32))
        xf[pl.ds(last * xstride + PAD, width), :] = keep(has_down, xh[1, i].astype(F32))
        xf[pl.ds(xstride + PAD - 1, height, stride=xstride), :] = keep(has_left, cl[0, 0, i])
        xf[pl.ds(xstride + PAD + width, height, stride=xstride), :] = keep(has_right, cl[0, 1, i])
        for corner in CORNERS:
            row = 0 if corner < 2 else last
            col = PAD - 1 if corner % 2 == 0 else PAD + width
            xf[row * xstride + col:row * xstride + col + 1, :] = keep(cor_ok[corner], kla[0, corner, i])
        for r in range(height + 2):
            base = r * xstride + PAD
            even = xf[pl.ds(base, half_w, stride=2), :]
            odd = xf[pl.ds(base + 1, half_w, stride=2), :]
            before = xf[pl.ds(base - 1, half_w, stride=2), :]
            after = xf[pl.ds(base + 2, half_w, stride=2), :]
            ya[r] = jnp.concatenate([even, odd], axis=1).astype(BF16)
            sa[r] = jnp.concatenate([before, after], axis=1).astype(BF16)

    def norm_a(e, par, i, k, up=True):
        za, yfa, ya, sa = zas[(e - 1) % 2], yfas[k], yas[k], sas[k]
        last = height + 1
        lo = 0 if up else 1
        for r in range(lo, height + 2):
            if r == 0:
                val = keep(has_up, bn(ha[e - 1, 0, i], par))
            elif r == last:
                val = keep(has_down, bn(ha[e - 1, 1, i], par))
            else:
                val = bn(za[i, pl.ds((r - 1) * line, line), :], par)
            base = r * 2 * fstride + PAD
            yfa[base:base + half_w, :] = val[0:half_w]
            yfa[base + fstride:base + fstride + half_w, :] = val[half_w:]
        if up:
            yfa[pl.ds(3 * fstride + PAD - 1, height, stride=2 * fstride), :] = keep(has_left, bn(cl[e, 0, i], par))
        yfa[pl.ds(2 * fstride + PAD + half_w, height, stride=2 * fstride), :] = keep(has_right, bn(cl[e, 1, i], par))
        for corner in CORNERS if up else (3,):
            row = 0 if corner < 2 else last
            at = row * 2 * fstride + (fstride + PAD - 1 if corner % 2 == 0 else PAD + half_w)
            yfa[at:at + 1, :] = keep(cor_ok[corner], bn(kla[e, corner, i], par))
        for r in range(lo, height + 2):
            base = r * 2 * fstride + PAD
            even = yfa[base:base + half_w, :]
            odd = yfa[base + fstride:base + fstride + half_w, :]
            before = yfa[base + fstride - 1:base + fstride - 1 + half_w, :]
            after = yfa[base + 1:base + 1 + half_w, :]
            ya[r] = jnp.concatenate([even, odd], axis=1).astype(BF16)
            sa[r] = jnp.concatenate([before, after], axis=1).astype(BF16)

    def norm_b(e, par, i, k):
        zb, yfb, yb = zbs[e % 2], yfbs[k], ybs[k]
        last = low_h + 1
        halves = [tuple(p[h:h + 1] for p in par) for h in SIDES]
        tall = tuple(jnp.concatenate([p] * low_h, axis=0) for p in par)
        for r in range(low_h + 2):
            for h in SIDES:
                if r == 0:
                    val = keep(has_up, bn(hb[e - 4, 0, i, pl.ds(h * half_w, half_w), :], halves[h]))
                elif r == last:
                    val = keep(has_down, bn(hb[e - 4, 1, i, pl.ds(h * half_w, half_w), :], halves[h]))
                else:
                    val = bn(zb[i, pl.ds(((r - 1) * 2 + h) * half_w, half_w), :], halves[h])
                base = (r * 2 + h) * fstride + PAD
                yfb[base:base + half_w, :] = val
        yfb[pl.ds(2 * fstride + PAD - 1, 2 * low_h, stride=fstride), :] = keep(has_left, bn(cl[e, 0, i], tall))
        yfb[pl.ds(2 * fstride + PAD + half_w, 2 * low_h, stride=fstride), :] = keep(has_right, bn(cl[e, 1, i], tall))
        for corner in CORNERS:
            row = 0 if corner < 2 else last
            val = keep(cor_ok[corner], bn(klb[e - 4, corner, i], par))
            for h in SIDES:
                at = (row * 2 + h) * fstride + (PAD - 1 if corner % 2 == 0 else PAD + half_w)
                yfb[at:at + 1, :] = val[h:h + 1]
        for r in range(low_h + 2):
            base = r * 2 * fstride + PAD
            for kx in TAPS:
                at = base + kx - 1
                yb[kx, r] = jnp.concatenate([yfb[at:at + half_w, :], yfb[at + fstride:at + fstride + half_w, :]], axis=1).astype(BF16)

    def add_sums(acc, carry):
        tiles = acc.reshape(acc.shape[0] // 8, 8, acc.shape[1])
        return carry[0] + jnp.sum(tiles, axis=0), carry[1] + jnp.sum(tiles * tiles, axis=0)

    zero_sums = (jnp.zeros((8, wide), F32), jnp.zeros((8, wide), F32))

    def edges_a(e, i):
        za = zas[(e - 1) % 2]
        first = za[i, pl.ds(0, height, stride=line), :]
        final = za[i, pl.ds(line - 1, height, stride=line), :]
        for side, edge in enumerate((first, final)):
            cs[e, side, i] = edge
            ksa[e, side, i] = edge[0:1]
            ksa[e, 2 + side, i] = edge[height - 1:height]

    def edges_b(e, i):
        zb = zbs[e % 2]
        first = zb[i, pl.ds(0, 2 * low_h, stride=half_w), :]
        final = zb[i, pl.ds(half_w - 1, 2 * low_h, stride=half_w), :]
        for side, edge in enumerate((first, final)):
            cs[e, side, i] = edge
            ksb[e - 4, side, i] = edge[0:2]
            ksb[e - 4, 2 + side, i] = edge[2 * low_h - 2:2 * low_h]

    def store_z(ref, i, acc, rows):
        for r in range(rows):
            at = r * line
            ref[i, at:at + half_w, :] = acc[r * half_w:(r + 1) * half_w, 0:chan]
            ref[i, at + half_w:at + line, :] = acc[r * half_w:(r + 1) * half_w, chan:wide]

    def products(pairs):
        acc = None
        for lhs, w in pairs:
            d = jnp.dot(lhs, w, preferred_element_type=F32)
            acc = d if acc is None else acc + d
        return acc

    def conv_a(layer, i, k, carry):
        pairs = []
        for ky in TAPS:
            for ref, w in ((yas[k], wy), (sas[k], ws)):
                pairs.append((ref[ky:ky + height].reshape(height * half_w, wide), w[layer, ky]))
        acc = products(pairs)
        store_z(zas[layer % 2], i, acc, height)
        edges_a(layer + 1, i)
        return add_sums(acc, carry)

    def conv_down(i, k, carry):
        pairs = []
        for ky in TAPS:
            for part, ref in enumerate((yas[k], sas[k])):
                pairs.append((jnp.concatenate([ref[1 + 2 * r + ky] for r in range(low_h)], axis=0), wd[ky, part]))
        acc = products(pairs)
        store_z(zbs[0], i, acc, low_h)
        edges_b(4, i)
        return add_sums(acc, carry)

    def conv_b(layer, i, k, carry):
        pairs = []
        for ky in TAPS:
            for kx in TAPS:
                pairs.append((ybs[k][kx, ky:ky + low_h].reshape(low_h * half_w, wide), wb[layer, ky, kx]))
        acc = products(pairs)
        if layer == 0:
            store_z(zb1, i, acc, low_h)
            edges_b(5, i)
        else:
            zo[i] = acc.reshape(low_h, half_w, wide)
        return add_sums(acc, carry)

    def layer(e, prep, conv, in_sides, out_sides, early):
        wait_rows(e, in_sides, (0,))
        prep(0, 0)

        half = n_img // 2

        def pair(j, carry):
            i = 2 * j
            wait_rows(e, in_sides, (i + 1, i + 2))
            for u in SIDES:
                prep(i + u + 1, 1 - u)
                carry = conv(i + u, u, carry)
            send_rows(e + 1, out_sides, (i, i + 1), i < early)
            return carry

        carry = lax.fori_loop(0, half // 2, pair, zero_sums)
        wait_rows(e, in_sides, range(half + 1, n_img))
        if e == 0:
            meet_again(1)
        for i in range(half, n_img):
            if i + 1 < n_img:
                prep(i + 1, (i + 1) % 2)
            carry = conv(i, i % 2, carry)
        s1, s2 = carry
        s1, s2 = (jnp.sum(s, axis=0, keepdims=True) for s in (s1, s2))
        if e < 3:
            part = [s1[:, 0:chan] + s1[:, chan:], s2[:, 0:chan] + s2[:, chan:]]
        else:
            part = [s1[:, 0:chan], s1[:, chan:], s2[:, 0:chan], s2[:, chan:]]
        if e == 0:
            for k in range(2, len(steps)):
                meet_again(k)
        start_sums(e, jnp.concatenate(part, axis=0))
        if e < 5:
            both = len(out_sides) == 2
            start_cols(e + 1, SIDES if both else (0,), CORNERS if both else (0,))
            send_rows(e + 1, out_sides, range(early, n_img))

    start_cols(0)
    send_rows(0, SIDES, range(n_img))
    call(meet.at[0], steps[0])
    zeros = jnp.zeros((chan, chan), BF16)
    for depth in TAPS:
        for ky in TAPS:
            ws[depth, ky, 0:chan, chan:wide] = zeros
            ws[depth, ky, chan:wide, 0:chan] = zeros
    for ky in TAPS:
        wd[ky, 1, 0:chan, :] = jnp.zeros((chan, wide), BF16)
    for copy in weight_copies[:6]:
        copy.wait()
    meet_again(0)
    wait_cols(0)

    pos_a = n_dev * n_img * height * width
    pos_b = n_dev * n_img * low_h * half_w

    def params_a(e, layer):
        mean, inv = finish_sums(e, pos_a)
        return mean, inv, ga[layer, 0:1], ga[layer, 1:2]

    def params_b(e, ref):
        mean, inv = finish_sums(e, pos_b)
        gain = jnp.concatenate([ref[0:1, 0:chan], ref[0:1, chan:]], axis=0)
        shift = jnp.concatenate([ref[1:2, 0:chan], ref[1:2, chan:]], axis=0)
        return mean, inv, gain, shift

    part = functools.partial
    layer(0, prep_x, part(conv_a, 0), SIDES, SIDES, EARLY_A)

    for copy in weight_copies[6:]:
        copy.wait()
    wait_row_sends(0)
    wait_col_sends(0)
    wait_cols(1)
    layer(1, part(norm_a, 1, params_a(0, 0)), part(conv_a, 1), SIDES, SIDES, EARLY_A)

    wait_row_sends(1)
    wait_col_sends(1)
    wait_cols(2)
    layer(2, part(norm_a, 2, params_a(1, 1)), part(conv_a, 2), SIDES, (0,), EARLY_A)

    wait_row_sends(2)
    wait_col_sends(2)
    wait_cols(3, (1,), (3,))
    layer(3, part(norm_a, 3, params_a(2, 2), up=False), conv_down, (1,), SIDES, EARLY_B)

    wait_row_sends(3, (0,))
    wait_col_sends(3, (0,), (0,))
    wait_cols(4)
    layer(4, part(norm_b, 4, params_b(3, gd)), part(conv_b, 0), SIDES, SIDES, EARLY_B)

    wait_row_sends(4)
    wait_col_sends(4)
    wait_cols(5)
    layer(5, part(norm_b, 5, params_b(4, gb.at[0])), part(conv_b, 1), SIDES, (), 0)

    wait_row_sends(5)
    wait_col_sends(5)
    mean, inv = finish_sums(5, pos_b)
    for out, val in ((mean_o, mean), (inv_o, inv)):
        for h in SIDES:
            out[:, h * chan:(h + 1) * chan] = val[h:h + 1]
    gain_o[...] = gb[1, 0:1]
    shift_o[...] = gb[1, 1:2]

    for e in range(6):
        buf = sums_refs(e)
        rest = buf.at[pl.ds(0, n_dev - 1)]
        pltpu.make_async_copy(rest, rest, st_send.at[e]).wait()


def net(rows_n, cols_n, x, w_a, bn_a, w_down, bn_down, w_b, bn_b):
    n_img, height, width, chan = x.shape
    half_w, low_h = width // 2, height // 2
    n_dev = rows_n * cols_n
    vmem, dma = pltpu.VMEM, pltpu.SemaphoreType.DMA
    line, wide = 2 * half_w, 2 * chan
    plane = half_w + 2 * PAD
    a_sums, b_sums = 3, 3
    n_ex = a_sums + b_sums
    two, corners = len(SIDES), len(CORNERS)
    scratch = [
        vmem(x.shape, BF16),
        vmem((two, n_img, width, chan), BF16),
        *[vmem(((height + 2) * (width + 2 * PAD), chan), F32)] * two,
        *[vmem((n_img, height * line, chan), F32)] * two,
        *[vmem((n_img, low_h * line, chan), F32)] * two,
        vmem((a_sums, two, n_img, line, chan), F32),
        vmem((b_sums - 1, two, n_img, line, chan), F32),
        *[vmem(((height + 2) * 2 * plane, chan), F32)] * two,
        *[vmem(((low_h + 2) * 2 * plane, chan), F32)] * two,
        *[vmem((height + 2, half_w, wide), BF16)] * 4,
        *[vmem((3, low_h + 2, half_w, wide), BF16)] * two,
        *[vmem((n_ex, two, n_img, height, chan), F32)] * two,
        *[vmem((a_sums + 1, corners, n_img, 1, chan), F32)] * two,
        *[vmem((b_sums - 1, corners, n_img, 2, chan), F32)] * two,
        vmem((a_sums, n_dev, 2, chan), F32),
        vmem((b_sums, n_dev, 4, chan), F32),
        *[vmem((a_sums, 3, wide, wide), BF16)] * two,
        vmem((3, two, wide, wide), BF16),
        vmem(w_b.shape, BF16),
        vmem(bn_a.shape, F32),
        vmem(bn_down.shape, F32),
        vmem(bn_b.shape, F32),
        dma((n_img,)),
        dma((13,)),
        *[dma((n_ex, two, n_img))] * two,
        *[dma((n_ex, two))] * two,
        *[dma((n_ex, corners))] * two,
        *[dma((n_ex,))] * two,
        pltpu.SemaphoreType.REGULAR((3,)),
    ]
    hbm_spec = pl.BlockSpec(memory_space=pltpu.HBM)
    line_out = jax.ShapeDtypeStruct((1, wide), F32)
    z, *vectors = pl.pallas_call(
        functools.partial(net_kernel, (rows_n, cols_n, n_img, height, width, chan)),
        out_shape=(jax.ShapeDtypeStruct((n_img, low_h, half_w, wide), F32),) + (line_out,) * 4,
        in_specs=[hbm_spec] * 7,
        out_specs=(pl.BlockSpec(memory_space=pltpu.VMEM),) * 5,
        scratch_shapes=scratch,
        compiler_params=pltpu.CompilerParams(collective_id=0, has_side_effects=True, vmem_limit_bytes=40 * 1024 * 1024),
        name="conv_bn_net",
    )(*[pltpu.with_memory_space_constraint(arg, pltpu.HBM) for arg in (x, w_a, bn_a, w_down, bn_down, w_b, bn_b)])
    mean, inv, gain, shift = [v.reshape(wide) for v in vectors]
    return jnp.maximum(gain * (z - mean) * inv + shift, 0.0).astype(BF16)


def solution(mesh):
    tile_spec = P("dp", "sp", "sp2", None)
    per_device = functools.partial(net, mesh.shape["sp"], mesh.shape["sp2"])
    return jax.shard_map(per_device, mesh=mesh, in_specs=(tile_spec, P(), P(), P(), P(), P(), P()), out_specs=tile_spec, check_vma=False)
```

```python
import functools

import jax
import jax.numpy as jnp
from jax import lax
from jax.experimental import pallas as pl
from jax.experimental.pallas import tpu as pltpu
from jax.sharding import PartitionSpec as P

MESH = pl.DeviceIdType.MESH
F32 = jnp.float32
BF16 = jnp.bfloat16
EPS = 1e-5
PAD = 8
SIDES = (0, 1)
CORNERS = (0, 1, 2, 3)
TAPS = range(3)
EARLY_A = 2
EARLY_B = 2


def net_kernel(dims, x, w_a, bn_a, w_down, bn_down, w_b, bn_b, zo, mean_o, inv_o, gain_o, shift_o,
               xin, xh, xf0, xf1, za0, za1, zb0, zb1, ha, hb, yfa0, yfa1, yfb0, yfb1, ya0, ya1, sa0, sa1, yb0, yb1,
               cs, cl, ksa, kla, ksb, klb, ta, tb, wy, ws, wd, wb, ga, gd, gb,
               in_sem, w_sem, row_recv, row_send, col_recv, col_send, cor_recv, cor_send, st_recv, st_send, meet):
    rows_n, cols_n, n_img, height, width, chan = dims
    n_dev = rows_n * cols_n
    half_w, low_h = width // 2, height // 2
    line, wide = 2 * half_w, 2 * chan
    xstride = width + 2 * PAD
    fstride = half_w + 2 * PAD
    xfs, zas, zbs, yfas, yfbs, yas, sas, ybs = (xf0, xf1), (za0, za1), (zb0, zb1), (yfa0, yfa1), (yfb0, yfb1), (ya0, ya1), (sa0, sa1), (yb0, yb1)
    sp = lax.axis_index("sp")
    sp2 = lax.axis_index("sp2")
    me = sp2 * rows_n + sp
    has_up = sp > 0
    has_down = sp < rows_n - 1
    has_left = sp2 > 0
    has_right = sp2 < cols_n - 1
    row_ok = (has_up, has_down)
    col_ok = (has_left, has_right)
    cor_ok = tuple(r & c for r in row_ok for c in col_ok)

    def device(d_sp, d_sp2):
        return {"sp": sp + d_sp, "sp2": sp2 + d_sp2}

    def ring(step):
        found = []
        for d_sp in (-step, 0, step):
            for d_sp2 in (-step, 0, step):
                if (d_sp or d_sp2) and abs(d_sp2) < cols_n and abs(d_sp) < rows_n:
                    ok = (sp + d_sp >= 0) & (sp + d_sp < rows_n) & (sp2 + d_sp2 >= 0) & (sp2 + d_sp2 < cols_n)
                    found.append((ok, device(d_sp, d_sp2)))
        return found

    def call(sem, step):
        for ok, where in ring(step):
            @pl.when(ok)
            def _():
                pl.semaphore_signal(sem, inc=1, device_id=where, device_id_type=MESH)

    def hear(sem, step):
        pl.semaphore_wait(sem, sum(ok.astype(jnp.int32) for ok, where in ring(step)))

    steps = [1]
    while 2 * steps[-1] < max(rows_n, cols_n) and len(steps) < meet.shape[0]:
        steps.append(2 * steps[-1])

    def meet_again(k):
        if k < len(steps):
            hear(meet.at[k], steps[k])
        if k + 1 < len(steps):
            call(meet.at[k + 1], steps[k + 1])

    chips = rows_n // 2
    chip, core = lax.div(sp, 2), lax.rem(sp, 2)
    others = []
    for d in sorted(range(chips), key=lambda d: -min(d, chips - d)):
        at = lax.rem(chip + d, chips) * 2
        others.append((at + 1 - core, at + core))

    for i in range(n_img):
        pltpu.make_async_copy(x.at[i], xin.at[i], in_sem.at[i]).start()
    weight_copies = []
    for kx, dst, k0, n0 in ((1, wy, 0, 0), (1, wy, chan, chan), (0, wy, 0, chan), (2, wy, chan, 0), (0, ws, 0, 0), (2, ws, chan, chan)):
        weight_copies.append((w_a.at[:, :, kx], dst.at[:, :, pl.ds(k0, chan), pl.ds(n0, chan)]))
    weight_copies.append((w_down.at[:, 0], wd.at[:, 0, pl.ds(0, chan), :]))
    weight_copies.append((w_down.at[:, 1], wd.at[:, 0, pl.ds(chan, chan), :]))
    weight_copies.append((w_down.at[:, 2], wd.at[:, 1, pl.ds(chan, chan), :]))
    weight_copies.append((w_b, wb))
    weight_copies.append((bn_a, ga))
    weight_copies.append((bn_down, gd))
    weight_copies.append((bn_b, gb))
    weight_copies = [pltpu.make_async_copy(s, d, w_sem.at[k]) for k, (s, d) in enumerate(weight_copies)]
    for copy in weight_copies:
        copy.start()

    barrier = pltpu.get_barrier_semaphore()
    call(barrier, 1)

    for i in range(n_img):
        pltpu.make_async_copy(x.at[i], xin.at[i], in_sem.at[i]).wait()
    for i in range(n_img):
        for side, col0, pick in ((0, 0, 0), (1, width - 16, 15)):
            blk = xin[i, :, col0:col0 + 16, :].astype(F32)
            at = side * height * 16
            za0[i, at:at + height * 16, :] = blk.reshape(height * 16, chan)
            edge = za0[i, pl.ds(at + pick, height, stride=16), :]
            cs[0, side, i] = edge
            ksa[0, side, i] = edge[0:1]
            ksa[0, 2 + side, i] = edge[height - 1:height]

    hear(barrier, 1)

    def cor_bufs(e):
        return (ksa.at[e], kla.at[e]) if e < 4 else (ksb.at[e - 4], klb.at[e - 4])

    def start_cols(e, sides=SIDES, corners=CORNERS):
        for side in sides:
            d = -1 if side == 0 else 1

            @pl.when(col_ok[side])
            def _():
                pltpu.make_async_remote_copy(cs.at[e, side], cl.at[e, 1 - side], col_send.at[e, side], col_recv.at[e, 1 - side],
                                             device_id=device(0, d), device_id_type=MESH).start()
        src, dst = cor_bufs(e)
        for corner in corners:
            d_sp = -1 if corner < 2 else 1
            d_sp2 = -1 if corner % 2 == 0 else 1

            @pl.when(cor_ok[corner])
            def _():
                pltpu.make_async_remote_copy(src.at[corner], dst.at[3 - corner], cor_send.at[e, corner], cor_recv.at[e, 3 - corner],
                                             device_id=device(d_sp, d_sp2), device_id_type=MESH).start()

    def wait_cols(e, sides=SIDES, corners=CORNERS):
        for side in sides:
            @pl.when(col_ok[side])
            def _():
                pltpu.make_async_copy(cl.at[e, side], cl.at[e, side], col_recv.at[e, side]).wait()
        src, dst = cor_bufs(e)
        for corner in corners:
            @pl.when(cor_ok[corner])
            def _():
                pltpu.make_async_copy(dst.at[corner], dst.at[corner], cor_recv.at[e, corner]).wait()

    def wait_col_sends(e, sides=SIDES, corners=CORNERS):
        for side in sides:
            @pl.when(col_ok[side])
            def _():
                pltpu.make_async_copy(cs.at[e, side], cs.at[e, side], col_send.at[e, side]).wait()
        src, dst = cor_bufs(e)
        for corner in corners:
            @pl.when(cor_ok[corner])
            def _():
                pltpu.make_async_copy(src.at[corner], src.at[corner], cor_send.at[e, corner]).wait()

    def row_landing(e, side):
        if e == 0:
            return xh.at[side]
        return ha.at[e - 1, side] if e < 4 else hb.at[e - 4, side]

    def row_source(e, side, i):
        if e == 0:
            return xin.at[i, 0 if side == 0 else height - 1]
        src, n_rows = (zas[(e - 1) % 2], height) if e < 4 else (zbs[e % 2], low_h)
        return src.at[i, pl.ds(0 if side == 0 else (n_rows - 1) * line, line)]

    def send_rows(e, sides, images, cond=True):
        for side in sides:
            @pl.when(row_ok[side] & cond)
            def _():
                for i in images:
                    pltpu.make_async_remote_copy(row_source(e, side, i), row_landing(e, 1 - side).at[i], row_send.at[e, side, i],
                                                 row_recv.at[e, 1 - side, i], device_id=device(-1 if side == 0 else 1, 0),
                                                 device_id_type=MESH).start()

    def wait_rows(e, sides, images, cond=True):
        for side in sides:
            @pl.when(row_ok[side] & cond)
            def _():
                for i in images:
                    ref = row_landing(e, side).at[i]
                    pltpu.make_async_copy(ref, ref, row_recv.at[e, side, i]).wait()

    def wait_row_sends(e, sides=SIDES):
        for side in sides:
            @pl.when(row_ok[side])
            def _():
                ref = row_landing(e, side)

                def one(i, carry):
                    pltpu.make_async_copy(ref.at[i], ref.at[i], row_send.at[e, side, i]).wait()
                    return carry

                lax.fori_loop(0, n_img, one, 0)

    def sums_refs(e):
        return ta.at[e] if e < 3 else tb.at[e - 3]

    def start_sums(e, part):
        buf = sums_refs(e)
        buf[me] = part

        def send(to_sp, to_sp2):
            pltpu.make_async_remote_copy(buf.at[me], buf.at[me], st_send.at[e], st_recv.at[e], device_id={"sp": to_sp, "sp2": to_sp2},
                                         device_id_type=MESH).start()

        for k, pair in enumerate(others):
            def send_file(t, carry, pair=pair):
                to_sp2 = lax.rem(sp2 + cols_n // 2 + lax.select(lax.rem(t, 2) == 0, lax.div(t + 1, 2), -lax.div(t + 1, 2)), cols_n)
                for to_sp in pair:
                    send(to_sp, to_sp2)
                return carry

            lax.fori_loop(0, cols_n if k + 1 < len(others) else cols_n - 1, send_file, 0)
        send(others[-1][0], sp2)

    def finish_sums(e, num_pos):
        buf = sums_refs(e)
        rest = buf.at[pl.ds(0, n_dev - 1)]
        pltpu.make_async_copy(rest, rest, st_recv.at[e]).wait()
        total = jnp.sum(buf[...], axis=0) * (1.0 / num_pos)
        lines = total.shape[0] // 2
        mean = total[0:lines]
        var = total[lines:] - mean * mean
        return mean, lax.rsqrt(var + EPS)

    def bn(z, par):
        mean, inv, gain, shift = par
        return jnp.maximum(gain * (z - mean) * inv + shift, 0.0)

    def keep(cond, val):
        return jnp.where(cond, val, 0.0)

    def prep_x(i, k):
        xf, ya, sa = xfs[k], yas[k], sas[k]
        last = height + 1
        for r in range(height):
            xf[pl.ds((r + 1) * xstride + PAD, width), :] = xin[i, r].astype(F32)
        xf[pl.ds(PAD, width), :] = keep(has_up, xh[0, i].astype(F32))
        xf[pl.ds(last * xstride + PAD, width), :] = keep(has_down, xh[1, i].astype(F32))
        xf[pl.ds(xstride + PAD - 1, height, stride=xstride), :] = keep(has_left, cl[0, 0, i])
        xf[pl.ds(xstride + PAD + width, height, stride=xstride), :] = keep(has_right, cl[0, 1, i])
        for corner in CORNERS:
            row = 0 if corner < 2 else last
            col = PAD - 1 if corner % 2 == 0 else PAD + width
            xf[row * xstride + col:row * xstride + col + 1, :] = keep(cor_ok[corner], kla[0, corner, i])
        for r in range(height + 2):
            base = r * xstride + PAD
            even = xf[pl.ds(base, half_w, stride=2), :]
            odd = xf[pl.ds(base + 1, half_w, stride=2), :]
            before = xf[pl.ds(base - 1, half_w, stride=2), :]
            after = xf[pl.ds(base + 2, half_w, stride=2), :]
            ya[r] = jnp.concatenate([even, odd], axis=1).astype(BF16)
            sa[r] = jnp.concatenate([before, after], axis=1).astype(BF16)

    def norm_a(e, par, i, k, up=True):
        za, yfa, ya, sa = zas[(e - 1) % 2], yfas[k], yas[k], sas[k]
        last = height + 1
        lo = 0 if up else 1
        for r in range(lo, height + 2):
            if r == 0:
                val = keep(has_up, bn(ha[e - 1, 0, i], par))
            elif r == last:
                val = keep(has_down, bn(ha[e - 1, 1, i], par))
            else:
                val = bn(za[i, pl.ds((r - 1) * line, line), :], par)
            base = r * 2 * fstride + PAD
            yfa[base:base + half_w, :] = val[0:half_w]
            yfa[base + fstride:base + fstride + half_w, :] = val[half_w:]
        if up:
            yfa[pl.ds(3 * fstride + PAD - 1, height, stride=2 * fstride), :] = keep(has_left, bn(cl[e, 0, i], par))
        yfa[pl.ds(2 * fstride + PAD + half_w, height, stride=2 * fstride), :] = keep(has_right, bn(cl[e, 1, i], par))
        for corner in CORNERS if up else (3,):
            row = 0 if corner < 2 else last
            at = row * 2 * fstride + (fstride + PAD - 1 if corner % 2 == 0 else PAD + half_w)
            yfa[at:at + 1, :] = keep(cor_ok[corner], bn(kla[e, corner, i], par))
        for r in range(lo, height + 2):
            base = r * 2 * fstride + PAD
            even = yfa[base:base + half_w, :]
            odd = yfa[base + fstride:base + fstride + half_w, :]
            before = yfa[base + fstride - 1:base + fstride - 1 + half_w, :]
            after = yfa[base + 1:base + 1 + half_w, :]
            ya[r] = jnp.concatenate([even, odd], axis=1).astype(BF16)
            sa[r] = jnp.concatenate([before, after], axis=1).astype(BF16)

    def norm_b(e, par, i, k):
        zb, yfb, yb = zbs[e % 2], yfbs[k], ybs[k]
        last = low_h + 1
        halves = [tuple(p[h:h + 1] for p in par) for h in SIDES]
        tall = tuple(jnp.concatenate([p] * low_h, axis=0) for p in par)
        for r in range(low_h + 2):
            for h in SIDES:
                if r == 0:
                    val = keep(has_up, bn(hb[e - 4, 0, i, pl.ds(h * half_w, half_w), :], halves[h]))
                elif r == last:
                    val = keep(has_down, bn(hb[e - 4, 1, i, pl.ds(h * half_w, half_w), :], halves[h]))
                else:
                    val = bn(zb[i, pl.ds(((r - 1) * 2 + h) * half_w, half_w), :], halves[h])
                base = (r * 2 + h) * fstride + PAD
                yfb[base:base + half_w, :] = val
        yfb[pl.ds(2 * fstride + PAD - 1, 2 * low_h, stride=fstride), :] = keep(has_left, bn(cl[e, 0, i], tall))
        yfb[pl.ds(2 * fstride + PAD + half_w, 2 * low_h, stride=fstride), :] = keep(has_right, bn(cl[e, 1, i], tall))
        for corner in CORNERS:
            row = 0 if corner < 2 else last
            val = keep(cor_ok[corner], bn(klb[e - 4, corner, i], par))
            for h in SIDES:
                at = (row * 2 + h) * fstride + (PAD - 1 if corner % 2 == 0 else PAD + half_w)
                yfb[at:at + 1, :] = val[h:h + 1]
        for r in range(low_h + 2):
            base = r * 2 * fstride + PAD
            for kx in TAPS:
                at = base + kx - 1
                yb[kx, r] = jnp.concatenate([yfb[at:at + half_w, :], yfb[at + fstride:at + fstride + half_w, :]], axis=1).astype(BF16)

    def add_sums(acc, carry):
        tiles = acc.reshape(acc.shape[0] // 8, 8, acc.shape[1])
        return carry[0] + jnp.sum(tiles, axis=0), carry[1] + jnp.sum(tiles * tiles, axis=0)

    zero_sums = (jnp.zeros((8, wide), F32), jnp.zeros((8, wide), F32))

    def edges_a(e, i):
        za = zas[(e - 1) % 2]
        first = za[i, pl.ds(0, height, stride=line), :]
        final = za[i, pl.ds(line - 1, height, stride=line), :]
        for side, edge in enumerate((first, final)):
            cs[e, side, i] = edge
            ksa[e, side, i] = edge[0:1]
            ksa[e, 2 + side, i] = edge[height - 1:height]

    def edges_b(e, i):
        zb = zbs[e % 2]
        first = zb[i, pl.ds(0, 2 * low_h, stride=half_w), :]
        final = zb[i, pl.ds(half_w - 1, 2 * low_h, stride=half_w), :]
        for side, edge in enumerate((first, final)):
            cs[e, side, i] = edge
            ksb[e - 4, side, i] = edge[0:2]
            ksb[e - 4, 2 + side, i] = edge[2 * low_h - 2:2 * low_h]

    def store_z(ref, i, acc, rows):
        for r in range(rows):
            at = r * line
            ref[i, at:at + half_w, :] = acc[r * half_w:(r + 1) * half_w, 0:chan]
            ref[i, at + half_w:at + line, :] = acc[r * half_w:(r + 1) * half_w, chan:wide]

    def products(pairs):
        acc = None
        for lhs, w in pairs:
            d = jnp.dot(lhs, w, preferred_element_type=F32)
            acc = d if acc is None else acc + d
        return acc

    def conv_a(layer, i, k, carry):
        pairs = []
        for ky in TAPS:
            for ref, w in ((yas[k], wy), (sas[k], ws)):
                pairs.append((ref[ky:ky + height].reshape(height * half_w, wide), w[layer, ky]))
        acc = products(pairs)
        store_z(zas[layer % 2], i, acc, height)
        edges_a(layer + 1, i)
        return add_sums(acc, carry)

    def conv_down(i, k, carry):
        pairs = []
        for ky in TAPS:
            for part, ref in enumerate((yas[k], sas[k])):
                pairs.append((jnp.concatenate([ref[1 + 2 * r + ky] for r in range(low_h)], axis=0), wd[ky, part]))
        acc = products(pairs)
        store_z(zbs[0], i, acc, low_h)
        edges_b(4, i)
        return add_sums(acc, carry)

    def conv_b(layer, i, k, carry):
        pairs = []
        for ky in TAPS:
            for kx in TAPS:
                pairs.append((ybs[k][kx, ky:ky + low_h].reshape(low_h * half_w, wide), wb[layer, ky, kx]))
        acc = products(pairs)
        if layer == 0:
            store_z(zb1, i, acc, low_h)
            edges_b(5, i)
        else:
            zo[i] = acc.reshape(low_h, half_w, wide)
        return add_sums(acc, carry)

    def layer(e, prep, conv, in_sides, out_sides, early):
        wait_rows(e, in_sides, (0,))
        prep(0, 0)

        half = n_img // 2

        def pair(j, carry):
            i = 2 * j
            wait_rows(e, in_sides, (i + 1, i + 2))
            for u in SIDES:
                prep(i + u + 1, 1 - u)
                carry = conv(i + u, u, carry)
            send_rows(e + 1, out_sides, (i, i + 1), i < early)
            return carry

        carry = lax.fori_loop(0, half // 2, pair, zero_sums)
        wait_rows(e, in_sides, range(half + 1, n_img))
        if e == 0:
            meet_again(1)
        for i in range(half, n_img):
            if i + 1 < n_img:
                prep(i + 1, (i + 1) % 2)
            carry = conv(i, i % 2, carry)
        s1, s2 = carry
        s1, s2 = (jnp.sum(s, axis=0, keepdims=True) for s in (s1, s2))
        if e < 3:
            part = [s1[:, 0:chan] + s1[:, chan:], s2[:, 0:chan] + s2[:, chan:]]
        else:
            part = [s1[:, 0:chan], s1[:, chan:], s2[:, 0:chan], s2[:, chan:]]
        if e == 0:
            for k in range(2, len(steps)):
                meet_again(k)
        start_sums(e, jnp.concatenate(part, axis=0))
        if e < 5:
            both = len(out_sides) == 2
            start_cols(e + 1, SIDES if both else (0,), CORNERS if both else (0,))
            send_rows(e + 1, out_sides, range(early, n_img))

    start_cols(0)
    send_rows(0, SIDES, range(n_img))
    call(meet.at[0], steps[0])
    zeros = jnp.zeros((chan, chan), BF16)
    for depth in TAPS:
        for ky in TAPS:
            ws[depth, ky, 0:chan, chan:wide] = zeros
            ws[depth, ky, chan:wide, 0:chan] = zeros
    for ky in TAPS:
        wd[ky, 1, 0:chan, :] = jnp.zeros((chan, wide), BF16)
    for copy in weight_copies[:6]:
        copy.wait()
    meet_again(0)
    wait_cols(0)

    pos_a = n_dev * n_img * height * width
    pos_b = n_dev * n_img * low_h * half_w

    def params_a(e, layer):
        mean, inv = finish_sums(e, pos_a)
        return mean, inv, ga[layer, 0:1], ga[layer, 1:2]

    def params_b(e, ref):
        mean, inv = finish_sums(e, pos_b)
        gain = jnp.concatenate([ref[0:1, 0:chan], ref[0:1, chan:]], axis=0)
        shift = jnp.concatenate([ref[1:2, 0:chan], ref[1:2, chan:]], axis=0)
        return mean, inv, gain, shift

    part = functools.partial
    layer(0, prep_x, part(conv_a, 0), SIDES, SIDES, EARLY_A)

    for copy in weight_copies[6:]:
        copy.wait()
    wait_row_sends(0)
    wait_col_sends(0)
    wait_cols(1)
    layer(1, part(norm_a, 1, params_a(0, 0)), part(conv_a, 1), SIDES, SIDES, EARLY_A)

    wait_row_sends(1)
    wait_col_sends(1)
    wait_cols(2)
    layer(2, part(norm_a, 2, params_a(1, 1)), part(conv_a, 2), SIDES, (0,), EARLY_A)

    wait_row_sends(2)
    wait_col_sends(2)
    wait_cols(3, (1,), (3,))
    layer(3, part(norm_a, 3, params_a(2, 2), up=False), conv_down, (1,), SIDES, EARLY_B)

    wait_row_sends(3, (0,))
    wait_col_sends(3, (0,), (0,))
    wait_cols(4)
    layer(4, part(norm_b, 4, params_b(3, gd)), part(conv_b, 0), SIDES, SIDES, EARLY_B)

    wait_row_sends(4)
    wait_col_sends(4)
    wait_cols(5)
    layer(5, part(norm_b, 5, params_b(4, gb.at[0])), part(conv_b, 1), SIDES, (), 0)

    wait_row_sends(5)
    wait_col_sends(5)
    mean, inv = finish_sums(5, pos_b)
    for out, val in ((mean_o, mean), (inv_o, inv)):
        for h in SIDES:
            out[:, h * chan:(h + 1) * chan] = val[h:h + 1]
    gain_o[...] = gb[1, 0:1]
    shift_o[...] = gb[1, 1:2]

    for e in range(6):
        buf = sums_refs(e)
        rest = buf.at[pl.ds(0, n_dev - 1)]
        pltpu.make_async_copy(rest, rest, st_send.at[e]).wait()


def net(rows_n, cols_n, x, w_a, bn_a, w_down, bn_down, w_b, bn_b):
    n_img, height, width, chan = x.shape
    half_w, low_h = width // 2, height // 2
    n_dev = rows_n * cols_n
    vmem, dma = pltpu.VMEM, pltpu.SemaphoreType.DMA
    line, wide = 2 * half_w, 2 * chan
    plane = half_w + 2 * PAD
    a_sums, b_sums = 3, 3
    n_ex = a_sums + b_sums
    two, corners = len(SIDES), len(CORNERS)
    scratch = [
        vmem(x.shape, BF16),
        vmem((two, n_img, width, chan), BF16),
        *[vmem(((height + 2) * (width + 2 * PAD), chan), F32)] * two,
        *[vmem((n_img, height * line, chan), F32)] * two,
        *[vmem((n_img, low_h * line, chan), F32)] * two,
        vmem((a_sums, two, n_img, line, chan), F32),
        vmem((b_sums - 1, two, n_img, line, chan), F32),
        *[vmem(((height + 2) * 2 * plane, chan), F32)] * two,
        *[vmem(((low_h + 2) * 2 * plane, chan), F32)] * two,
        *[vmem((height + 2, half_w, wide), BF16)] * 4,
        *[vmem((3, low_h + 2, half_w, wide), BF16)] * two,
        *[vmem((n_ex, two, n_img, height, chan), F32)] * two,
        *[vmem((a_sums + 1, corners, n_img, 1, chan), F32)] * two,
        *[vmem((b_sums - 1, corners, n_img, 2, chan), F32)] * two,
        vmem((a_sums, n_dev, 2, chan), F32),
        vmem((b_sums, n_dev, 4, chan), F32),
        *[vmem((a_sums, 3, wide, wide), BF16)] * two,
        vmem((3, two, wide, wide), BF16),
        vmem(w_b.shape, BF16),
        vmem(bn_a.shape, F32),
        vmem(bn_down.shape, F32),
        vmem(bn_b.shape, F32),
        dma((n_img,)),
        dma((13,)),
        *[dma((n_ex, two, n_img))] * two,
        *[dma((n_ex, two))] * two,
        *[dma((n_ex, corners))] * two,
        *[dma((n_ex,))] * two,
        pltpu.SemaphoreType.REGULAR((3,)),
    ]
    hbm_spec = pl.BlockSpec(memory_space=pltpu.HBM)
    line_out = jax.ShapeDtypeStruct((1, wide), F32)
    z, *vectors = pl.pallas_call(
        functools.partial(net_kernel, (rows_n, cols_n, n_img, height, width, chan)),
        out_shape=(jax.ShapeDtypeStruct((n_img, low_h, half_w, wide), F32),) + (line_out,) * 4,
        in_specs=[hbm_spec] * 7,
        out_specs=(pl.BlockSpec(memory_space=pltpu.VMEM),) * 5,
        scratch_shapes=scratch,
        compiler_params=pltpu.CompilerParams(collective_id=0, has_side_effects=True, vmem_limit_bytes=40 * 1024 * 1024),
        name="conv_bn_net",
    )(*[pltpu.with_memory_space_constraint(arg, pltpu.HBM) for arg in (x, w_a, bn_a, w_down, bn_down, w_b, bn_b)])
    mean, inv, gain, shift = [v.reshape(wide) for v in vectors]
    return jnp.maximum(gain * (z - mean) * inv + shift, 0.0).astype(BF16)


def solution(mesh):
    tile_spec = P("dp", "sp", "sp2", None)
    per_device = functools.partial(net, mesh.shape["sp"], mesh.shape["sp2"])
    return jax.shard_map(per_device, mesh=mesh, in_specs=(tile_spec, P(), P(), P(), P(), P(), P()), out_specs=tile_spec, check_vma=False)
```

```python
import functools

import jax
import jax.numpy as jnp
from jax import lax
from jax.experimental import pallas as pl
from jax.experimental.pallas import tpu as pltpu
from jax.sharding import PartitionSpec as P

MESH = pl.DeviceIdType.MESH
F32 = jnp.float32
BF16 = jnp.bfloat16
EPS = 1e-5
PAD = 8
SIDES = (0, 1)
CORNERS = (0, 1, 2, 3)
TAPS = range(3)
EARLY_A = 3
EARLY_B = 3


def net_kernel(dims, x, w_a, bn_a, w_down, bn_down, w_b, bn_b, zo, mean_o, inv_o, gain_o, shift_o,
               xin, xh, xf0, xf1, za0, za1, zb0, zb1, ha, hb, yfa0, yfa1, yfb0, yfb1, ya0, ya1, sa0, sa1, yb0, yb1,
               cs, cl, ksa, kla, ksb, klb, ta, tb, wy, ws, wd, wb, ga, gd, gb,
               in_sem, w_sem, row_recv, row_send, col_recv, col_send, cor_recv, cor_send, st_recv, st_send, meet):
    rows_n, cols_n, n_img, height, width, chan = dims
    n_dev = rows_n * cols_n
    half_w, low_h = width // 2, height // 2
    line, wide = 2 * half_w, 2 * chan
    xstride = width + 2 * PAD
    fstride = half_w + 2 * PAD
    xfs, zas, zbs, yfas, yfbs, yas, sas, ybs = (xf0, xf1), (za0, za1), (zb0, zb1), (yfa0, yfa1), (yfb0, yfb1), (ya0, ya1), (sa0, sa1), (yb0, yb1)
    sp = lax.axis_index("sp")
    sp2 = lax.axis_index("sp2")
    me = sp2 * rows_n + sp
    has_up = sp > 0
    has_down = sp < rows_n - 1
    has_left = sp2 > 0
    has_right = sp2 < cols_n - 1
    row_ok = (has_up, has_down)
    col_ok = (has_left, has_right)
    cor_ok = tuple(r & c for r in row_ok for c in col_ok)

    def device(d_sp, d_sp2):
        return {"sp": sp + d_sp, "sp2": sp2 + d_sp2}

    def ring(step):
        found = []
        for d_sp in (-step, 0, step):
            for d_sp2 in (-step, 0, step):
                if (d_sp or d_sp2) and abs(d_sp2) < cols_n and abs(d_sp) < rows_n:
                    ok = (sp + d_sp >= 0) & (sp + d_sp < rows_n) & (sp2 + d_sp2 >= 0) & (sp2 + d_sp2 < cols_n)
                    found.append((ok, device(d_sp, d_sp2)))
        return found

    def call(sem, step):
        for ok, where in ring(step):
            @pl.when(ok)
            def _():
                pl.semaphore_signal(sem, inc=1, device_id=where, device_id_type=MESH)

    def hear(sem, step):
        pl.semaphore_wait(sem, sum(ok.astype(jnp.int32) for ok, where in ring(step)))

    steps = [1]
    while 2 * steps[-1] < max(rows_n, cols_n) and len(steps) < meet.shape[0]:
        steps.append(2 * steps[-1])

    def meet_again(k):
        if k < len(steps):
            hear(meet.at[k], steps[k])
        if k + 1 < len(steps):
            call(meet.at[k + 1], steps[k + 1])

    chips = rows_n // 2
    chip, core = lax.div(sp, 2), lax.rem(sp, 2)
    others = []
    for d in sorted(range(chips), key=lambda d: -min(d, chips - d)):
        at = lax.rem(chip + d, chips) * 2
        others.append((at + 1 - core, at + core))

    for i in range(n_img):
        pltpu.make_async_copy(x.at[i], xin.at[i], in_sem.at[i]).start()
    weight_copies = []
    for kx, dst, k0, n0 in ((1, wy, 0, 0), (1, wy, chan, chan), (0, wy, 0, chan), (2, wy, chan, 0), (0, ws, 0, 0), (2, ws, chan, chan)):
        weight_copies.append((w_a.at[:, :, kx], dst.at[:, :, pl.ds(k0, chan), pl.ds(n0, chan)]))
    weight_copies.append((w_down.at[:, 0], wd.at[:, 0, pl.ds(0, chan), :]))
    weight_copies.append((w_down.at[:, 1], wd.at[:, 0, pl.ds(chan, chan), :]))
    weight_copies.append((w_down.at[:, 2], wd.at[:, 1, pl.ds(chan, chan), :]))
    weight_copies.append((w_b, wb))
    weight_copies.append((bn_a, ga))
    weight_copies.append((bn_down, gd))
    weight_copies.append((bn_b, gb))
    weight_copies = [pltpu.make_async_copy(s, d, w_sem.at[k]) for k, (s, d) in enumerate(weight_copies)]
    for copy in weight_copies:
        copy.start()

    barrier = pltpu.get_barrier_semaphore()
    call(barrier, 1)

    for i in range(n_img):
        pltpu.make_async_copy(x.at[i], xin.at[i], in_sem.at[i]).wait()
    for i in range(n_img):
        for side, col0, pick in ((0, 0, 0), (1, width - 16, 15)):
            blk = xin[i, :, col0:col0 + 16, :].astype(F32)
            at = side * height * 16
            za0[i, at:at + height * 16, :] = blk.reshape(height * 16, chan)
            edge = za0[i, pl.ds(at + pick, height, stride=16), :]
            cs[0, side, i] = edge
            ksa[0, side, i] = edge[0:1]
            ksa[0, 2 + side, i] = edge[height - 1:height]

    hear(barrier, 1)

    def cor_bufs(e):
        return (ksa.at[e], kla.at[e]) if e < 4 else (ksb.at[e - 4], klb.at[e - 4])

    def start_cols(e, sides=SIDES, corners=CORNERS):
        for side in sides:
            d = -1 if side == 0 else 1

            @pl.when(col_ok[side])
            def _():
                pltpu.make_async_remote_copy(cs.at[e, side], cl.at[e, 1 - side], col_send.at[e, side], col_recv.at[e, 1 - side],
                                             device_id=device(0, d), device_id_type=MESH).start()
        src, dst = cor_bufs(e)
        for corner in corners:
            d_sp = -1 if corner < 2 else 1
            d_sp2 = -1 if corner % 2 == 0 else 1

            @pl.when(cor_ok[corner])
            def _():
                pltpu.make_async_remote_copy(src.at[corner], dst.at[3 - corner], cor_send.at[e, corner], cor_recv.at[e, 3 - corner],
                                             device_id=device(d_sp, d_sp2), device_id_type=MESH).start()

    def wait_cols(e, sides=SIDES, corners=CORNERS):
        for side in sides:
            @pl.when(col_ok[side])
            def _():
                pltpu.make_async_copy(cl.at[e, side], cl.at[e, side], col_recv.at[e, side]).wait()
        src, dst = cor_bufs(e)
        for corner in corners:
            @pl.when(cor_ok[corner])
            def _():
                pltpu.make_async_copy(dst.at[corner], dst.at[corner], cor_recv.at[e, corner]).wait()

    def wait_col_sends(e, sides=SIDES, corners=CORNERS):
        for side in sides:
            @pl.when(col_ok[side])
            def _():
                pltpu.make_async_copy(cs.at[e, side], cs.at[e, side], col_send.at[e, side]).wait()
        src, dst = cor_bufs(e)
        for corner in corners:
            @pl.when(cor_ok[corner])
            def _():
                pltpu.make_async_copy(src.at[corner], src.at[corner], cor_send.at[e, corner]).wait()

    def row_landing(e, side):
        if e == 0:
            return xh.at[side]
        return ha.at[e - 1, side] if e < 4 else hb.at[e - 4, side]

    def row_source(e, side, i):
        if e == 0:
            return xin.at[i, 0 if side == 0 else height - 1]
        src, n_rows = (zas[(e - 1) % 2], height) if e < 4 else (zbs[e % 2], low_h)
        return src.at[i, pl.ds(0 if side == 0 else (n_rows - 1) * line, line)]

    def send_rows(e, sides, images, cond=True):
        for side in sides:
            @pl.when(row_ok[side] & cond)
            def _():
                for i in images:
                    pltpu.make_async_remote_copy(row_source(e, side, i), row_landing(e, 1 - side).at[i], row_send.at[e, side, i],
                                                 row_recv.at[e, 1 - side, i], device_id=device(-1 if side == 0 else 1, 0),
                                                 device_id_type=MESH).start()

    def wait_rows(e, sides, images, cond=True):
        for side in sides:
            @pl.when(row_ok[side] & cond)
            def _():
                for i in images:
                    ref = row_landing(e, side).at[i]
                    pltpu.make_async_copy(ref, ref, row_recv.at[e, side, i]).wait()

    def wait_row_sends(e, sides=SIDES):
        for side in sides:
            @pl.when(row_ok[side])
            def _():
                ref = row_landing(e, side)

                def one(i, carry):
                    pltpu.make_async_copy(ref.at[i], ref.at[i], row_send.at[e, side, i]).wait()
                    return carry

                lax.fori_loop(0, n_img, one, 0)

    def sums_refs(e):
        return ta.at[e] if e < 3 else tb.at[e - 3]

    def start_sums(e, part):
        buf = sums_refs(e)
        buf[me] = part

        def send(to_sp, to_sp2):
            pltpu.make_async_remote_copy(buf.at[me], buf.at[me], st_send.at[e], st_recv.at[e], device_id={"sp": to_sp, "sp2": to_sp2},
                                         device_id_type=MESH).start()

        for k, pair in enumerate(others):
            def send_file(t, carry, pair=pair):
                to_sp2 = lax.rem(sp2 + cols_n // 2 + lax.select(lax.rem(t, 2) == 0, lax.div(t + 1, 2), -lax.div(t + 1, 2)), cols_n)
                for to_sp in pair:
                    send(to_sp, to_sp2)
                return carry

            lax.fori_loop(0, cols_n if k + 1 < len(others) else cols_n - 1, send_file, 0)
        send(others[-1][0], sp2)

    def finish_sums(e, num_pos):
        buf = sums_refs(e)
        rest = buf.at[pl.ds(0, n_dev - 1)]
        pltpu.make_async_copy(rest, rest, st_recv.at[e]).wait()
        total = jnp.sum(buf[...], axis=0) * (1.0 / num_pos)
        lines = total.shape[0] // 2
        mean = total[0:lines]
        var = total[lines:] - mean * mean
        return mean, lax.rsqrt(var + EPS)

    def bn(z, par):
        mean, inv, gain, shift = par
        return jnp.maximum(gain * (z - mean) * inv + shift, 0.0)

    def keep(cond, val):
        return jnp.where(cond, val, 0.0)

    def prep_x(i, k):
        xf, ya, sa = xfs[k], yas[k], sas[k]
        last = height + 1
        for r in range(height):
            xf[pl.ds((r + 1) * xstride + PAD, width), :] = xin[i, r].astype(F32)
        xf[pl.ds(PAD, width), :] = keep(has_up, xh[0, i].astype(F32))
        xf[pl.ds(last * xstride + PAD, width), :] = keep(has_down, xh[1, i].astype(F32))
        xf[pl.ds(xstride + PAD - 1, height, stride=xstride), :] = keep(has_left, cl[0, 0, i])
        xf[pl.ds(xstride + PAD + width, height, stride=xstride), :] = keep(has_right, cl[0, 1, i])
        for corner in CORNERS:
            row = 0 if corner < 2 else last
            col = PAD - 1 if corner % 2 == 0 else PAD + width
            xf[row * xstride + col:row * xstride + col + 1, :] = keep(cor_ok[corner], kla[0, corner, i])
        for r in range(height + 2):
            base = r * xstride + PAD
            even = xf[pl.ds(base, half_w, stride=2), :]
            odd = xf[pl.ds(base + 1, half_w, stride=2), :]
            before = xf[pl.ds(base - 1, half_w, stride=2), :]
            after = xf[pl.ds(base + 2, half_w, stride=2), :]
            ya[r] = jnp.concatenate([even, odd], axis=1).astype(BF16)
            sa[r] = jnp.concatenate([before, after], axis=1).astype(BF16)

    def norm_a(e, par, i, k, up=True):
        za, yfa, ya, sa = zas[(e - 1) % 2], yfas[k], yas[k], sas[k]
        last = height + 1
        lo = 0 if up else 1
        for r in range(lo, height + 2):
            if r == 0:
                val = keep(has_up, bn(ha[e - 1, 0, i], par))
            elif r == last:
                val = keep(has_down, bn(ha[e - 1, 1, i], par))
            else:
                val = bn(za[i, pl.ds((r - 1) * line, line), :], par)
            base = r * 2 * fstride + PAD
            yfa[base:base + half_w, :] = val[0:half_w]
            yfa[base + fstride:base + fstride + half_w, :] = val[half_w:]
        if up:
            yfa[pl.ds(3 * fstride + PAD - 1, height, stride=2 * fstride), :] = keep(has_left, bn(cl[e, 0, i], par))
        yfa[pl.ds(2 * fstride + PAD + half_w, height, stride=2 * fstride), :] = keep(has_right, bn(cl[e, 1, i], par))
        for corner in CORNERS if up else (3,):
            row = 0 if corner < 2 else last
            at = row * 2 * fstride + (fstride + PAD - 1 if corner % 2 == 0 else PAD + half_w)
            yfa[at:at + 1, :] = keep(cor_ok[corner], bn(kla[e, corner, i], par))
        for r in range(lo, height + 2):
            base = r * 2 * fstride + PAD
            even = yfa[base:base + half_w, :]
            odd = yfa[base + fstride:base + fstride + half_w, :]
            before = yfa[base + fstride - 1:base + fstride - 1 + half_w, :]
            after = yfa[base + 1:base + 1 + half_w, :]
            ya[r] = jnp.concatenate([even, odd], axis=1).astype(BF16)
            sa[r] = jnp.concatenate([before, after], axis=1).astype(BF16)

    def norm_b(e, par, i, k):
        zb, yfb, yb = zbs[e % 2], yfbs[k], ybs[k]
        last = low_h + 1
        halves = [tuple(p[h:h + 1] for p in par) for h in SIDES]
        tall = tuple(jnp.concatenate([p] * low_h, axis=0) for p in par)
        for r in range(low_h + 2):
            for h in SIDES:
                if r == 0:
                    val = keep(has_up, bn(hb[e - 4, 0, i, pl.ds(h * half_w, half_w), :], halves[h]))
                elif r == last:
                    val = keep(has_down, bn(hb[e - 4, 1, i, pl.ds(h * half_w, half_w), :], halves[h]))
                else:
                    val = bn(zb[i, pl.ds(((r - 1) * 2 + h) * half_w, half_w), :], halves[h])
                base = (r * 2 + h) * fstride + PAD
                yfb[base:base + half_w, :] = val
        yfb[pl.ds(2 * fstride + PAD - 1, 2 * low_h, stride=fstride), :] = keep(has_left, bn(cl[e, 0, i], tall))
        yfb[pl.ds(2 * fstride + PAD + half_w, 2 * low_h, stride=fstride), :] = keep(has_right, bn(cl[e, 1, i], tall))
        for corner in CORNERS:
            row = 0 if corner < 2 else last
            val = keep(cor_ok[corner], bn(klb[e - 4, corner, i], par))
            for h in SIDES:
                at = (row * 2 + h) * fstride + (PAD - 1 if corner % 2 == 0 else PAD + half_w)
                yfb[at:at + 1, :] = val[h:h + 1]
        for r in range(low_h + 2):
            base = r * 2 * fstride + PAD
            for kx in TAPS:
                at = base + kx - 1
                yb[kx, r] = jnp.concatenate([yfb[at:at + half_w, :], yfb[at + fstride:at + fstride + half_w, :]], axis=1).astype(BF16)

    def add_sums(acc, carry):
        tiles = acc.reshape(acc.shape[0] // 8, 8, acc.shape[1])
        return carry[0] + jnp.sum(tiles, axis=0), carry[1] + jnp.sum(tiles * tiles, axis=0)

    zero_sums = (jnp.zeros((8, wide), F32), jnp.zeros((8, wide), F32))

    def edges_a(e, i):
        za = zas[(e - 1) % 2]
        first = za[i, pl.ds(0, height, stride=line), :]
        final = za[i, pl.ds(line - 1, height, stride=line), :]
        for side, edge in enumerate((first, final)):
            cs[e, side, i] = edge
            ksa[e, side, i] = edge[0:1]
            ksa[e, 2 + side, i] = edge[height - 1:height]

    def edges_b(e, i):
        zb = zbs[e % 2]
        first = zb[i, pl.ds(0, 2 * low_h, stride=half_w), :]
        final = zb[i, pl.ds(half_w - 1, 2 * low_h, stride=half_w), :]
        for side, edge in enumerate((first, final)):
            cs[e, side, i] = edge
            ksb[e - 4, side, i] = edge[0:2]
            ksb[e - 4, 2 + side, i] = edge[2 * low_h - 2:2 * low_h]

    def store_z(ref, i, acc, rows):
        for r in range(rows):
            at = r * line
            ref[i, at:at + half_w, :] = acc[r * half_w:(r + 1) * half_w, 0:chan]
            ref[i, at + half_w:at + line, :] = acc[r * half_w:(r + 1) * half_w, chan:wide]

    def products(pairs):
        acc = None
        for lhs, w in pairs:
            d = jnp.dot(lhs, w, preferred_element_type=F32)
            acc = d if acc is None else acc + d
        return acc

    def conv_a(layer, i, k, carry):
        pairs = []
        for ky in TAPS:
            for ref, w in ((yas[k], wy), (sas[k], ws)):
                pairs.append((ref[ky:ky + height].reshape(height * half_w, wide), w[layer, ky]))
        acc = products(pairs)
        store_z(zas[layer % 2], i, acc, height)
        edges_a(layer + 1, i)
        return add_sums(acc, carry)

    def conv_down(i, k, carry):
        pairs = []
        for ky in TAPS:
            for part, ref in enumerate((yas[k], sas[k])):
                pairs.append((jnp.concatenate([ref[1 + 2 * r + ky] for r in range(low_h)], axis=0), wd[ky, part]))
        acc = products(pairs)
        store_z(zbs[0], i, acc, low_h)
        edges_b(4, i)
        return add_sums(acc, carry)

    def conv_b(layer, i, k, carry):
        pairs = []
        for ky in TAPS:
            for kx in TAPS:
                pairs.append((ybs[k][kx, ky:ky + low_h].reshape(low_h * half_w, wide), wb[layer, ky, kx]))
        acc = products(pairs)
        if layer == 0:
            store_z(zb1, i, acc, low_h)
            edges_b(5, i)
        else:
            zo[i] = acc.reshape(low_h, half_w, wide)
        return add_sums(acc, carry)

    def layer(e, prep, conv, in_sides, out_sides, early):
        wait_rows(e, in_sides, (0,))
        prep(0, 0)

        half = n_img // 2

        def pair(j, carry):
            i = 2 * j
            wait_rows(e, in_sides, (i + 1, i + 2))
            for u in SIDES:
                prep(i + u + 1, 1 - u)
                carry = conv(i + u, u, carry)
            for u in SIDES:
                send_rows(e + 1, out_sides, (i + u,), i + u < early)
            return carry

        carry = lax.fori_loop(0, half // 2, pair, zero_sums)
        wait_rows(e, in_sides, range(half + 1, n_img))
        if e == 0:
            meet_again(1)
        for i in range(half, n_img):
            if i + 1 < n_img:
                prep(i + 1, (i + 1) % 2)
            carry = conv(i, i % 2, carry)
        s1, s2 = carry
        s1, s2 = (jnp.sum(s, axis=0, keepdims=True) for s in (s1, s2))
        if e < 3:
            part = [s1[:, 0:chan] + s1[:, chan:], s2[:, 0:chan] + s2[:, chan:]]
        else:
            part = [s1[:, 0:chan], s1[:, chan:], s2[:, 0:chan], s2[:, chan:]]
        if e == 0:
            for k in range(2, len(steps)):
                meet_again(k)
        start_sums(e, jnp.concatenate(part, axis=0))
        if e < 5:
            both = len(out_sides) == 2
            start_cols(e + 1, SIDES if both else (0,), CORNERS if both else (0,))
            send_rows(e + 1, out_sides, range(early, n_img))

    start_cols(0)
    send_rows(0, SIDES, range(n_img))
    call(meet.at[0], steps[0])
    zeros = jnp.zeros((chan, chan), BF16)
    for depth in TAPS:
        for ky in TAPS:
            ws[depth, ky, 0:chan, chan:wide] = zeros
            ws[depth, ky, chan:wide, 0:chan] = zeros
    for ky in TAPS:
        wd[ky, 1, 0:chan, :] = jnp.zeros((chan, wide), BF16)
    for copy in weight_copies[:6]:
        copy.wait()
    meet_again(0)
    wait_cols(0)

    pos_a = n_dev * n_img * height * width
    pos_b = n_dev * n_img * low_h * half_w

    def params_a(e, layer):
        mean, inv = finish_sums(e, pos_a)
        return mean, inv, ga[layer, 0:1], ga[layer, 1:2]

    def params_b(e, ref):
        mean, inv = finish_sums(e, pos_b)
        gain = jnp.concatenate([ref[0:1, 0:chan], ref[0:1, chan:]], axis=0)
        shift = jnp.concatenate([ref[1:2, 0:chan], ref[1:2, chan:]], axis=0)
        return mean, inv, gain, shift

    part = functools.partial
    layer(0, prep_x, part(conv_a, 0), SIDES, SIDES, EARLY_A)

    for copy in weight_copies[6:]:
        copy.wait()
    wait_row_sends(0)
    wait_col_sends(0)
    wait_cols(1)
    layer(1, part(norm_a, 1, params_a(0, 0)), part(conv_a, 1), SIDES, SIDES, EARLY_A)

    wait_row_sends(1)
    wait_col_sends(1)
    wait_cols(2)
    layer(2, part(norm_a, 2, params_a(1, 1)), part(conv_a, 2), SIDES, (0,), EARLY_A)

    wait_row_sends(2)
    wait_col_sends(2)
    wait_cols(3, (1,), (3,))
    layer(3, part(norm_a, 3, params_a(2, 2), up=False), conv_down, (1,), SIDES, EARLY_B)

    wait_row_sends(3, (0,))
    wait_col_sends(3, (0,), (0,))
    wait_cols(4)
    layer(4, part(norm_b, 4, params_b(3, gd)), part(conv_b, 0), SIDES, SIDES, EARLY_B)

    wait_row_sends(4)
    wait_col_sends(4)
    wait_cols(5)
    layer(5, part(norm_b, 5, params_b(4, gb.at[0])), part(conv_b, 1), SIDES, (), 0)

    wait_row_sends(5)
    wait_col_sends(5)
    mean, inv = finish_sums(5, pos_b)
    for out, val in ((mean_o, mean), (inv_o, inv)):
        for h in SIDES:
            out[:, h * chan:(h + 1) * chan] = val[h:h + 1]
    gain_o[...] = gb[1, 0:1]
    shift_o[...] = gb[1, 1:2]

    for e in range(6):
        buf = sums_refs(e)
        rest = buf.at[pl.ds(0, n_dev - 1)]
        pltpu.make_async_copy(rest, rest, st_send.at[e]).wait()


def net(rows_n, cols_n, x, w_a, bn_a, w_down, bn_down, w_b, bn_b):
    n_img, height, width, chan = x.shape
    half_w, low_h = width // 2, height // 2
    n_dev = rows_n * cols_n
    vmem, dma = pltpu.VMEM, pltpu.SemaphoreType.DMA
    line, wide = 2 * half_w, 2 * chan
    plane = half_w + 2 * PAD
    a_sums, b_sums = 3, 3
    n_ex = a_sums + b_sums
    two, corners = len(SIDES), len(CORNERS)
    scratch = [
        vmem(x.shape, BF16),
        vmem((two, n_img, width, chan), BF16),
        *[vmem(((height + 2) * (width + 2 * PAD), chan), F32)] * two,
        *[vmem((n_img, height * line, chan), F32)] * two,
        *[vmem((n_img, low_h * line, chan), F32)] * two,
        vmem((a_sums, two, n_img, line, chan), F32),
        vmem((b_sums - 1, two, n_img, line, chan), F32),
        *[vmem(((height + 2) * 2 * plane, chan), F32)] * two,
        *[vmem(((low_h + 2) * 2 * plane, chan), F32)] * two,
        *[vmem((height + 2, half_w, wide), BF16)] * 4,
        *[vmem((3, low_h + 2, half_w, wide), BF16)] * two,
        *[vmem((n_ex, two, n_img, height, chan), F32)] * two,
        *[vmem((a_sums + 1, corners, n_img, 1, chan), F32)] * two,
        *[vmem((b_sums - 1, corners, n_img, 2, chan), F32)] * two,
        vmem((a_sums, n_dev, 2, chan), F32),
        vmem((b_sums, n_dev, 4, chan), F32),
        *[vmem((a_sums, 3, wide, wide), BF16)] * two,
        vmem((3, two, wide, wide), BF16),
        vmem(w_b.shape, BF16),
        vmem(bn_a.shape, F32),
        vmem(bn_down.shape, F32),
        vmem(bn_b.shape, F32),
        dma((n_img,)),
        dma((13,)),
        *[dma((n_ex, two, n_img))] * two,
        *[dma((n_ex, two))] * two,
        *[dma((n_ex, corners))] * two,
        *[dma((n_ex,))] * two,
        pltpu.SemaphoreType.REGULAR((3,)),
    ]
    hbm_spec = pl.BlockSpec(memory_space=pltpu.HBM)
    line_out = jax.ShapeDtypeStruct((1, wide), F32)
    z, *vectors = pl.pallas_call(
        functools.partial(net_kernel, (rows_n, cols_n, n_img, height, width, chan)),
        out_shape=(jax.ShapeDtypeStruct((n_img, low_h, half_w, wide), F32),) + (line_out,) * 4,
        in_specs=[hbm_spec] * 7,
        out_specs=(pl.BlockSpec(memory_space=pltpu.VMEM),) * 5,
        scratch_shapes=scratch,
        compiler_params=pltpu.CompilerParams(collective_id=0, has_side_effects=True, vmem_limit_bytes=40 * 1024 * 1024),
        name="conv_bn_net",
    )(*[pltpu.with_memory_space_constraint(arg, pltpu.HBM) for arg in (x, w_a, bn_a, w_down, bn_down, w_b, bn_b)])
    mean, inv, gain, shift = [v.reshape(wide) for v in vectors]
    return jnp.maximum(gain * (z - mean) * inv + shift, 0.0).astype(BF16)


def solution(mesh):
    tile_spec = P("dp", "sp", "sp2", None)
    per_device = functools.partial(net, mesh.shape["sp"], mesh.shape["sp2"])
    return jax.shard_map(per_device, mesh=mesh, in_specs=(tile_spec, P(), P(), P(), P(), P(), P()), out_specs=tile_spec, check_vma=False)
```

```python
import functools

import jax
import jax.numpy as jnp
from jax import lax
from jax.experimental import pallas as pl
from jax.experimental.pallas import tpu as pltpu
from jax.sharding import PartitionSpec as P

MESH = pl.DeviceIdType.MESH
F32 = jnp.float32
BF16 = jnp.bfloat16
EPS = 1e-5
PAD = 8
SIDES = (0, 1)
CORNERS = (0, 1, 2, 3)
TAPS = range(3)
EARLY_A = 3
EARLY_B = 3


def net_kernel(dims, x, w_a, bn_a, w_down, bn_down, w_b, bn_b, zo, mean_o, inv_o, gain_o, shift_o,
               xin, xh, xf0, xf1, za0, za1, zb0, zb1, ha, hb, yfa0, yfa1, yfb0, yfb1, ya0, ya1, sa0, sa1, yb0, yb1,
               cs, cl, ksa, kla, ksb, klb, ta, tb, wy, ws, wd, wb, ga, gd, gb,
               in_sem, w_sem, row_recv, row_send, col_recv, col_send, cor_recv, cor_send, st_recv, st_send, meet):
    rows_n, cols_n, n_img, height, width, chan = dims
    n_dev = rows_n * cols_n
    half_w, low_h = width // 2, height // 2
    line, wide = 2 * half_w, 2 * chan
    xstride = width + 2 * PAD
    fstride = half_w + 2 * PAD
    xfs, zas, zbs, yfas, yfbs, yas, sas, ybs = (xf0, xf1), (za0, za1), (zb0, zb1), (yfa0, yfa1), (yfb0, yfb1), (ya0, ya1), (sa0, sa1), (yb0, yb1)
    sp = lax.axis_index("sp")
    sp2 = lax.axis_index("sp2")
    me = sp2 * rows_n + sp
    has_up = sp > 0
    has_down = sp < rows_n - 1
    has_left = sp2 > 0
    has_right = sp2 < cols_n - 1
    row_ok = (has_up, has_down)
    col_ok = (has_left, has_right)
    cor_ok = tuple(r & c for r in row_ok for c in col_ok)

    def device(d_sp, d_sp2):
        return {"sp": sp + d_sp, "sp2": sp2 + d_sp2}

    def ring(step):
        found = []
        for d_sp in (-step, 0, step):
            for d_sp2 in (-step, 0, step):
                if (d_sp or d_sp2) and abs(d_sp2) < cols_n and abs(d_sp) < rows_n:
                    ok = (sp + d_sp >= 0) & (sp + d_sp < rows_n) & (sp2 + d_sp2 >= 0) & (sp2 + d_sp2 < cols_n)
                    found.append((ok, device(d_sp, d_sp2)))
        return found

    def call(sem, step):
        for ok, where in ring(step):
            @pl.when(ok)
            def _():
                pl.semaphore_signal(sem, inc=1, device_id=where, device_id_type=MESH)

    def hear(sem, step):
        pl.semaphore_wait(sem, sum(ok.astype(jnp.int32) for ok, where in ring(step)))

    steps = [1]
    while 2 * steps[-1] < max(rows_n, cols_n) and len(steps) < meet.shape[0]:
        steps.append(2 * steps[-1])

    def meet_again(k):
        if k < len(steps):
            hear(meet.at[k], steps[k])
        if k + 1 < len(steps):
            call(meet.at[k + 1], steps[k + 1])

    chips = rows_n // 2
    chip, core = lax.div(sp, 2), lax.rem(sp, 2)
    others = []
    for d in sorted(range(chips), key=lambda d: -min(d, chips - d)):
        at = lax.rem(chip + d, chips) * 2
        others.append((at + 1 - core, at + core))

    for i in range(n_img):
        pltpu.make_async_copy(x.at[i], xin.at[i], in_sem.at[i]).start()
    weight_copies = []
    for kx, dst, k0, n0 in ((1, wy, 0, 0), (1, wy, chan, chan), (0, wy, 0, chan), (2, wy, chan, 0), (0, ws, 0, 0), (2, ws, chan, chan)):
        weight_copies.append((w_a.at[:, :, kx], dst.at[:, :, pl.ds(k0, chan), pl.ds(n0, chan)]))
    weight_copies.append((w_down.at[:, 0], wd.at[:, 0, pl.ds(0, chan), :]))
    weight_copies.append((w_down.at[:, 1], wd.at[:, 0, pl.ds(chan, chan), :]))
    weight_copies.append((w_down.at[:, 2], wd.at[:, 1, pl.ds(chan, chan), :]))
    weight_copies.append((w_b, wb))
    weight_copies.append((bn_a, ga))
    weight_copies.append((bn_down, gd))
    weight_copies.append((bn_b, gb))
    weight_copies = [pltpu.make_async_copy(s, d, w_sem.at[k]) for k, (s, d) in enumerate(weight_copies)]
    for copy in weight_copies:
        copy.start()

    barrier = pltpu.get_barrier_semaphore()
    call(barrier, 1)

    for i in range(n_img):
        pltpu.make_async_copy(x.at[i], xin.at[i], in_sem.at[i]).wait()
    for i in range(n_img):
        for side, col0, pick in ((0, 0, 0), (1, width - 16, 15)):
            blk = xin[i, :, col0:col0 + 16, :].astype(F32)
            at = side * height * 16
            za0[i, at:at + height * 16, :] = blk.reshape(height * 16, chan)
            edge = za0[i, pl.ds(at + pick, height, stride=16), :]
            cs[0, side, i] = edge
            ksa[0, side, i] = edge[0:1]
            ksa[0, 2 + side, i] = edge[height - 1:height]

    hear(barrier, 1)

    def cor_bufs(e):
        return (ksa.at[e], kla.at[e]) if e < 4 else (ksb.at[e - 4], klb.at[e - 4])

    def start_cols(e, sides=SIDES, corners=CORNERS):
        for side in sides:
            d = -1 if side == 0 else 1

            @pl.when(col_ok[side])
            def _():
                pltpu.make_async_remote_copy(cs.at[e, side], cl.at[e, 1 - side], col_send.at[e, side], col_recv.at[e, 1 - side],
                                             device_id=device(0, d), device_id_type=MESH).start()
        src, dst = cor_bufs(e)
        for corner in corners:
            d_sp = -1 if corner < 2 else 1
            d_sp2 = -1 if corner % 2 == 0 else 1

            @pl.when(cor_ok[corner])
            def _():
                pltpu.make_async_remote_copy(src.at[corner], dst.at[3 - corner], cor_send.at[e, corner], cor_recv.at[e, 3 - corner],
                                             device_id=device(d_sp, d_sp2), device_id_type=MESH).start()

    def wait_cols(e, sides=SIDES, corners=CORNERS):
        for side in sides:
            @pl.when(col_ok[side])
            def _():
                pltpu.make_async_copy(cl.at[e, side], cl.at[e, side], col_recv.at[e, side]).wait()
        src, dst = cor_bufs(e)
        for corner in corners:
            @pl.when(cor_ok[corner])
            def _():
                pltpu.make_async_copy(dst.at[corner], dst.at[corner], cor_recv.at[e, corner]).wait()

    def wait_col_sends(e, sides=SIDES, corners=CORNERS):
        for side in sides:
            @pl.when(col_ok[side])
            def _():
                pltpu.make_async_copy(cs.at[e, side], cs.at[e, side], col_send.at[e, side]).wait()
        src, dst = cor_bufs(e)
        for corner in corners:
            @pl.when(cor_ok[corner])
            def _():
                pltpu.make_async_copy(src.at[corner], src.at[corner], cor_send.at[e, corner]).wait()

    def row_landing(e, side):
        if e == 0:
            return xh.at[side]
        return ha.at[e - 1, side] if e < 4 else hb.at[e - 4, side]

    def row_source(e, side, i):
        if e == 0:
            return xin.at[i, 0 if side == 0 else height - 1]
        src, n_rows = (zas[(e - 1) % 2], height) if e < 4 else (zbs[e % 2], low_h)
        return src.at[i, pl.ds(0 if side == 0 else (n_rows - 1) * line, line)]

    def send_rows(e, sides, images, cond=True):
        for side in sides:
            @pl.when(row_ok[side] & cond)
            def _():
                for i in images:
                    pltpu.make_async_remote_copy(row_source(e, side, i), row_landing(e, 1 - side).at[i], row_send.at[e, side, i],
                                                 row_recv.at[e, 1 - side, i], device_id=device(-1 if side == 0 else 1, 0),
                                                 device_id_type=MESH).start()

    def wait_rows(e, sides, images, cond=True):
        for side in sides:
            @pl.when(row_ok[side] & cond)
            def _():
                for i in images:
                    ref = row_landing(e, side).at[i]
                    pltpu.make_async_copy(ref, ref, row_recv.at[e, side, i]).wait()

    def wait_row_sends(e, sides=SIDES):
        for side in sides:
            @pl.when(row_ok[side])
            def _():
                ref = row_landing(e, side)

                def one(i, carry):
                    pltpu.make_async_copy(ref.at[i], ref.at[i], row_send.at[e, side, i]).wait()
                    return carry

                lax.fori_loop(0, n_img, one, 0)

    def sums_refs(e):
        return ta.at[e] if e < 3 else tb.at[e - 3]

    def start_sums(e, part):
        buf = sums_refs(e)
        buf[me] = part

        def send(to_sp, to_sp2):
            pltpu.make_async_remote_copy(buf.at[me], buf.at[me], st_send.at[e], st_recv.at[e], device_id={"sp": to_sp, "sp2": to_sp2},
                                         device_id_type=MESH).start()

        for k, pair in enumerate(others):
            def send_file(t, carry, pair=pair):
                to_sp2 = lax.rem(sp2 + cols_n // 2 + lax.select(lax.rem(t, 2) == 0, lax.div(t + 1, 2), -lax.div(t + 1, 2)), cols_n)
                for to_sp in pair:
                    send(to_sp, to_sp2)
                return carry

            lax.fori_loop(0, cols_n if k + 1 < len(others) else cols_n - 1, send_file, 0)
        send(others[-1][0], sp2)

    def finish_sums(e, num_pos):
        buf = sums_refs(e)
        rest = buf.at[pl.ds(0, n_dev - 1)]
        pltpu.make_async_copy(rest, rest, st_recv.at[e]).wait()
        total = jnp.sum(buf[...], axis=0) * (1.0 / num_pos)
        lines = total.shape[0] // 2
        mean = total[0:lines]
        var = total[lines:] - mean * mean
        return mean, lax.rsqrt(var + EPS)

    def bn(z, par):
        mean, inv, gain, shift = par
        return jnp.maximum(gain * (z - mean) * inv + shift, 0.0)

    def keep(cond, val):
        return jnp.where(cond, val, 0.0)

    def prep_x(i, k):
        xf, ya, sa = xfs[k], yas[k], sas[k]
        last = height + 1
        for r in range(height):
            xf[pl.ds((r + 1) * xstride + PAD, width), :] = xin[i, r].astype(F32)
        xf[pl.ds(PAD, width), :] = keep(has_up, xh[0, i].astype(F32))
        xf[pl.ds(last * xstride + PAD, width), :] = keep(has_down, xh[1, i].astype(F32))
        xf[pl.ds(xstride + PAD - 1, height, stride=xstride), :] = keep(has_left, cl[0, 0, i])
        xf[pl.ds(xstride + PAD + width, height, stride=xstride), :] = keep(has_right, cl[0, 1, i])
        for corner in CORNERS:
            row = 0 if corner < 2 else last
            col = PAD - 1 if corner % 2 == 0 else PAD + width
            xf[row * xstride + col:row * xstride + col + 1, :] = keep(cor_ok[corner], kla[0, corner, i])
        for r in range(height + 2):
            base = r * xstride + PAD
            even = xf[pl.ds(base, half_w, stride=2), :]
            odd = xf[pl.ds(base + 1, half_w, stride=2), :]
            before = xf[pl.ds(base - 1, half_w, stride=2), :]
            after = xf[pl.ds(base + 2, half_w, stride=2), :]
            ya[r] = jnp.concatenate([even, odd], axis=1).astype(BF16)
            sa[r] = jnp.concatenate([before, after], axis=1).astype(BF16)

    def norm_a(e, par, i, k, up=True):
        za, yfa, ya, sa = zas[(e - 1) % 2], yfas[k], yas[k], sas[k]
        last = height + 1
        lo = 0 if up else 1
        for r in range(lo, height + 2):
            if r == 0:
                val = keep(has_up, bn(ha[e - 1, 0, i], par))
            elif r == last:
                val = keep(has_down, bn(ha[e - 1, 1, i], par))
            else:
                val = bn(za[i, pl.ds((r - 1) * line, line), :], par)
            base = r * 2 * fstride + PAD
            yfa[base:base + half_w, :] = val[0:half_w]
            yfa[base + fstride:base + fstride + half_w, :] = val[half_w:]
        if up:
            yfa[pl.ds(3 * fstride + PAD - 1, height, stride=2 * fstride), :] = keep(has_left, bn(cl[e, 0, i], par))
        yfa[pl.ds(2 * fstride + PAD + half_w, height, stride=2 * fstride), :] = keep(has_right, bn(cl[e, 1, i], par))
        for corner in CORNERS if up else (3,):
            row = 0 if corner < 2 else last
            at = row * 2 * fstride + (fstride + PAD - 1 if corner % 2 == 0 else PAD + half_w)
            yfa[at:at + 1, :] = keep(cor_ok[corner], bn(kla[e, corner, i], par))
        for r in range(lo, height + 2):
            base = r * 2 * fstride + PAD
            even = yfa[base:base + half_w, :]
            odd = yfa[base + fstride:base + fstride + half_w, :]
            before = yfa[base + fstride - 1:base + fstride - 1 + half_w, :]
            after = yfa[base + 1:base + 1 + half_w, :]
            ya[r] = jnp.concatenate([even, odd], axis=1).astype(BF16)
            sa[r] = jnp.concatenate([before, after], axis=1).astype(BF16)

    def norm_b(e, par, i, k):
        zb, yfb, yb = zbs[e % 2], yfbs[k], ybs[k]
        last = low_h + 1
        halves = [tuple(p[h:h + 1] for p in par) for h in SIDES]
        tall = tuple(jnp.concatenate([p] * low_h, axis=0) for p in par)
        for r in range(low_h + 2):
            for h in SIDES:
                if r == 0:
                    val = keep(has_up, bn(hb[e - 4, 0, i, pl.ds(h * half_w, half_w), :], halves[h]))
                elif r == last:
                    val = keep(has_down, bn(hb[e - 4, 1, i, pl.ds(h * half_w, half_w), :], halves[h]))
                else:
                    val = bn(zb[i, pl.ds(((r - 1) * 2 + h) * half_w, half_w), :], halves[h])
                base = (r * 2 + h) * fstride + PAD
                yfb[base:base + half_w, :] = val
        yfb[pl.ds(2 * fstride + PAD - 1, 2 * low_h, stride=fstride), :] = keep(has_left, bn(cl[e, 0, i], tall))
        yfb[pl.ds(2 * fstride + PAD + half_w, 2 * low_h, stride=fstride), :] = keep(has_right, bn(cl[e, 1, i], tall))
        for corner in CORNERS:
            row = 0 if corner < 2 else last
            val = keep(cor_ok[corner], bn(klb[e - 4, corner, i], par))
            for h in SIDES:
                at = (row * 2 + h) * fstride + (PAD - 1 if corner % 2 == 0 else PAD + half_w)
                yfb[at:at + 1, :] = val[h:h + 1]
        for r in range(low_h + 2):
            base = r * 2 * fstride + PAD
            for kx in TAPS:
                at = base + kx - 1
                yb[kx, r] = jnp.concatenate([yfb[at:at + half_w, :], yfb[at + fstride:at + fstride + half_w, :]], axis=1).astype(BF16)

    def add_sums(acc, carry):
        tiles = acc.reshape(acc.shape[0] // 8, 8, acc.shape[1])
        return carry[0] + jnp.sum(tiles, axis=0), carry[1] + jnp.sum(tiles * tiles, axis=0)

    zero_sums = (jnp.zeros((8, wide), F32), jnp.zeros((8, wide), F32))

    def edges_a(e, i):
        za = zas[(e - 1) % 2]
        first = za[i, pl.ds(0, height, stride=line), :]
        final = za[i, pl.ds(line - 1, height, stride=line), :]
        for side, edge in enumerate((first, final)):
            cs[e, side, i] = edge
            ksa[e, side, i] = edge[0:1]
            ksa[e, 2 + side, i] = edge[height - 1:height]

    def edges_b(e, i):
        zb = zbs[e % 2]
        first = zb[i, pl.ds(0, 2 * low_h, stride=half_w), :]
        final = zb[i, pl.ds(half_w - 1, 2 * low_h, stride=half_w), :]
        for side, edge in enumerate((first, final)):
            cs[e, side, i] = edge
            ksb[e - 4, side, i] = edge[0:2]
            ksb[e - 4, 2 + side, i] = edge[2 * low_h - 2:2 * low_h]

    def store_z(ref, i, acc, rows):
        for r in range(rows):
            at = r * line
            ref[i, at:at + half_w, :] = acc[r * half_w:(r + 1) * half_w, 0:chan]
            ref[i, at + half_w:at + line, :] = acc[r * half_w:(r + 1) * half_w, chan:wide]

    def products(pairs):
        acc = None
        for lhs, w in pairs:
            d = jnp.dot(lhs, w, preferred_element_type=F32)
            acc = d if acc is None else acc + d
        return acc

    def conv_a(layer, i, k, carry):
        pairs = []
        for ky in TAPS:
            for ref, w in ((yas[k], wy), (sas[k], ws)):
                pairs.append((ref[ky:ky + height].reshape(height * half_w, wide), w[layer, ky]))
        acc = products(pairs)
        store_z(zas[layer % 2], i, acc, height)
        edges_a(layer + 1, i)
        return add_sums(acc, carry)

    def conv_down(i, k, carry):
        pairs = []
        for ky in TAPS:
            for part, ref in enumerate((yas[k], sas[k])):
                pairs.append((jnp.concatenate([ref[1 + 2 * r + ky] for r in range(low_h)], axis=0), wd[ky, part]))
        acc = products(pairs)
        store_z(zbs[0], i, acc, low_h)
        edges_b(4, i)
        return add_sums(acc, carry)

    def conv_b(layer, i, k, carry):
        pairs = []
        for ky in TAPS:
            for kx in TAPS:
                pairs.append((ybs[k][kx, ky:ky + low_h].reshape(low_h * half_w, wide), wb[layer, ky, kx]))
        acc = products(pairs)
        if layer == 0:
            store_z(zb1, i, acc, low_h)
            edges_b(5, i)
        else:
            zo[i] = acc.reshape(low_h, half_w, wide)
        return add_sums(acc, carry)

    def layer(e, prep, conv, in_sides, out_sides, early):
        prep(0, 0)

        half = n_img // 2

        def pair(j, carry):
            i = 2 * j
            wait_rows(e, in_sides, (i + 1, i + 2))
            for u in SIDES:
                prep(i + u + 1, 1 - u)
                carry = conv(i + u, u, carry)
            for u in SIDES:
                send_rows(e + 1, out_sides, (i + u,), i + u < early)
            return carry

        carry = lax.fori_loop(0, half // 2, pair, zero_sums)
        wait_rows(e, in_sides, range(half + 1, n_img))
        if e == 0:
            meet_again(1)
        for i in range(half, n_img):
            if i + 1 < n_img:
                prep(i + 1, (i + 1) % 2)
            carry = conv(i, i % 2, carry)
        s1, s2 = carry
        s1, s2 = (jnp.sum(s, axis=0, keepdims=True) for s in (s1, s2))
        if e < 3:
            part = [s1[:, 0:chan] + s1[:, chan:], s2[:, 0:chan] + s2[:, chan:]]
        else:
            part = [s1[:, 0:chan], s1[:, chan:], s2[:, 0:chan], s2[:, chan:]]
        if e == 0:
            for k in range(2, len(steps)):
                meet_again(k)
        start_sums(e, jnp.concatenate(part, axis=0))
        if e < 5:
            both = len(out_sides) == 2
            start_cols(e + 1, SIDES if both else (0,), CORNERS if both else (0,))
            send_rows(e + 1, out_sides, range(early, n_img))

    start_cols(0)
    send_rows(0, SIDES, range(n_img))
    call(meet.at[0], steps[0])
    zeros = jnp.zeros((chan, chan), BF16)
    for depth in TAPS:
        for ky in TAPS:
            ws[depth, ky, 0:chan, chan:wide] = zeros
            ws[depth, ky, chan:wide, 0:chan] = zeros
    for ky in TAPS:
        wd[ky, 1, 0:chan, :] = jnp.zeros((chan, wide), BF16)
    for copy in weight_copies[:6]:
        copy.wait()
    meet_again(0)
    wait_cols(0)

    pos_a = n_dev * n_img * height * width
    pos_b = n_dev * n_img * low_h * half_w

    def params_a(e, layer):
        mean, inv = finish_sums(e, pos_a)
        return mean, inv, ga[layer, 0:1], ga[layer, 1:2]

    def params_b(e, ref):
        mean, inv = finish_sums(e, pos_b)
        gain = jnp.concatenate([ref[0:1, 0:chan], ref[0:1, chan:]], axis=0)
        shift = jnp.concatenate([ref[1:2, 0:chan], ref[1:2, chan:]], axis=0)
        return mean, inv, gain, shift

    part = functools.partial
    wait_rows(0, SIDES, SIDES[:1])
    layer(0, prep_x, part(conv_a, 0), SIDES, SIDES, EARLY_A)

    for copy in weight_copies[6:]:
        copy.wait()
    wait_row_sends(0)
    wait_col_sends(0)
    wait_cols(1)
    wait_rows(1, SIDES, SIDES[:1])
    layer(1, part(norm_a, 1, params_a(0, 0)), part(conv_a, 1), SIDES, SIDES, EARLY_A)

    wait_row_sends(1)
    wait_col_sends(1)
    wait_cols(2)
    wait_rows(2, SIDES, SIDES[:1])
    layer(2, part(norm_a, 2, params_a(1, 1)), part(conv_a, 2), SIDES, (0,), EARLY_A)

    wait_row_sends(2)
    wait_col_sends(2)
    wait_cols(3, (1,), (3,))
    wait_rows(3, SIDES[1:], SIDES[:1])
    layer(3, part(norm_a, 3, params_a(2, 2), up=False), conv_down, (1,), SIDES, EARLY_B)

    wait_row_sends(3, (0,))
    wait_col_sends(3, (0,), (0,))
    wait_cols(4)
    wait_rows(4, SIDES, SIDES[:1])
    layer(4, part(norm_b, 4, params_b(3, gd)), part(conv_b, 0), SIDES, SIDES, EARLY_B)

    wait_row_sends(4)
    wait_col_sends(4)
    wait_cols(5)
    wait_rows(5, SIDES, SIDES[:1])
    layer(5, part(norm_b, 5, params_b(4, gb.at[0])), part(conv_b, 1), SIDES, (), 0)

    wait_row_sends(5)
    wait_col_sends(5)
    mean, inv = finish_sums(5, pos_b)
    for out, val in ((mean_o, mean), (inv_o, inv)):
        for h in SIDES:
            out[:, h * chan:(h + 1) * chan] = val[h:h + 1]
    gain_o[...] = gb[1, 0:1]
    shift_o[...] = gb[1, 1:2]

    for e in range(6):
        buf = sums_refs(e)
        rest = buf.at[pl.ds(0, n_dev - 1)]
        pltpu.make_async_copy(rest, rest, st_send.at[e]).wait()


def net(rows_n, cols_n, x, w_a, bn_a, w_down, bn_down, w_b, bn_b):
    n_img, height, width, chan = x.shape
    half_w, low_h = width // 2, height // 2
    n_dev = rows_n * cols_n
    vmem, dma = pltpu.VMEM, pltpu.SemaphoreType.DMA
    line, wide = 2 * half_w, 2 * chan
    plane = half_w + 2 * PAD
    a_sums, b_sums = 3, 3
    n_ex = a_sums + b_sums
    two, corners = len(SIDES), len(CORNERS)
    scratch = [
        vmem(x.shape, BF16),
        vmem((two, n_img, width, chan), BF16),
        *[vmem(((height + 2) * (width + 2 * PAD), chan), F32)] * two,
        *[vmem((n_img, height * line, chan), F32)] * two,
        *[vmem((n_img, low_h * line, chan), F32)] * two,
        vmem((a_sums, two, n_img, line, chan), F32),
        vmem((b_sums - 1, two, n_img, line, chan), F32),
        *[vmem(((height + 2) * 2 * plane, chan), F32)] * two,
        *[vmem(((low_h + 2) * 2 * plane, chan), F32)] * two,
        *[vmem((height + 2, half_w, wide), BF16)] * 4,
        *[vmem((3, low_h + 2, half_w, wide), BF16)] * two,
        *[vmem((n_ex, two, n_img, height, chan), F32)] * two,
        *[vmem((a_sums + 1, corners, n_img, 1, chan), F32)] * two,
        *[vmem((b_sums - 1, corners, n_img, 2, chan), F32)] * two,
        vmem((a_sums, n_dev, 2, chan), F32),
        vmem((b_sums, n_dev, 4, chan), F32),
        *[vmem((a_sums, 3, wide, wide), BF16)] * two,
        vmem((3, two, wide, wide), BF16),
        vmem(w_b.shape, BF16),
        vmem(bn_a.shape, F32),
        vmem(bn_down.shape, F32),
        vmem(bn_b.shape, F32),
        dma((n_img,)),
        dma((13,)),
        *[dma((n_ex, two, n_img))] * two,
        *[dma((n_ex, two))] * two,
        *[dma((n_ex, corners))] * two,
        *[dma((n_ex,))] * two,
        pltpu.SemaphoreType.REGULAR((3,)),
    ]
    hbm_spec = pl.BlockSpec(memory_space=pltpu.HBM)
    line_out = jax.ShapeDtypeStruct((1, wide), F32)
    z, *vectors = pl.pallas_call(
        functools.partial(net_kernel, (rows_n, cols_n, n_img, height, width, chan)),
        out_shape=(jax.ShapeDtypeStruct((n_img, low_h, half_w, wide), F32),) + (line_out,) * 4,
        in_specs=[hbm_spec] * 7,
        out_specs=(pl.BlockSpec(memory_space=pltpu.VMEM),) * 5,
        scratch_shapes=scratch,
        compiler_params=pltpu.CompilerParams(collective_id=0, has_side_effects=True, vmem_limit_bytes=40 * 1024 * 1024),
        name="conv_bn_net",
    )(*[pltpu.with_memory_space_constraint(arg, pltpu.HBM) for arg in (x, w_a, bn_a, w_down, bn_down, w_b, bn_b)])
    mean, inv, gain, shift = [v.reshape(wide) for v in vectors]
    return jnp.maximum(gain * (z - mean) * inv + shift, 0.0).astype(BF16)


def solution(mesh):
    tile_spec = P("dp", "sp", "sp2", None)
    per_device = functools.partial(net, mesh.shape["sp"], mesh.shape["sp2"])
    return jax.shard_map(per_device, mesh=mesh, in_specs=(tile_spec, P(), P(), P(), P(), P(), P()), out_specs=tile_spec, check_vma=False)
```
